32 devices in a mesh: cp: 8 (over z, x), tp: 4 (over y, core).
Axes of the slice: x: 2, y: 2, z: 4, core: 2. Of those that a mesh axis runs over, the one named last changes fastest.
Arguments:
- tokens_in: bfloat16 [2048, 2048], P('cp'), may hold values from -6 to 6
- doc_ids: int32 [2048], P('cp'), may hold values from 0 to 3, never falling along the last dimension, each value on 1 to 1024 neighbouring positions
- expert_ids: int32 [2048, 2], P('cp'), may hold values from 0 to 7, all different within a row; in each aligned block of 256 rows (0 to 255, 256 to 511, ...) at most 96 rows name the same one
- attn_gain: bfloat16 [2048], P('cp'), may hold values from 0.099609375 to 1.8984375
- q_gain: bfloat16 [128], replicated, may hold values from 0.099609375 to 1.8984375
- k_gain: bfloat16 [128], replicated, may hold values from 0.099609375 to 1.8984375
- w_query: bfloat16 [2048, 2048], P('cp', 'tp'), may hold values from -0.125 to 0.125
- w_key: bfloat16 [2048, 2048], P('cp', 'tp'), may hold values from -0.125 to 0.125
- w_value: bfloat16 [2048, 2048], P('cp', 'tp'), may hold values from -0.125 to 0.125
- w_output: bfloat16 [2048, 2048], P('cp', 'tp'), may hold values from -2 to 2
- ffn_gain: bfloat16 [2048], P('cp'), may hold values from 0.099609375 to 1.8984375
- w_router: bfloat16 [2048, 8], P('cp'), may hold values from -0.25 to 0.25
- w_gate: bfloat16 [2048, 8, 1024], P('cp', None, 'tp'), may hold values from -0.125 to 0.125
- w_up: bfloat16 [2048, 8, 1024], P('cp', None, 'tp'), may hold values from -0.125 to 0.125
- w_down: bfloat16 [2048, 8, 1024], P('cp', None, 'tp'), may hold values from -0.75 to 0.75
- cotangent: bfloat16 [2048, 2048], P('cp'), may hold values from -6 to 6
Outputs:
- block_out: bfloat16 [2048, 2048], P('cp')
- grad_in: float32 [2048, 2048], P('cp')
- grad_attn_gain: float32 [2048], P('cp')
- grad_q_gain: float32 [128], replicated
- grad_k_gain: float32 [128], replicated
- grad_query: float32 [2048, 2048], P('cp', 'tp')
- grad_key: float32 [2048, 2048], P('cp', 'tp')
- grad_value: float32 [2048, 2048], P('cp', 'tp')
- grad_output: float32 [2048, 2048], P('cp', 'tp')
- grad_ffn_gain: float32 [2048], P('cp')
- grad_router: float32 [2048, 8], P('cp')
- grad_gate: float32 [2048, 8, 1024], P('cp', None, 'tp')
- grad_up: float32 [2048, 8, 1024], P('cp', None, 'tp')
- grad_down: float32 [2048, 8, 1024], P('cp', None, 'tp')
The draws below stay inside these ranges and needn't reach their ends.
Inputs may be any that keep to these rules, and one draw needn't show every extreme that they name: `doc_ids`: document numbers never fall along the stream; every document holds 1 to 1024 tokens and one holds exactly 1024. `expert_ids`: the 2 experts of a token differ. Among the tokens of one index of cp no expert is named more than 96 times, and on some index some expert is named exactly 96 times.
All inputs are finite; a program needn't handle non-finite values.
Results may differ from the reference program's by a relative error of at most 0.025.
Values may be sent and summed in bfloat16 or wider, within the bound.
A program may use at most 256 MiB of HBM per device.

```python
import math
import jax
import jax.numpy as jnp
import numpy as np
from jax import lax

D = 2048
HEADS = 16
HEAD_DIM = 128
FF = 1024
EXPERTS = 8
TOPK = 2
DOCS = 4
TOK_DEV = 256
TOKENS = 2048
DOC_MOST = 1024
CAP = 96


def level_of(own_key, dims, split, least, top_value):
    loudness = 1.0
    for dim, blocks in split:
        steps = jax.random.uniform(jax.random.fold_in(jax.random.fold_in(own_key, 6), dim), (blocks,), jnp.float32, least / len(split), top_value / len(split))
        loudness = loudness * jnp.repeat(jnp.exp(steps), dims[dim] // blocks).reshape((-1,) + (1,) * (len(dims) - 1 - dim))
    return loudness


def split_up(number_of, total, reach, lean):
    loads = [(1 << 20) // math.isqrt(grade ** lean) + 1 for grade in range(2, number_of + 1)]
    rest, counts = total - reach - (number_of - 1), [1] * (number_of - 1)
    while rest > 0:
        free = [i for i in range(number_of - 1) if counts[i] < reach]
        pool, remaining = sum([loads[i] for i in free]), rest
        for i in free:
            addition = min(reach - counts[i], max(1, remaining * loads[i] // pool), rest)
            counts[i] = counts[i] + addition
            rest = rest - addition
    return np.array([reach] + counts)


def uneven(key, amount, total, limit, slope):
    if amount == 2:
        one = jax.random.randint(key, (), max(1, total - limit), min(limit, total - 1) + 1)
        return jnp.stack([one, total - one])
    sizes = jnp.asarray(split_up(amount, total, limit, slope), jnp.int32)
    twos = (amount - 1) // 2
    donor, receiver = sizes[1:1 + 2 * twos:2], sizes[2:2 + 2 * twos:2]
    margin = jnp.minimum(donor - 1, limit - receiver)
    shifted = jax.random.randint(jax.random.fold_in(key, 1), (twos,), 0, 1 << 20) % (margin + 1)
    sizes = sizes.at[1:1 + 2 * twos:2].set(donor - shifted).at[2:2 + 2 * twos:2].set(receiver + shifted)
    return sizes[jax.random.permutation(jax.random.fold_in(key, 2), amount)]


def routed_block(rng, own, number, rows, count, top, limit, slope):
    sequence = jax.random.permutation(rng, count)
    packed, usual = portions_of(count, rows * top, limit, slope, True), portions_of(count, rows * top, limit, slope, False)
    places = jnp.arange(count)

    def named(lengths, turn):
        used = int((lengths > 0).sum())
        fixed = max(1, used // 4)
        passed = fixed + (places - fixed + turn * (used - fixed)) % max(1, count - fixed)
        return jnp.zeros((count,), jnp.int32).at[sequence[jnp.where(places < fixed, places, passed)]].set(jnp.asarray(lengths, jnp.int32))

    lengths = jnp.where(number % 4 == 0, named(packed, number // 4), named(usual, number - number // 4 - 1))
    mixed = jax.random.permutation(jax.random.fold_in(own, 3), count)
    source_of, taker = mixed[0:count // 2 * 2:2], mixed[1:count // 2 * 2:2]
    room = jnp.minimum(lengths[source_of] - 1, limit - lengths[taker]) // 2
    room = jnp.where((source_of == sequence[0]) | (taker == sequence[0]) | (lengths[taker] == 0), 0, jnp.maximum(room, 0))
    passed = jax.random.randint(jax.random.fold_in(own, 4), (count // 2,), 0, 1 << 20) % (room + 1)
    lengths = lengths.at[source_of].add(-passed).at[taker].add(passed)
    members = jnp.searchsorted(jnp.cumsum(lengths), jnp.arange(rows * top), side="right").astype(jnp.int32)
    table = members.reshape(top, rows).T
    table = table[jax.random.permutation(jax.random.fold_in(own, 1), rows)]
    turn = jax.random.randint(jax.random.fold_in(own, 2), (rows, 1), 0, top)
    return jnp.take_along_axis(table, (jnp.arange(top)[None, :] + turn) % top, axis=1)


def portions_of(number_of, total, limit, skew, full):
    loads = [(1 << 20) // math.isqrt(rank ** skew) + 1 for rank in range(1, number_of + 1)]
    largest = limit if full else min(limit, max(-(-total // number_of), total * loads[0] // sum(loads)))
    least = 1 if total - largest >= number_of - 1 else 0
    holding, surplus = [largest] + [least] * (number_of - 1), total - largest - least * (number_of - 1)
    while surplus > 0:
        candidates = [i for i in range(1, number_of) if holding[i] < largest] or [i for i in range(1, number_of) if holding[i] < limit]
        whole, budget = sum([loads[i] for i in candidates]), surplus
        for i in candidates:
            addition = min(limit - holding[i], max(1, budget * loads[i] // whole), surplus)
            holding[i] = holding[i] + addition
            surplus = surplus - addition
    return np.array(holding)


def noise(rng, shape, deviation, most, cuts=(), kind=jnp.bfloat16):
    values = jax.random.normal(rng, shape, jnp.float32) * deviation
    if len(cuts) > 0:
        values = level_of(rng, shape, cuts, -0.22, 0.18) * values
    return jnp.clip(values, min=-most, max=most).astype(kind)


def setup_inputs(seed: int = 0) -> dict:
    key_of = jax.random.split(jax.random.key(seed), 17)
    tokens_in = noise(key_of[0], (TOKENS, D), 1.0, 6.0, ((0, 8),))
    doc_ids = jnp.searchsorted(jnp.cumsum(uneven(key_of[1], DOCS, TOKENS, DOC_MOST, 1)), jnp.arange(TOKENS), side="right").astype(jnp.int32)
    expert_ids_keys = jax.random.split(jax.random.fold_in(key_of[2], 1), TOKENS // TOK_DEV)
    expert_ids_turns = jax.random.permutation(jax.random.fold_in(key_of[2], 3), TOKENS // TOK_DEV)
    expert_ids = jax.vmap(lambda own, number: routed_block(jax.random.fold_in(key_of[2], 2), own, number, TOK_DEV, EXPERTS, TOPK, CAP, 1))(expert_ids_keys, expert_ids_turns).reshape((TOKENS, TOPK))
    attn_gain = jnp.clip(1.0 + 0.18 * jax.random.normal(key_of[3], (D,), jnp.float32), 0.099609375, 1.8984375).astype(jnp.bfloat16)
    q_gain = jnp.clip(1.0 + 0.18 * jax.random.normal(key_of[4], (HEAD_DIM,), jnp.float32), 0.099609375, 1.8984375).astype(jnp.bfloat16)
    k_gain = jnp.clip(1.0 + 0.18 * jax.random.normal(key_of[5], (HEAD_DIM,), jnp.float32), 0.099609375, 1.8984375).astype(jnp.bfloat16)
    w_query = noise(key_of[6], (D, HEADS * HEAD_DIM), D ** -0.5, 0.125, ((0, 8), (1, 4)))
    w_key = noise(key_of[7], (D, HEADS * HEAD_DIM), D ** -0.5, 0.125, ((0, 8), (1, 4)))
    w_value = noise(key_of[8], (D, HEADS * HEAD_DIM), D ** -0.5, 0.125, ((0, 8), (1, 4)))
    w_output = noise(key_of[9], (D, HEADS * HEAD_DIM), (max(1, 8 * HEADS * HEAD_DIM // TOKENS)) ** -0.5, 2.0, ((0, 8), (1, 4)))
    ffn_gain = jnp.clip(1.0 + 0.18 * jax.random.normal(key_of[10], (D,), jnp.float32), 0.099609375, 1.8984375).astype(jnp.bfloat16)
    w_router = noise(key_of[11], (D, EXPERTS), (D // 4) ** -0.5, 0.25, ((0, 8),))
    w_gate = noise(key_of[12], (D, EXPERTS, FF), D ** -0.5, 0.125, ((0, 8), (2, 4)))
    w_up = noise(key_of[13], (D, EXPERTS, FF), D ** -0.5, 0.125, ((0, 8), (2, 4)))
    w_down = noise(key_of[14], (D, EXPERTS, FF), (FF // 16) ** -0.5, 0.75, ((0, 8), (2, 4)))
    cotangent = noise(key_of[15], (TOKENS, D), 1.0, 6.0, ((0, 8),))
    return {"tokens_in": tokens_in, "doc_ids": doc_ids, "expert_ids": expert_ids, "attn_gain": attn_gain, "q_gain": q_gain, "k_gain": k_gain, "w_query": w_query, "w_key": w_key, "w_value": w_value, "w_output": w_output, "ffn_gain": ffn_gain, "w_router": w_router, "w_gate": w_gate, "w_up": w_up, "w_down": w_down, "cotangent": cotangent}


@jax.custom_vjp
def low(v):
    return lax.optimization_barrier(v.astype(jnp.bfloat16)).astype(jnp.float32)

@jax.custom_vjp
def low_back(v):
    return v

def low_keep(v):
    return (low(v), None)

def low_pass(kept, grad):
    return (grad,)

def back_keep(v):
    return (v, None)

def back_low(kept, grad):
    return (low(grad),)
low.defvjp(low_keep, low_pass)
low_back.defvjp(back_keep, back_low)
eps = 1e-05
theta = 50000.0
negative = -1e+30
highest = lax.Precision.HIGHEST

def rms_norm(values, gain_vec):
    factor = lax.rsqrt(lax.optimization_barrier(jnp.mean(values * values, axis=-1, keepdims=True)) + eps)
    return values * factor * gain_vec

def rotary_tables(positions, head_dim):
    half_dim = head_dim // 2
    inverse_freq = theta ** (-2.0 * jnp.arange(half_dim, dtype=jnp.float32) / head_dim)
    angles = positions[:, None] * inverse_freq[None, :]
    cos_tab = jnp.concatenate([jnp.cos(angles), jnp.cos(angles)], axis=-1)
    sin_tab = jnp.concatenate([jnp.sin(angles), jnp.sin(angles)], axis=-1)
    return (cos_tab, sin_tab)

def rotate_half(tensor):
    half_dim = tensor.shape[-1] // 2
    return jnp.concatenate([-tensor[..., half_dim:], tensor[..., :half_dim]], axis=-1)

def qk_prepare(raw_heads, gain_vec, cos_tab, sin_tab):
    normed = rms_norm(raw_heads, gain_vec)
    return normed * cos_tab[:, None, :] + rotate_half(normed) * sin_tab[:, None, :]

def forward(tokens, attn_gain, q_gain, k_gain, w_query, w_key, w_value, w_output, ffn_gain, w_router, w_gate, w_up, w_down, doc_ids, expert_ids):
    length = tokens.shape[0]
    positions = jnp.arange(length, dtype=jnp.float32)
    cos_tab, sin_tab = rotary_tables(positions, HEAD_DIM)
    normed_in = low(rms_norm(tokens, attn_gain))
    q_raw = low_back(jnp.dot(normed_in, w_query, precision=highest)).reshape(length, HEADS, HEAD_DIM)
    k_raw = low_back(jnp.dot(normed_in, w_key, precision=highest)).reshape(length, HEADS, HEAD_DIM)
    q_rot = low(qk_prepare(q_raw, q_gain, cos_tab, sin_tab))
    k_rot = low(qk_prepare(k_raw, k_gain, cos_tab, sin_tab))
    values = low(low_back(jnp.dot(normed_in, w_value, precision=highest))).reshape(length, HEADS, HEAD_DIM)
    block_rows = min(512, length)
    blocks = length // block_rows
    scale_factor = HEAD_DIM ** (-0.5)

    def attend(inputs):
        q_block, doc_block = inputs
        scores = low_back(jnp.einsum('qhd,khd->hqk', q_block, k_rot, precision=highest) * scale_factor)
        keep_mask = (doc_block[:, None] == doc_ids[None, :])[None, :, :]
        soft_probs = jax.nn.softmax(jnp.where(keep_mask, scores, negative), axis=-1)
        mixture = jnp.einsum('hqk,khd->qhd', low(soft_probs), values, precision=highest)
        return low(low_back(mixture))
    heads_out = lax.map(jax.checkpoint(attend), (q_rot.reshape(blocks, block_rows, HEADS, HEAD_DIM), doc_ids.reshape(blocks, block_rows)))
    heads_out = heads_out.reshape(length, HEADS * HEAD_DIM)
    attn_mix = low_back(jnp.dot(heads_out, w_output.T, precision=highest))
    hidden = tokens + attn_mix
    normed_mid = low(rms_norm(hidden, ffn_gain))
    logits = low_back(jnp.dot(normed_mid, w_router, precision=highest))
    router_probs = jax.nn.softmax(logits, axis=-1)
    chosen = lax.optimization_barrier(jnp.sum((expert_ids[:, :, None] == jnp.arange(EXPERTS, dtype=jnp.int32)[None, None, :]).astype(jnp.float32), axis=1))
    combine = router_probs * chosen
    gate_pre = low_back(jnp.einsum('sd,def->sef', normed_mid, w_gate, precision=highest))
    up_pre = low_back(jnp.einsum('sd,def->sef', normed_mid, w_up, precision=highest))
    activated = low(jax.nn.silu(gate_pre) * up_pre)
    expert_out = low_back(jnp.einsum('sef,def->sed', activated, w_down, precision=highest))
    mixture = lax.optimization_barrier(jnp.sum(combine[:, :, None] * expert_out, axis=1))
    return hidden + mixture

def reference(tokens_in, doc_ids, expert_ids, attn_gain, q_gain, k_gain, w_query, w_key, w_value, w_output, ffn_gain, w_router, w_gate, w_up, w_down, cotangent):
    floats = [member.astype(jnp.float32) for member in (tokens_in, attn_gain, q_gain, k_gain, w_query, w_key, w_value, w_output, ffn_gain, w_router, w_gate, w_up, w_down)]

    def wrapped(*inputs):
        return forward(*inputs, doc_ids, expert_ids)
    block_out, pullback = jax.vjp(wrapped, *floats)
    grads = pullback(cotangent.astype(jnp.float32))
    return (block_out.astype(jnp.bfloat16), grads[0], grads[1], grads[2], grads[3], grads[4], grads[5], grads[6], grads[7], grads[8], grads[9], grads[10], grads[11], grads[12])
```

```python
import functools
import itertools

import jax
import jax.numpy as jnp
from jax import lax
from jax.experimental import pallas as pl
from jax.experimental.pallas import tpu as pltpu
from jax.sharding import Mesh
from jax.sharding import PartitionSpec as P

eps = 1e-05
theta = 50000.0
negative = -1e30
AXES = ("b", "a", "y", "c")
TP = ("y", "c")
MESH = pl.DeviceIdType.MESH
bf16 = jnp.bfloat16
f32 = jnp.float32


def exchange(sizes, cid, items):
    counts = []
    outs = []
    for kind, axes, array, space in items:
        count = 1
        for axis in axes:
            count *= sizes[axis]
        counts.append(count)
        block = array.shape if kind == "all" else array.shape[1:]
        outs.append(jax.ShapeDtypeStruct((count,) + tuple(block), array.dtype))

    plans = []
    peers = []
    for (kind, axes, array, space), count in zip(items, counts):
        plan = []
        for offs in itertools.product(*[range(sizes[axis]) for axis in axes]):
            if not any(offs):
                continue
            full = tuple(offs[axes.index(axis)] if axis in axes else 0 for axis in AXES)
            plan.append(full)
            if full not in peers:
                peers.append(full)
        plans.append(plan)
    total = sum(len(plan) for plan in plans)
    number = len(items)

    def kernel(*refs):
        ins, dst = refs[:number], refs[number : 2 * number]
        send, recv, local = refs[2 * number :]
        me = {axis: lax.axis_index(axis) for axis in AXES}

        def there(full):
            return {
                axis: lax.rem(me[axis] + off, sizes[axis]) for axis, off in zip(AXES, full) if off
            }

        def rank(axes, place):
            index = 0
            for axis in axes:
                index = index * sizes[axis] + place.get(axis, me[axis])
            return index

        barrier = pltpu.get_barrier_semaphore()
        for full in peers:
            pl.semaphore_signal(barrier, inc=1, device_id=there(full), device_id_type=MESH)
        pl.semaphore_wait(barrier, len(peers))
        copies = []
        slot = 0
        for i, (kind, axes, array, space) in enumerate(items):
            mine = rank(axes, {})
            for full in plans[i]:
                place = there(full)
                source = ins[i] if kind == "all" else ins[i].at[rank(axes, place)]
                copy = pltpu.make_async_remote_copy(
                    src_ref=source,
                    dst_ref=dst[i].at[mine],
                    send_sem=send.at[slot],
                    recv_sem=recv.at[slot],
                    device_id=place,
                    device_id_type=MESH,
                )
                copy.start()
                copies.append(copy)
                slot += 1
        for i, (kind, axes, array, space) in enumerate(items):
            mine = rank(axes, {})
            source = ins[i] if kind == "all" else ins[i].at[mine]
            copy = pltpu.make_async_copy(source, dst[i].at[mine], local.at[i])
            copy.start()
            copies.append(copy)
        for copy in copies:
            copy.wait()

    spaces = [
        pl.BlockSpec(memory_space=pltpu.VMEM if item[3] == "v" else pl.ANY) for item in items
    ]
    return pl.pallas_call(
        kernel,
        out_shape=outs,
        in_specs=spaces,
        out_specs=spaces,
        scratch_shapes=[
            pltpu.SemaphoreType.DMA((total,)),
            pltpu.SemaphoreType.DMA((total,)),
            pltpu.SemaphoreType.DMA((number,)),
        ],
        compiler_params=pltpu.CompilerParams(collective_id=cid, has_side_effects=True),
    )(*[item[2] for item in items])


def pack(vector):
    flat = vector.reshape(-1)
    flat = flat if flat.dtype == jnp.int32 else flat.astype(f32)
    extra = -flat.shape[0] % 1024
    return jnp.pad(flat, (0, extra)).reshape(-1, 128)


def unpack(packed, lead, shape):
    count = 1
    for size in shape:
        count *= size
    return packed.reshape(lead, -1)[:, :count].reshape((lead,) + tuple(shape))


def rms_norm(values, gain_vec):
    factor = lax.rsqrt(jnp.mean(values * values, axis=-1, keepdims=True) + eps)
    return values * factor * gain_vec


def rotary_tables(positions, head_dim):
    half_dim = head_dim // 2
    inverse_freq = theta ** (-2.0 * jnp.arange(half_dim, dtype=f32) / head_dim)
    angles = positions[:, None] * inverse_freq[None, :]
    cos_tab = jnp.concatenate([jnp.cos(angles), jnp.cos(angles)], axis=-1)
    sin_tab = jnp.concatenate([jnp.sin(angles), jnp.sin(angles)], axis=-1)
    return (cos_tab, sin_tab)


def rotate_half(tensor):
    half_dim = tensor.shape[-1] // 2
    return jnp.concatenate([-tensor[..., half_dim:], tensor[..., :half_dim]], axis=-1)


def qk_prepare(raw, gain_vec, cos_tab, sin_tab):
    normed = rms_norm(raw, gain_vec)
    return normed * cos_tab + rotate_half(normed) * sin_tab


NT = (((1,), (1,)), ((), ()))
TN = (((0,), (0,)), ((), ()))


def dot(left, right, dims=(((1,), (0,)), ((), ()))):
    return lax.dot_general(left, right, dims, preferred_element_type=f32)


def attend_kernel(scale, q_ref, kv_ref, dq_ref, dk_ref, out_ref, norm_ref):
    head = q_ref.shape[1]
    keys, values = kv_ref[:, :head], kv_ref[:, head:]
    scores = dot(q_ref[...], keys, NT) * scale
    keep = dq_ref[...] == dk_ref[...]
    scores = jnp.where(keep, scores, negative)
    top = jnp.max(scores, axis=1, keepdims=True)
    terms = jnp.exp(scores - top)
    total = jnp.sum(terms, axis=1, keepdims=True)
    probs = (terms * (1.0 / total)).astype(bf16)
    out_ref[...] = dot(probs, values).astype(bf16)
    norm_ref[...] = top + jnp.log(total)


def attend(q_rot, kv, docs_q, docs_k, scale):
    rows, head = q_rot.shape
    keys = kv.shape[0]
    tile = 256
    return pl.pallas_call(
        functools.partial(attend_kernel, scale),
        grid=(rows // tile,),
        out_shape=[
            jax.ShapeDtypeStruct((rows, head), bf16),
            jax.ShapeDtypeStruct((rows, 1), f32),
        ],
        in_specs=[
            pl.BlockSpec((tile, head), lambda i: (i, 0)),
            pl.BlockSpec((keys, 2 * head), lambda i: (0, 0)),
            pl.BlockSpec((tile, 1), lambda i: (i, 0)),
            pl.BlockSpec((1, keys), lambda i: (0, 0)),
        ],
        out_specs=[
            pl.BlockSpec((tile, head), lambda i: (i, 0)),
            pl.BlockSpec((tile, 1), lambda i: (i, 0)),
        ],
    )(q_rot, kv, docs_q[:, None], docs_k[None, :])


def attend_back_kernel(
    scale, q_ref, kv_ref, dq_ref, dk_ref, norm_ref, cot_ref, qgrad_ref, kvgrad_ref
):
    head = q_ref.shape[1]
    queries, cot = q_ref[...], cot_ref[...]
    keys, values = kv_ref[:, :head], kv_ref[:, head:]
    scores = dot(queries, keys, NT) * scale
    keep = dq_ref[...] == dk_ref[...]
    probs = jnp.where(keep, jnp.exp(scores - norm_ref[...]), 0.0)
    d_soft = dot(cot, values, NT)
    delta = jnp.sum(probs * d_soft, axis=1, keepdims=True)
    d_scores = (probs * (d_soft - delta)).astype(bf16)
    qgrad_ref[...] = dot(d_scores, keys) * scale

    @pl.when(pl.program_id(0) == 0)
    def _():
        kvgrad_ref[...] = jnp.zeros_like(kvgrad_ref)

    kvgrad_ref[:, :head] += dot(d_scores, queries, TN) * scale
    kvgrad_ref[:, head:] += dot(probs.astype(bf16), cot, TN)


def attend_back(q_rot, kv, docs_q, docs_k, norm, cot, scale):
    rows, head = q_rot.shape
    keys = kv.shape[0]
    tile = 256 if keys <= 4096 else 128
    return pl.pallas_call(
        functools.partial(attend_back_kernel, scale),
        grid=(rows // tile,),
        out_shape=[
            jax.ShapeDtypeStruct((rows, head), f32),
            jax.ShapeDtypeStruct((keys, 2 * head), f32),
        ],
        in_specs=[
            pl.BlockSpec((tile, head), lambda i: (i, 0)),
            pl.BlockSpec((keys, 2 * head), lambda i: (0, 0)),
            pl.BlockSpec((tile, 1), lambda i: (i, 0)),
            pl.BlockSpec((1, keys), lambda i: (0, 0)),
            pl.BlockSpec((tile, 1), lambda i: (i, 0)),
            pl.BlockSpec((tile, head), lambda i: (i, 0)),
        ],
        out_specs=[
            pl.BlockSpec((tile, head), lambda i: (i, 0)),
            pl.BlockSpec((keys, 2 * head), lambda i: (0, 0)),
        ],
    )(q_rot, kv, docs_q[:, None], docs_k[None, :], norm, cot)


def on_device(
    sizes,
    tokens_in,
    doc_ids,
    expert_ids,
    attn_gain,
    q_gain,
    k_gain,
    w_query,
    w_key,
    w_value,
    w_output,
    ffn_gain,
    w_router,
    w_gate,
    w_up,
    w_down,
    cotangent,
):
    nb, na = sizes["b"], sizes["a"]
    nt = sizes["y"] * sizes["c"]
    tok, model = tokens_in.shape
    col = nb * tok
    part = model // nb
    sub = part // na
    head = q_gain.shape[0]
    width = w_query.shape[1]
    heads = width // head
    experts, ff = w_gate.shape[1], w_gate.shape[2]
    top = expert_ids.shape[1]
    quarter = tok // nt
    scale = head**-0.5
    comm = functools.partial(exchange, sizes)
    a_me = lax.axis_index("a")
    t_me = lax.axis_index("y") * sizes["c"] + lax.axis_index("c")

    def blocks(array):
        return array.reshape(tok, nb, part).transpose(1, 0, 2)

    def share(array):
        rest = array.shape[1]
        array = array.reshape(nb, nt, quarter, rest).transpose(1, 0, 2, 3)
        return array.reshape(nt, nb * quarter, rest)

    def unshare(array):
        rest = array.shape[-1]
        array = array.reshape(nt, nb, quarter, rest).transpose(1, 0, 2, 3)
        return array.reshape(col, rest)

    def own(array):
        rest = array.shape[1]
        array = array.reshape(nb, nt, quarter, rest)
        return lax.dynamic_index_in_dim(array, t_me, 1, keepdims=False).reshape(nb * quarter, rest)

    tokens = tokens_in.astype(f32)
    r_own = lax.rsqrt(jnp.mean(tokens * tokens, axis=-1) + eps)
    got = comm(
        1,
        [
            ("each", ("b",), blocks(tokens_in), "v"),
            ("all", ("a",), w_query, "v"),
            ("all", ("a",), w_key, "v"),
            ("all", ("a",), w_value, "v"),
            ("all", ("b",), pack(r_own), "v"),
            ("all", ("a",), pack(attn_gain), "v"),
            ("all", ("b",), pack(expert_ids), "v"),
            ("all", ("b", "a"), pack(doc_ids), "v"),
        ],
    )
    xc = got[0].reshape(col, part)
    wq, wk, wv = [w.reshape(part, heads, head) for w in got[1:4]]
    r_in = unpack(got[4], nb, (tok,)).reshape(col, 1)
    gain_in = unpack(got[5], na, (sub,)).reshape(1, part)
    chosen = unpack(got[6], nb, (tok, top)).reshape(col, top)
    docs = unpack(got[7], nb * na, (tok,)).reshape(nb, na, tok)
    docs_k = docs.transpose(1, 0, 2).reshape(-1)
    docs_q = lax.dynamic_index_in_dim(docs, a_me, 1, keepdims=False).reshape(col)

    normed_in = (xc.astype(f32) * r_in * gain_in).astype(bf16)
    w_qkv = jnp.stack([wq, wk, wv], axis=2)
    flat_qkv = w_qkv.reshape(part, heads * 3 * head)
    qkv_part = dot(normed_in, flat_qkv).astype(bf16)
    qkv_part = qkv_part.reshape(col, heads, 3 * head).transpose(1, 0, 2)

    got = comm(
        2,
        [
            ("each", ("b",), qkv_part, "v"),
            ("all", ("a",), w_output, "h"),
            ("all", ("a",), w_down, "h"),
            ("all", ("a",), w_gate, "h"),
            ("all", ("a",), w_up, "h"),
            ("all", ("a",), pack(ffn_gain), "v"),
            ("all", ("a",), pack(w_router), "v"),
        ],
    )
    raw = jnp.sum(got[0].astype(f32), axis=0)
    wo = got[1].reshape(part, width)
    wd, wg, wu = [w.reshape(part, experts * ff) for w in got[2:5]]
    gain_mid = unpack(got[5], na, (sub,)).reshape(1, part)
    router = unpack(got[6], na, (sub, experts)).reshape(part, experts).astype(bf16)

    q_raw, k_raw, v_raw = raw[:, :head], raw[:, head : 2 * head], raw[:, 2 * head :]
    index = jnp.arange(col, dtype=jnp.int32)
    positions = ((index // tok * na + a_me) * tok + index % tok).astype(f32)
    cos_tab, sin_tab = rotary_tables(positions, head)
    q_rot, q_back = jax.vjp(
        lambda u, g: qk_prepare(u, g, cos_tab, sin_tab), q_raw, q_gain.astype(f32)
    )
    k_rot, k_back = jax.vjp(
        lambda u, g: qk_prepare(u, g, cos_tab, sin_tab), k_raw, k_gain.astype(f32)
    )
    q_rot = q_rot.astype(bf16)
    kv_own = jnp.concatenate([k_rot.astype(bf16), v_raw.astype(bf16)], axis=1)

    got = comm(
        3,
        [("all", ("a",), kv_own, "v"), ("each", ("b",), blocks(cotangent), "v")],
    )
    kv = got[0].reshape(na * col, 2 * head)
    cotc = got[1].reshape(col, part)
    heads_own, norm = attend(q_rot, kv, docs_q, docs_k, scale)

    expert_range = jnp.arange(experts, dtype=jnp.int32)

    def select(array):
        array = array.reshape(col, experts, -1)
        picked = [
            jnp.sum(
                jnp.where((chosen[:, k : k + 1] == expert_range)[:, :, None], array, 0), axis=1
            )
            for k in range(top)
        ]
        return jnp.stack(picked, axis=1)

    def spread(array):
        total = 0
        for k in range(top):
            mask = (chosen[:, k : k + 1] == expert_range)[:, :, None]
            total = total + jnp.where(mask, array[:, k, None, :], jnp.zeros((), array.dtype))
        return total.reshape(col, -1)

    cot_down = select(dot(cotc, wd).astype(bf16)).reshape(nb, tok, top * ff)
    got = comm(
        4,
        [("all", ("b",), heads_own, "v"), ("each", ("b",), cot_down, "v")],
    )
    heads_out = got[0].transpose(1, 0, 2).reshape(col, width)
    down_cot = jnp.sum(got[1].astype(f32), axis=0).reshape(tok, top, ff)
    attn_part = dot(heads_out, wo, NT).astype(bf16)
    got = comm(5, [("each", TP, share(attn_part), "v")])
    hidden = own(xc).astype(f32) + jnp.sum(got[0].astype(f32), axis=0)
    scaled = (hidden * gain_mid).astype(bf16)
    squares = jnp.sum(hidden * hidden, axis=1)
    logit_part = dot(scaled, router)
    small = jnp.concatenate(
        [logit_part.T, squares[None], jnp.zeros((15 - experts, squares.shape[0]), f32)], axis=0
    )
    got = comm(6, [("all", TP, scaled, "v"), ("all", TP, small, "v")])
    scaled_all = unshare(got[0])
    small_all = (
        got[1].reshape(nt, 16, nb, quarter).transpose(2, 1, 0, 3).reshape(nb, 16, nt * quarter)
    )
    gate_part = select(dot(scaled_all, wg).astype(bf16))
    up_part = select(dot(scaled_all, wu).astype(bf16))
    pre_part = jnp.concatenate([gate_part, up_part], axis=2).reshape(nb, tok, top * 2 * ff)
    got = comm(7, [("each", ("b",), pre_part, "v"), ("each", ("b",), small_all, "v")])
    pre = jnp.sum(got[0].astype(f32), axis=0).reshape(tok, top, 2 * ff)
    small = jnp.sum(got[1], axis=0)
    r_mid = lax.rsqrt(small[experts] / model + eps)
    logits = small[:experts].T * r_mid[:, None]
    router_probs = jax.nn.softmax(logits, axis=-1)
    picked = (expert_ids[:, :, None] == expert_range).astype(f32)
    combine = jnp.sum(router_probs[:, None, :] * picked, axis=-1)
    pre = pre * r_mid[:, None, None]
    gate_pre, up_pre = pre[:, :, :ff], pre[:, :, ff:]
    sig = 1.0 / (1.0 + jnp.exp(-gate_pre))
    silu = gate_pre * sig
    act = silu * up_pre
    d_act = combine[:, :, None] * down_cot
    d_gate = d_act * up_pre * (sig * (1.0 + gate_pre * (1.0 - sig)))
    d_up = d_act * silu
    pay = jnp.stack(
        [
            (combine[:, :, None] * act).astype(bf16),
            (d_gate * r_mid[:, None, None]).astype(bf16),
            (d_up * r_mid[:, None, None]).astype(bf16),
        ],
        axis=1,
    ).reshape(tok, 3 * top * ff)
    d_combine_part = jnp.sum(act * down_cot, axis=2)
    inner_part = jnp.sum(d_gate * gate_pre + d_up * up_pre, axis=(1, 2))
    small = jnp.concatenate(
        [d_combine_part.T, inner_part[None], jnp.zeros((7 - top, tok), f32)], axis=0
    )
    got = comm(8, [("all", ("b",), pay, "v"), ("all", TP, small, "v")])
    pay_all = got[0].reshape(col, 3, top, ff)
    small = jnp.sum(got[1], axis=0)
    d_combine, inner = small[:top].T, small[top]
    d_probs = jnp.sum(d_combine[:, :, None] * picked, axis=1)
    d_logits = router_probs * (d_probs - jnp.sum(router_probs * d_probs, axis=-1, keepdims=True))
    inner = inner + jnp.sum(d_logits * logits, axis=1)
    back = r_mid * r_mid * inner / model
    small = jnp.concatenate(
        [(d_logits * r_mid[:, None]).T, back[None], jnp.zeros((15 - experts, tok), f32)], axis=0
    )
    wide_act, wide_gate, wide_up = [spread(pay_all[:, i]) for i in range(3)]
    mid_part = (dot(wide_gate, wg, NT) + dot(wide_up, wu, NT)).astype(bf16)
    mix_part = dot(wide_act, wd, NT).astype(bf16)
    got = comm(
        9,
        [
            ("each", TP, share(mid_part), "v"),
            ("each", TP, share(mix_part), "v"),
            ("all", ("b",), small, "v"),
        ],
    )
    small = got[2]
    small_all = small.transpose(0, 2, 1).reshape(col, 16)
    small_own = own(small_all)
    dl_all = small_all[:, :experts].astype(bf16)
    mid = jnp.sum(got[0].astype(f32), axis=0) + dot(
        small_own[:, :experts].astype(bf16), router, NT
    )
    d_hidden = own(cotc).astype(f32) + gain_mid * mid - hidden * small_own[:, experts : experts + 1]
    ffn_gain_part = jnp.sum(mid * hidden, axis=0)
    d_attn = d_hidden.astype(bf16)
    out_own = (hidden + jnp.sum(got[1].astype(f32), axis=0)).astype(bf16)
    router_part = dot(scaled_all, dl_all, TN)
    got = comm(
        10,
        [("all", TP, d_attn, "v"), ("each", ("b",), out_own.reshape(nb, quarter, part), "v")],
    )
    d_attn_all = unshare(got[0])
    out_rows = got[1].transpose(1, 0, 2).reshape(quarter, model)
    d_heads_part = dot(d_attn_all, wo).astype(bf16).reshape(col, heads, head).transpose(1, 0, 2)
    output_part = dot(d_attn_all, heads_out, TN).astype(bf16)
    got = comm(
        11,
        [
            ("each", ("b",), d_heads_part, "v"),
            ("all", TP, out_rows, "v"),
            ("all", ("a",) + TP, pack(ffn_gain_part), "v"),
        ],
    )
    d_heads = jnp.sum(got[0].astype(f32), axis=0).astype(bf16)
    block_out = got[1].reshape(tok, model)
    ffn_gain_sum = jnp.sum(unpack(got[2], na * nt, (part,)), axis=0).reshape(na, sub)
    grad_ffn_gain = lax.dynamic_index_in_dim(ffn_gain_sum, a_me, 0, keepdims=False)

    d_q_rot, d_kv = attend_back(q_rot, kv, docs_q, docs_k, norm, d_heads, scale)
    gate_grad = dot(scaled_all, wide_gate, TN).astype(bf16).reshape(na, sub, experts * ff)
    up_grad = dot(scaled_all, wide_up, TN).astype(bf16).reshape(na, sub, experts * ff)
    down_grad = dot(cotc, wide_act, TN).astype(bf16).reshape(na, sub, experts * ff)
    got = comm(12, [("each", ("a",), d_kv.astype(bf16).reshape(na, col, 2 * head), "v")])
    d_kv = jnp.sum(got[0].astype(f32), axis=0)
    d_q_raw, q_gain_part = q_back(d_q_rot)
    d_k_raw, k_gain_part = k_back(d_kv[:, :head])
    d_v_raw = d_kv[:, head:]
    inner_part = jnp.sum(d_q_raw * q_raw + d_k_raw * k_raw + d_v_raw * v_raw, axis=1)
    d_qkv = jnp.concatenate([d_q_raw, d_k_raw, d_v_raw], axis=1).astype(bf16)
    got = comm(
        13,
        [
            ("all", ("b",), d_qkv, "v"),
            ("each", ("a",), gate_grad, "h"),
            ("each", ("a",), up_grad, "h"),
            ("each", ("a",), down_grad, "h"),
            ("all", ("b",), pack(inner_part), "v"),
            ("all", ("b",), pack(jnp.concatenate([q_gain_part, k_gain_part])), "v"),
        ],
    )
    d_qkv_all = got[0].transpose(1, 0, 2).reshape(col, heads * 3 * head)
    grad_gate, grad_up, grad_down = [
        jnp.sum(g.astype(f32), axis=0).reshape(sub, experts, ff) for g in got[1:4]
    ]
    inner_part = jnp.sum(unpack(got[4], nb, (col,)), axis=0)
    head_gain_part = jnp.sum(got[5], axis=0)
    in_part = dot(d_qkv_all, flat_qkv, NT).astype(bf16)
    qkv_grad = dot(normed_in, d_qkv_all, TN).astype(bf16).reshape(na, sub, heads * 3 * head)
    inner_share = share(inner_part[:, None]).reshape(nt, -1)
    inner_share = jnp.pad(inner_share, ((0, 0), (0, -inner_share.shape[1] % 1024)))
    got = comm(
        14,
        [
            ("each", TP, share(in_part), "v"),
            ("each", TP, inner_share.reshape(nt, -1, 128), "v"),
            ("each", ("a",), qkv_grad, "v"),
            ("each", ("a",), output_part.reshape(na, sub, width), "v"),
            ("each", ("a",), jax.vmap(pack)(router_part.reshape(na, sub * experts)), "v"),
            ("all", ("a",) + TP, head_gain_part, "v"),
        ],
    )
    d_in = jnp.sum(got[0].astype(f32), axis=0)
    inner = jnp.sum(got[1].reshape(nt, -1), axis=0)[: nb * quarter, None]
    qkv_grad = jnp.sum(got[2].astype(f32), axis=0).reshape(sub, heads, 3, head)
    grad_query, grad_key, grad_value = [qkv_grad[:, :, i].reshape(sub, width) for i in range(3)]
    grad_output = jnp.sum(got[3].astype(f32), axis=0)
    grad_router = jnp.sum(unpack(got[4], na, (sub, experts)), axis=0)
    head_gains = jnp.sum(unpack(got[5], na * nt, (2, head)), axis=0)
    x_own = own(xc).astype(f32)
    r_q = own(r_in)
    grad_in = d_hidden + r_q * gain_in * d_in - x_own * (r_q * r_q * inner / model)
    attn_gain_part = jnp.sum(d_in * x_own * r_q, axis=0)
    got = comm(
        15,
        [
            ("each", ("b",), grad_in.astype(bf16).reshape(nb, quarter, part), "v"),
            ("all", ("a",) + TP, pack(attn_gain_part), "v"),
        ],
    )
    in_rows = got[0].transpose(1, 0, 2).reshape(quarter, model)
    attn_gain_sum = jnp.sum(unpack(got[1], na * nt, (part,)), axis=0).reshape(na, sub)
    grad_attn_gain = lax.dynamic_index_in_dim(attn_gain_sum, a_me, 0, keepdims=False)
    got = comm(16, [("all", TP, in_rows, "v")])
    grad_in = got[0].reshape(tok, model).astype(f32)
    return (
        block_out,
        grad_in,
        grad_attn_gain,
        head_gains[0],
        head_gains[1],
        grad_query,
        grad_key,
        grad_value,
        grad_output,
        grad_ffn_gain,
        grad_router,
        grad_gate,
        grad_up,
        grad_down,
    )


def solution(mesh):
    cp, tp = mesh.shape["cp"], mesh.shape["tp"]
    sizes = {"b": 4, "a": cp // 4, "y": 2, "c": tp // 2}
    split = Mesh(mesh.devices.reshape([sizes[axis] for axis in AXES]), AXES)
    cp, tp = ("b", "a"), ("y", "c")
    return jax.shard_map(
        functools.partial(on_device, sizes),
        mesh=split,
        in_specs=(
            P(cp, None),
            P(cp),
            P(cp, None),
            P(cp),
            P(),
            P(),
            P(cp, tp),
            P(cp, tp),
            P(cp, tp),
            P(cp, tp),
            P(cp),
            P(cp, None),
            P(cp, None, tp),
            P(cp, None, tp),
            P(cp, None, tp),
            P(cp, None),
        ),
        out_specs=(
            P(cp, None),
            P(cp, None),
            P(cp),
            P(),
            P(),
            P(cp, tp),
            P(cp, tp),
            P(cp, tp),
            P(cp, tp),
            P(cp),
            P(cp, None),
            P(cp, None, tp),
            P(cp, None, tp),
            P(cp, None, tp),
        ),
        check_vma=False,
    )
```

```python
import functools
import types

import jax
import jax.numpy as jnp
import numpy as np
from jax import lax
from jax.experimental import pallas as pl
from jax.experimental.pallas import tpu as pltpu
from jax.sharding import Mesh
from jax.sharding import PartitionSpec as P

eps = 1e-05
theta = 50000.0
negative = -1e30
AXES = ("b", "a", "y", "c")
MESH = pl.DeviceIdType.MESH
bf16 = jnp.bfloat16
f32 = jnp.float32


NT = (((1,), (1,)), ((), ()))
TN = (((0,), (0,)), ((), ()))


def dot(left, right, dims=(((1,), (0,)), ((), ()))):
    return lax.dot_general(left, right, dims, preferred_element_type=f32)


class Net:
    def __init__(self, sizes, send, recv):
        self.sizes, self.send, self.recv, self.used = sizes, send, recv, 0
        self.me = {axis: lax.axis_index(axis) for axis in AXES}

    def near(self, **offs):
        return {axis: lax.rem(self.me[axis] + off, self.sizes[axis]) for axis, off in offs.items()}

    def copy(self, source, target, place):
        slot = self.used
        self.used += 1
        return pltpu.make_async_remote_copy(
            src_ref=source,
            dst_ref=target,
            send_sem=self.send.at[slot],
            recv_sem=self.recv.at[slot],
            device_id=place,
            device_id_type=MESH,
        )

    def greet(self, places):
        barrier = pltpu.get_barrier_semaphore()
        for place in places:
            pl.semaphore_signal(barrier, inc=1, device_id=place, device_id_type=MESH)
        pl.semaphore_wait(barrier, len(places))

    def pick(self, *values):
        result = values[-1]
        for i in range(len(values) - 2, -1, -1):
            result = jnp.where(self.me["b"] == i, values[i], result)
        return result

    def reduce(self, *args):
        return Reduce(self, *args)

    def spread(self, *blocks):
        return Spread(self, blocks)


class Reduce:
    def __init__(self, net, parts, got, make=None):
        self.net, self.parts, self.got = net, parts, got
        self.b = b = net.me["b"]
        self.base = net.used
        net.used += 4
        self.order = [3 - b, net.pick(2, 0, 3, 1), net.pick(1, 3, 0, 2)]
        for k in range(2):
            if make is not None:
                make(self.order[k])
            self.hop(self.order[k]).start()
        if make is not None:
            make(self.order[2])

    def hop(self, d):
        net, b = self.net, self.b
        far = ((b == 0) & (d == 3)) | ((b == 3) & (d == 0))
        beside = jnp.where(b == 0, 1, 2)
        target, slot = jnp.where(far, beside, d), jnp.where(far, beside, b)
        return pltpu.make_async_remote_copy(
            src_ref=self.parts.at[d],
            dst_ref=self.got.at[slot],
            send_sem=net.send.at[self.base + d],
            recv_sem=net.recv.at[self.base + slot],
            device_id={"b": target},
            device_id_type=MESH,
        )

    def came(self, i):
        net = self.net
        return pltpu.make_async_remote_copy(
            src_ref=self.got.at[i],
            dst_ref=self.got.at[i],
            send_sem=net.send.at[self.base + i],
            recv_sem=net.recv.at[self.base + i],
            device_id=net.near(b=1),
            device_id_type=MESH,
        )

    def inner(self):
        b, d = self.b, self.order[2]

        @pl.when((b == 1) | (b == 2))
        def _():
            self.came(b).wait_recv()
            rows = self.parts.shape[1]
            step = 256 if rows % 256 == 0 else rows

            @pl.loop(0, rows // step)
            def _(i):
                sl = pl.ds(pl.multiple_of(i * step, step), step)
                total = self.parts[d, sl, :].astype(f32) + self.got[b, sl, :].astype(f32)
                self.parts[d, sl, :] = total.astype(bf16)

        self.hop(d).start()

    def wait(self):
        for i in range(4):

            @pl.when((self.b != i) & (jnp.abs(self.b - i) <= 2))
            def _():
                self.came(i).wait_recv()

    def total(self, *index):
        b = self.b
        value = self.parts[(b,) + index].astype(f32)
        for i in range(4):
            valid = (b != i) & (jnp.abs(b - i) <= 2)
            value = value + jnp.where(valid, self.got[(i,) + index].astype(f32), 0.0)
        return value

    def finish(self):
        for d in range(4):

            @pl.when(self.b != d)
            def _():
                self.hop(d).wait_send()


class Spread:
    def __init__(self, net, blocks):
        self.net, self.blocks = net, blocks
        self.b = b = net.me["b"]
        self.base = net.used
        net.used += 4 * len(blocks)
        self.targets = [net.pick(2, 3, 0, 1), net.pick(1, 0, 3, 2), net.pick(2, 2, 1, 1)]
        self.order = [net.pick(1, 3, 0, 2), net.pick(2, 0, 3, 1), net.pick(3, 2, 1, 0)]
        self.inner = (b == 1) | (b == 2)
        for k, target in enumerate(self.targets):
            if k < 2:
                for j in range(len(blocks)):
                    self.hop(b, target, target, j).start()
            else:

                @pl.when(self.inner)
                def _():
                    for j in range(len(blocks)):
                        self.hop(b, target, target, j).start()

    def hop(self, i, target, slot, j):
        net, count = self.net, len(self.blocks)
        return pltpu.make_async_remote_copy(
            src_ref=self.blocks[j](i),
            dst_ref=self.blocks[j](i),
            send_sem=net.send.at[self.base + slot * count + j],
            recv_sem=net.recv.at[self.base + i * count + j],
            device_id={"b": target},
            device_id_type=MESH,
        )

    def take(self, i):
        b = self.b
        onward = ((b == 1) & (i == 3)) | ((b == 2) & (i == 0))
        for j in range(len(self.blocks)):
            self.hop(i, self.net.near(b=1)["b"], b, j).wait_recv()

            @pl.when(onward)
            def _():
                self.hop(i, jnp.where(b == 1, 0, 3), b, j).start()

    def take_all(self):
        for i in self.order:
            self.take(i)

    def finish(self):
        b = self.b
        for k, target in enumerate(self.targets):
            for j in range(len(self.blocks)):
                if k < 2:
                    self.hop(b, target, target, j).wait_send()
                else:

                    @pl.when(self.inner)
                    def _():
                        self.hop(b, target, target, j).wait_send()
                        self.hop(b, jnp.where(b == 1, 0, 3), b, j).wait_send()


def rope(values, cos_tab, sin_tab):
    return values * cos_tab + pltpu.roll(values, values.shape[1] // 2, 1) * sin_tab


def head_norm(values):
    return lax.rsqrt(jnp.mean(values * values, axis=1, keepdims=True) + eps)


def unrope(grad, raw, gain, cos_tab, sin_tab):
    factor = head_norm(raw)
    normed = raw * factor
    turned = grad * cos_tab + pltpu.roll(grad * sin_tab, grad.shape[1] // 2, 1)
    gain_part = jnp.sum(turned * normed, axis=0, keepdims=True)
    inner = turned * gain
    slope = jnp.mean(raw * inner, axis=1, keepdims=True)
    return factor * inner - raw * (factor * factor * factor * slope), gain_part


class TwoLevel:
    def __init__(self, net, acc, sendc, recvc, sendy, recvy, used):
        self.net, self.acc = net, acc
        self.sendc, self.recvc, self.sendy, self.recvy = sendc, recvc, sendy, recvy
        self.used = used
        self.base = net.used
        net.used += 16
        self.part = acc.shape[2]
        self.half = acc.shape[1]

    def lane(self, j):
        return slice(j * self.part, (j + 1) * self.part)

    def hop(self, i, j, level):
        net = self.net
        source, target = ((self.sendc, self.recvc), (self.sendy, self.recvy))[level]
        slot = self.base + 8 * level + 2 * i + j
        lane = pl.ds(j * self.part, self.part)
        return pltpu.make_async_remote_copy(
            src_ref=source.at[i, :, lane],
            dst_ref=target.at[i, :, lane],
            send_sem=net.send.at[slot],
            recv_sem=net.recv.at[slot],
            device_id=net.near(c=1) if level == 0 else net.near(y=1),
            device_id_type=MESH,
        )

    def put(self, i, j, term, k):
        first = self.net.me["c"] == 0
        low, high = term[: self.half], term[self.half :]
        self.acc[k] = jnp.where(first, low, high)
        self.sendc[i, :, self.lane(j)] = jnp.where(first, high, low).astype(bf16)
        self.hop(i, j, 0).start()

    def onward(self, i, j, k):
        self.hop(i, j, 0).wait_recv()
        total = self.acc[k] + self.recvc[i, :, self.lane(j)].astype(f32)
        self.sendy[i, :, self.lane(j)] = total.astype(bf16)
        self.hop(i, j, 1).start()

    def total(self, i, j):
        self.hop(i, j, 1).wait_recv()
        lane = self.lane(j)
        return self.sendy[i, :, lane].astype(f32) + self.recvy[i, :, lane].astype(f32)

    def finish(self):
        for i in range(4):
            for j in range(self.used):
                self.hop(i, j, 0).wait_send()
                self.hop(i, j, 1).wait_send()


def transpose_columns(columns, rows):
    lane = lax.broadcasted_iota(jnp.int32, (rows, 128), 1)
    table = jnp.zeros((rows, 128), f32)
    for k, column in enumerate(columns):
        table = jnp.where(lane == k, column, table)
    return jnp.transpose(table)[:8, :]


INS = (
    "tok", "cot", "wq_in", "wk_in", "wv_in", "wo_in", "wg_in", "wu_in", "wd_in", "ids_in",
    "docs_in", "router_in", "gain_in_a", "gain_in_f", "gain_q", "gain_k", "speed_in",
)
OUTS = (
    "out_rows", "in_rows", "gate_own", "up_own", "down_own", "gate_in", "up_in", "down_in",
    "proj_out", "tail",
)
WORK = (
    "xc", "cotc", "rows_all", "rows_own", "cols_own", "cols_all", "cols_sum", "wqkv", "wo",
    "wg", "wu", "wd", "stage", "hn", "raw", "q_rot", "kv", "stat", "ho", "cos_tab", "sin_tab",
    "pkv", "gkv", "pq", "gq", "pcd", "gcd", "acc", "sendc", "recvc", "sendy", "recvy", "hidden", "scaled",
    "small", "small_in", "pay", "wide", "pair", "late_small", "extra_own", "extra_in", "d_attn",
    "out_half", "block_out", "head_acc", "dkv_acc", "dkv_send", "dkv_in", "gsend", "gin_w",
    "gout", "gout_in", "gin", "s4", "gain_acc", "tail_all", "gains", "ids", "docs", "proj",
    "send", "recv", "local",
)


def layer_kernel(sizes, dims, *refs):
    r = types.SimpleNamespace(**dict(zip(INS + OUTS + WORK, refs)))
    nb, na, head, heads, experts, ff, top = dims
    net = Net(sizes, r.send, r.recv)
    me = net.me
    b, a, y, c = me["b"], me["a"], me["y"], me["c"]
    tok, part = r.xc.shape[1], r.xc.shape[2]
    half, col, model, width, sub = tok // 2, nb * tok, nb * part, heads * head, part // na
    scale = head**-0.5
    mine = pl.ds(pl.multiple_of(c * half, half), half)
    own_lane = pl.ds(pl.multiple_of(b * part, part), part)
    head_lane = pl.ds(pl.multiple_of(b * head, head), head)
    core, across = net.near(c=1), net.near(y=1)
    b_peers = [net.near(b=k) for k in range(1, nb)]
    a_peers = [net.near(a=k) for k in range(1, na)]
    ab_peers = [net.near(b=j, a=k) for j in range(nb) for k in range(na) if j or k]
    group = [
        net.near(b=i, y=j, c=k)
        for i in range(nb) for j in range(2) for k in range(2) if i or j or k
    ]
    tp_peers = [net.near(y=j, c=k) for j in range(2) for k in range(2) if j or k]
    sent = []
    local_used = [0]

    def rows_of(i):
        return pl.ds(pl.multiple_of(i * tok, tok), tok)

    def lane_of(place):
        return pl.ds(pl.multiple_of(place * part, part), part)

    def move(source, target):
        copy = pltpu.make_async_copy(source, target, r.local.at[local_used[0]])
        local_used[0] += 1
        copy.start()
        return copy

    def ship(source, target, place):
        copy = net.copy(source, target, place)
        copy.start()
        sent.append(copy)
        return copy

    def arrive(copies):
        for copy in copies:
            copy.wait_recv()

    def drain(copies):
        for copy in copies:
            copy.wait_send()
            sent[:] = [other for other in sent if other is not copy]

    tok_here = move(r.tok, r.gin)
    w_here = [move(w, r.wqkv.at[j, a]) for j, w in ((1, r.wk_in), (2, r.wv_in), (0, r.wq_in))]
    stage_copy = move(r.wd_in, r.stage)
    late_here = [move(r.wo_in, r.wo.at[a]), move(r.cot.at[:, own_lane], r.cotc.at[b])]
    net.greet(group + [net.near(b=j, a=k) for j in range(nb) for k in range(1, na)])

    r.cols_own[...] = jnp.zeros_like(r.cols_own)
    r.cols_own[0:experts, :] = r.router_in[...].astype(f32)
    r.cols_own[experts : experts + 1, :] = r.gain_in_a[...].astype(f32)
    r.cols_own[experts + 1 : experts + 2, :] = r.gain_in_f[...].astype(f32)
    r.gains[0:1, :] = r.gain_q[...].astype(f32)
    r.gains[1:2, :] = r.gain_k[...].astype(f32)
    r.gains[2:3, :] = r.speed_in[...]
    r.rows_own[...] = jnp.zeros_like(r.rows_own)
    r.rows_own[1 : 1 + top, :] = r.ids_in[...].astype(f32)
    r.rows_own[3:4, :] = r.docs_in[...].astype(f32)

    exchange = [net.pick(2, 3, 0, 1), net.pick(3, 2, 1, 0), net.pick(1, 0, 3, 2)]

    def to_quarters(source, target):
        return [
            ship(source.at[mine, lane_of(d)], target.at[b, mine, :], {"b": d}) for d in exchange
        ]

    def over_a(source, target):
        return [ship(source, target.at[a], place) for place in a_peers]

    def to_core(copies, target):
        more = []
        for source_b, copy in zip(exchange, copies):
            copy.wait_recv()
            block = target.at[source_b, mine, :]
            more.append(ship(block, block, core))
        return more

    x_copies = to_quarters(r.tok, r.xc)
    cols_copies = over_a(r.cols_own, r.cols_all)
    r.cols_all[a] = r.cols_own[...]
    kv_weights = over_a(r.wk_in, r.wqkv.at[1]) + over_a(r.wv_in, r.wqkv.at[2])
    q_weights = over_a(r.wq_in, r.wqkv.at[0])
    tok_here.wait()
    square_columns = []
    for s in range(tok // 64):
        piece = r.gin[s * 64 : (s + 1) * 64, :].astype(f32)
        square_columns.append(jnp.sum(piece * piece, axis=1, keepdims=True))
    squares = transpose_columns([jnp.concatenate(square_columns, axis=0)], tok)[0:1, :]
    which8 = lax.broadcasted_iota(jnp.int32, (8, tok), 0)
    r.rows_own[0:1, :] = lax.rsqrt(squares / model + eps)
    rows_copies = [ship(r.rows_own, r.rows_all.at[a, b], place) for place in ab_peers]
    r.rows_all[a, b] = r.rows_own[...]
    r.xc[b] = r.gin[:, own_lane]
    cot_copies = to_quarters(r.cot, r.cotc)
    wo_copies = over_a(r.wo_in, r.wo)

    def relayout(target):
        step = 32

        @pl.loop(0, sub // step)
        def _(n):
            rows = pl.ds(pl.multiple_of(n * step, step), step)
            turned = jnp.swapaxes(r.stage[rows].astype(f32), 0, 1)
            for e in range(experts):
                target[a, rows, e * ff : (e + 1) * ff] = turned[e].astype(bf16)

    stage_copy.wait()
    relayout(r.wd)
    wd_copies = over_a(r.wd.at[a], r.wd)
    stage_copy = move(r.wg_in, r.stage)

    lane_index = lax.broadcasted_iota(jnp.int32, (tok, head), 1)
    row_index = lax.broadcasted_iota(jnp.int32, (tok, head), 0)

    @pl.loop(0, nb)
    def _(i):
        place = ((i * na + a) * tok + row_index).astype(f32)
        angle = place * r.gains[2:3, :]
        r.cos_tab[rows_of(i), :] = jnp.cos(angle)
        turned = jnp.sin(angle)
        r.sin_tab[rows_of(i), :] = jnp.where(lane_index < head // 2, -turned, turned)

    x_more = to_core(x_copies, r.xc)
    arrive(rows_copies + cols_copies + x_more)
    arrive(kv_weights)
    for copy in w_here:
        copy.wait()
    for k in range(na):
        r.cols_sum[:, k * sub : (k + 1) * sub] = r.cols_all[k]
    gain_in = r.cols_sum[experts : experts + 1, :]
    for i in range(nb):
        columns = jnp.transpose(r.rows_all[a, i])
        r.ids[i] = columns
        r.hn[i] = (r.xc[i].astype(f32) * columns[:, 0:1] * gain_in).astype(bf16)
        for j in range(na):
            r.docs[j, :, i * tok : (i + 1) * tok] = r.rows_all[j, i][3:4, :]

    def weight(j):
        return r.wqkv[j].reshape(part, width)

    @pl.loop(0, nb)
    def _(i):
        for j in (1, 2):
            term = dot(r.hn[i], weight(j)).astype(bf16)
            for h in range(heads):
                piece = term[:, h * head : (h + 1) * head]
                r.pkv[h, rows_of(i), (j - 1) * head : j * head] = piece

    kv_sum = net.reduce(r.pkv, r.gkv)
    arrive(q_weights)

    @pl.loop(0, nb)
    def _(i):
        term = dot(r.hn[i], weight(0)).astype(bf16)
        for h in range(heads):
            r.pq[h, rows_of(i), :] = term[:, h * head : (h + 1) * head]

    stage_copy.wait()
    relayout(r.wg)
    wg_copies = over_a(r.wg.at[a], r.wg)
    stage_copy = move(r.wu_in, r.stage)
    kv_sum.inner()
    q_sum = net.reduce(r.pq, r.gq)
    stage_copy.wait()
    relayout(r.wu)
    q_sum.inner()
    cot_more = to_core(cot_copies, r.cotc)
    kv_sum.wait()

    @pl.loop(0, nb)
    def _(i):
        rows = rows_of(i)
        both = kv_sum.total(rows)
        r.raw[rows, head:] = both
        keys = both[:, :head]
        normed = keys * head_norm(keys) * r.gains[1:2, :]
        r.kv[a, rows, :head] = rope(normed, r.cos_tab[rows, :], r.sin_tab[rows, :]).astype(bf16)
        r.kv[a, rows, head:] = both[:, head:].astype(bf16)

    kv_copies = over_a(r.kv.at[a], r.kv)
    wu_copies = over_a(r.wu.at[a], r.wu)
    arrive(wd_copies + cot_more)
    for copy in late_here:
        copy.wait()

    def chosen(left, weights, d, put):
        columns = r.ids[d]
        values = [jnp.zeros((tok, ff), f32) for k in range(top)]
        for e in range(experts):
            term = dot(left, weights[:, :, e * ff : (e + 1) * ff].reshape(part, ff))
            for k in range(top):
                values[k] = jnp.where(columns[:, 1 + k : 2 + k] == e, term, values[k])
        for k in range(top):
            put(k, values[k].astype(bf16))

    groups = ff // head

    @pl.loop(0, nb)
    def _(i):
        def put(k, value):
            for g in range(groups):
                r.pcd[k, i, g * tok : (g + 1) * tok, :] = value[:, g * head : (g + 1) * head]

        chosen(r.cotc[i], r.wd, i, put)

    cd_sums = [net.reduce(r.pcd.at[0], r.gcd.at[0])]
    q_sum.wait()

    @pl.loop(0, nb)
    def _(i):
        rows = rows_of(i)
        query = q_sum.total(rows)
        r.raw[rows, :head] = query
        normed = query * head_norm(query) * r.gains[0:1, :]
        r.q_rot[rows, :] = rope(normed, r.cos_tab[rows, :], r.sin_tab[rows, :]).astype(bf16)

    cd_sums[0].inner()

    def attend(block, first, last):
        @pl.loop(0, nb)
        def _(i):
            rows = rows_of(i)
            columns = r.ids[i]
            scores = dot(r.q_rot[rows, :], r.kv[block, :, :head], NT) * scale
            scores = jnp.where(columns[:, 3:4] == r.docs[block], scores, negative)
            most = jnp.max(scores, axis=1, keepdims=True)
            if not first:
                before = r.stat[rows, 0:1]
                most = jnp.maximum(before, most)
            terms = jnp.exp(scores - most)
            total = jnp.sum(terms, axis=1, keepdims=True)
            mixed = dot(terms.astype(bf16), r.kv[block, :, head:])
            if not first:
                fade = jnp.exp(before - most)
                total = r.stat[rows, 1:2] * fade + total
                mixed = r.head_acc[rows, :] * fade + mixed
            if last:
                r.ho[rows, head_lane] = (mixed * (1.0 / total)).astype(bf16)
                r.stat[rows, 2:3] = most + jnp.log(total)
            else:
                r.stat[rows, 0:1] = most
                r.stat[rows, 1:2] = total
                r.head_acc[rows, :] = mixed

    attend(a, True, na == 1)
    for k in range(1, na):
        kv_copies[k - 1].wait_recv()
        attend(lax.rem(a + na - k, na), False, k == na - 1)

    def head_block(array, i, start, size):
        return array.at[pl.ds(start, size), pl.ds(pl.multiple_of(i * head, head), head)]

    cuts = [0, nb - 1, nb]

    def ho_half(s):
        start, size = cuts[s] * tok, (cuts[s + 1] - cuts[s]) * tok
        return net.spread(lambda i: head_block(r.ho, i, start, size))

    ho_lines = [ho_half(0)]
    arrive(wo_copies)
    ho_lines[0].take(ho_lines[0].order[0])
    ho_lines.append(ho_half(1))

    mixer = TwoLevel(net, r.acc, r.sendc, r.recvc, r.sendy, r.recvy, 1)
    for s in range(2):
        if s == 0:
            ho_lines[0].take(ho_lines[0].order[1])
            ho_lines[0].take(ho_lines[0].order[2])
        else:
            ho_lines[1].take_all()
            for k in range(1, top):
                cd_sums.append(net.reduce(r.pcd.at[k], r.gcd.at[k]))
        for i in range(cuts[s], cuts[s + 1]):
            term = dot(r.ho[i * tok : (i + 1) * tok, :], r.wo[...].reshape(part, width), NT)
            mixer.put(i, 0, term, i)
        for i in range(cuts[s], cuts[s + 1]):
            mixer.onward(i, 0, i)
    for group_sum in cd_sums[1:]:
        group_sum.inner()
    gain_mid = r.cols_sum[experts + 1 : experts + 2, :]
    router = r.cols_sum[...].astype(bf16)
    last_copies = []
    for i in range(nb):
        value = r.xc[i, mine, :].astype(f32) + mixer.total(i, 0)
        r.hidden[i] = value
        piece = (value * gain_mid).astype(bf16)
        r.scaled[i, mine, :] = piece
        logits = dot(router, piece, NT)
        squares = jnp.sum(value * value, axis=1, keepdims=True)
        squares = jnp.transpose(jnp.broadcast_to(squares, (half, 128)))[:1, :]
        which = lax.broadcasted_iota(jnp.int32, logits.shape, 0)
        r.small[i, :, mine] = jnp.where(which == experts, squares, logits)
        for array in (r.scaled.at[i, mine, :], r.small.at[i, :, mine]):
            last_copies.append(ship(array, array, core))
    arrive(wg_copies + wu_copies + last_copies)
    mixer.finish()
    kv_sum.finish()
    q_sum.finish()

    small_copies = [ship(r.small.at[p["b"]], r.small_in.at[b], p) for p in b_peers]
    r.small_in[b] = r.small[b]

    def make(d):
        for j, w in enumerate((r.wg, r.wu)):

            def put(k, value, j=j):
                r.pkv[d, (2 * k + j) * tok : (2 * k + j + 1) * tok, :] = value

            chosen(r.scaled[d], w, d, put)

    gu_sum = net.reduce(r.pkv, r.gkv, make)
    gu_sum.inner()
    make(b)
    arrive(small_copies)
    for group_sum in cd_sums:
        group_sum.wait()
    gu_sum.wait()
    total = jnp.sum(r.small_in[...], axis=0)
    r_mid = lax.rsqrt(total[experts : experts + 1] / model + eps)
    logits = total[:experts] * r_mid
    terms = jnp.exp(logits - jnp.max(logits, axis=0, keepdims=True))
    probs = terms / jnp.sum(terms, axis=0, keepdims=True)
    which = lax.broadcasted_iota(jnp.int32, probs.shape, 0).astype(f32)
    picks = [r.rows_own[1 + k : 2 + k] == which for k in range(top)]
    combine = [jnp.sum(jnp.where(pick, probs, 0.0), axis=0, keepdims=True) for pick in picks]
    table = jnp.where(which8 == 0, r_mid, 0.0)
    for k in range(top):
        table = jnp.where(which8 == 1 + k, combine[k], table)
    columns = jnp.transpose(table)
    r_col = columns[:, 0:1]
    columns_back = []
    inner = jnp.zeros((tok, 1), f32)
    for k in range(top):
        gate = gu_sum.total(slice((2 * k) * tok, (2 * k + 1) * tok)) * r_col
        up = gu_sum.total(slice((2 * k + 1) * tok, (2 * k + 2) * tok)) * r_col
        back = jnp.concatenate(
            [
                cd_sums[k].total(slice(g * tok, (g + 1) * tok))
                for g in range(groups)
            ],
            axis=1,
        )
        sig = 1.0 / (1.0 + jnp.exp(-gate))
        silu = gate * sig
        act = silu * up
        weighed = columns[:, 1 + k : 2 + k]
        d_act = weighed * back
        d_gate = d_act * up * (sig * (1.0 + gate * (1.0 - sig)))
        d_up = d_act * silu
        for j, value in enumerate((weighed * act, d_gate * r_col, d_up * r_col)):
            r.pay[b, :, (top * j + k) * ff : (top * j + k + 1) * ff] = value.astype(bf16)
        columns_back.append(jnp.sum(act * back, axis=1, keepdims=True))
        inner = inner + jnp.sum(d_gate * gate + d_up * up, axis=1, keepdims=True)

    pay_line = net.spread(lambda i: r.pay.at[i])
    rank = y * sizes["c"] + c
    r.pair[rank] = transpose_columns(columns_back + [inner], tok)
    arrive([ship(r.pair.at[rank], r.pair.at[rank], place) for place in tp_peers])
    sums = r.pair[0] + r.pair[1] + r.pair[2] + r.pair[3]
    d_probs = jnp.zeros_like(probs)
    for k in range(top):
        d_probs = d_probs + jnp.where(picks[k], sums[k : k + 1], 0.0)
    d_logits = probs * (d_probs - jnp.sum(probs * d_probs, axis=0, keepdims=True))
    inner_row = sums[top : top + 1] + jnp.sum(d_logits * logits, axis=0, keepdims=True)
    r.late_small[b, 0:8, :] = d_logits * r_mid
    r.late_small[b, 8:16, :] = jnp.broadcast_to(r_mid * r_mid * inner_row / model, (8, tok))
    late_copies = [ship(r.late_small.at[b], r.late_small.at[b], place) for place in b_peers]

    mixer = TwoLevel(net, r.acc, r.sendc, r.recvc, r.sendy, r.recvy, 2)
    pieces = experts * ff // width
    by_piece = width // ff

    def expand(j, i, e):
        columns = r.ids[i]
        value = jnp.zeros((tok, ff), f32)
        for k in range(top):
            taken = r.pay[i, :, (top * j + k) * ff : (top * j + k + 1) * ff].astype(f32)
            value = jnp.where(columns[:, 1 + k : 2 + k] == e, taken, value)
        return value.astype(bf16)

    def use(i):
        def widen(j):
            for e in range(experts):
                g, h = e // by_piece, e % by_piece
                r.wide[j, g * tok : (g + 1) * tok, h * ff : (h + 1) * ff] = expand(j, i, e)

        def times(j, w):
            total = 0.0
            for g in range(pieces):
                piece = w[:, :, g * width : (g + 1) * width].reshape(part, width)
                total = total + dot(r.wide[j, g * tok : (g + 1) * tok, :], piece, NT)
            return total

        widen(1)
        widen(2)
        mixer.put(i, 0, times(1, r.wg) + times(2, r.wu), 0)
        widen(0)
        mixer.onward(i, 0, 0)
        mixer.put(i, 1, times(0, r.wd), 1)
        mixer.onward(i, 1, 1)

    @pl.loop(0, nb)
    def _(n):
        index = b
        for k in range(nb - 1):
            index = jnp.where(n == k + 1, pay_line.order[k], index)

        @pl.when(n > 0)
        def _():
            pay_line.take(index)

        use(index)

    arrive(late_copies)
    which16 = lax.broadcasted_iota(jnp.int32, (16, tok), 0)
    ffn_part = jnp.zeros((1, part), f32)
    attn_copies = []
    for i in range(nb):
        columns = jnp.transpose(r.late_small[i, :, mine])
        d_log = jnp.where(which16[:, :half] < experts, r.late_small[i, :, mine], 0.0).astype(bf16)
        mid = mixer.total(i, 0) + dot(d_log, router, TN)
        value = r.hidden[i]
        grad = r.cotc[i, mine, :].astype(f32) + gain_mid * mid - value * columns[:, 8:9]
        r.d_attn[i, mine, :] = grad.astype(bf16)
        attn_copies.append(ship(r.d_attn.at[i, mine, :], r.d_attn.at[i, mine, :], core))
        ffn_part = ffn_part + jnp.sum(mid * value, axis=0, keepdims=True)
        mix = mixer.total(i, 1)
        r.out_half[i] = (value + mix).astype(bf16)
        r.hidden[i] = grad
    d_hidden = r.hidden
    arrive(attn_copies)

    @pl.loop(0, nb)
    def _(i):
        term = dot(r.d_attn[i], r.wo[...].reshape(part, width)).astype(bf16)
        for h in range(heads):
            r.pq[h, rows_of(i), :] = term[:, h * head : (h + 1) * head]

    heads_sum = net.reduce(r.pq, r.gq)

    drain(wd_copies + wg_copies + wu_copies)
    gu_sum.finish()

    def to_a(source, target):
        return [ship(source.at[p["a"]], target.at[k], p) for k, p in enumerate(a_peers)]

    def expert_grad(j, left, target):
        @pl.loop(0, experts)
        def _(e):
            for i in range(nb):
                r.pkv[0, i * tok : (i + 1) * tok, :] = expand(j, i, e)
            grad = dot(left[...].reshape(col, part), r.pkv[0], TN).astype(bf16)
            lane = pl.ds(pl.multiple_of(e * ff, ff), ff)
            for k in range(na):
                target[k, :, lane] = grad[k * sub : (k + 1) * sub, :]

    expert_grad(0, r.cotc, r.wd)
    pending = to_a(r.wd, r.down_in)
    results = [move(r.wd.at[a], r.down_own)]
    heads_sum.inner()
    term = dot(r.d_attn[...].reshape(col, part), r.ho[...], TN).astype(bf16)
    r.gout[...] = term.reshape(na, sub, width)
    extra = 0.0
    for i in range(nb):
        d_log = jnp.where(which16 < experts, r.late_small[i], 0.0).astype(bf16)
        extra = extra + dot(d_log, r.scaled[i])
    which_row = lax.broadcasted_iota(jnp.int32, (16, part), 0)
    r.extra_own[...] = jnp.where(which_row == experts + 1, ffn_part, extra)
    expert_grad(1, r.scaled, r.wg)
    heads_sum.wait()
    out_copies = [
        ship(r.out_half.at[p["b"]], r.block_out.at[mine, own_lane], p) for p in b_peers
    ]
    r.block_out[mine, own_lane] = r.out_half[b]

    r.gain_acc[...] = jnp.zeros_like(r.gain_acc)

    @pl.loop(0, nb)
    def _(i):
        rows = rows_of(i)
        cot = heads_sum.total(rows).astype(bf16)
        r.pq[b, rows, :] = cot
        delta = jnp.sum(cot.astype(f32) * r.ho[rows, head_lane].astype(f32), axis=1, keepdims=True)
        r.stat[rows, 4:5] = delta

    def attend_back(block, first, last, start, stop):
        @pl.loop(start, stop)
        def _(i):
            rows = rows_of(i)
            columns = r.ids[i]
            query, cot = r.q_rot[rows, :], r.pq[b, rows, :]
            keys, values = r.kv[block, :, :head], r.kv[block, :, head:]
            scores = dot(query, keys, NT) * scale
            keep = columns[:, 3:4] == r.docs[block]
            probs = jnp.where(keep, jnp.exp(scores - r.stat[rows, 2:3]), 0.0)
            d_scores = (probs * (dot(cot, values, NT) - r.stat[rows, 4:5])).astype(bf16)
            key_term = dot(d_scores, query, TN) * scale
            value_term = dot(probs.astype(bf16), cot, TN)

            @pl.when(i == 0)
            def _():
                r.dkv_acc[:, :head] = key_term
                r.dkv_acc[:, head:] = value_term

            @pl.when(i > 0)
            def _():
                r.dkv_acc[:, :head] += key_term
                r.dkv_acc[:, head:] += value_term

            grad = dot(d_scores, keys) * scale
            if not first:
                grad = r.head_acc[rows, :] + grad
            if not last:
                r.head_acc[rows, :] = grad
            else:
                source = r.raw[rows, :head]
                grad, gain_part = unrope(
                    grad, source, r.gains[0:1, :], r.cos_tab[rows, :], r.sin_tab[rows, :]
                )
                r.gain_acc[0:1, :] += gain_part
                r.wide[0, rows, head_lane] = grad.astype(bf16)
                r.stat[rows, 3:4] = jnp.sum(grad * source, axis=1, keepdims=True)

    kv_back = []
    for k in range(1, na):
        attend_back(lax.rem(a + k, na), k == 1, False, 0, nb)
        r.dkv_send[k - 1] = r.dkv_acc[...].astype(bf16)
        kv_back.append(ship(r.dkv_send.at[k - 1], r.dkv_in.at[k - 1], a_peers[k - 1]))
    pending += to_a(r.wg, r.gate_in) + to_a(r.gout, r.gout_in)
    results.append(move(r.wg.at[a], r.gate_own))
    q_lines = []
    for s in range(2):
        attend_back(a, na == 1, True, s * (nb // 2), (s + 1) * (nb // 2))
        q_lines.append(
            net.spread(lambda i, s=s: head_block(r.wide.at[0], i, s * (col // 2), col // 2))
        )
    out_more = []
    for k, copy in zip(range(1, nb), out_copies):
        lane = lane_of(lax.rem(b + nb - k, nb))
        copy.wait_recv()
        out_more.append(ship(r.block_out.at[mine, lane], r.block_out.at[mine, lane], core))
    out_more.append(ship(r.block_out.at[mine, own_lane], r.block_out.at[mine, own_lane], core))
    expert_grad(2, r.scaled, r.wu)
    pending += to_a(r.wu, r.up_in)
    results.append(move(r.wu.at[a], r.up_own))
    arrive(kv_back)

    @pl.loop(0, nb)
    def _(i):
        rows = rows_of(i)
        both = r.dkv_acc[rows, :]
        for k in range(na - 1):
            both = both + r.dkv_in[k, rows, :].astype(f32)
        source = r.raw[rows, head : 2 * head]
        grad, gain_part = unrope(
            both[:, :head], source, r.gains[1:2, :], r.cos_tab[rows, :], r.sin_tab[rows, :]
        )
        r.gain_acc[1:2, :] += gain_part
        value_grad = both[:, head:]
        r.wide[1, rows, head_lane] = grad.astype(bf16)
        r.wide[2, rows, head_lane] = value_grad.astype(bf16)
        r.stat[rows, 3:4] += jnp.sum(
            grad * source + value_grad * r.raw[rows, 2 * head :], axis=1, keepdims=True
        )

    def kv_half(s):
        start, size = cuts[s] * tok, (cuts[s + 1] - cuts[s]) * tok
        return net.spread(
            lambda i: head_block(r.wide.at[1], i, start, size),
            lambda i: head_block(r.wide.at[2], i, start, size),
        )

    for line in q_lines:
        line.take(line.order[0])
    kv_lines = [kv_half(0)]
    place16 = (b * 2 + y) * 2 + c
    r.s4[place16] = transpose_columns([r.stat[i * tok : (i + 1) * tok, 3:4] for i in range(nb)], tok)
    r.s4[place16, 4:6, 0:head] = r.gain_acc[0:2, :]
    s4_copies = [ship(r.s4.at[place16], r.s4.at[place16], place) for place in group]

    def weight_grad(j):
        grad = dot(r.hn[...].reshape(col, part), r.wide[j], TN).astype(bf16)
        r.gsend[j] = grad.reshape(na, sub, width)
        return to_a(r.gsend.at[j], r.gin_w.at[j])

    for line in q_lines:
        line.take(line.order[1])
        line.take(line.order[2])
    pending += weight_grad(0)
    kv_lines[0].take(kv_lines[0].order[0])
    kv_lines.append(kv_half(1))

    mixer_in = TwoLevel(net, r.acc, r.sendc, r.recvc, r.sendy, r.recvy, 1)
    mixer.finish()
    arrive(s4_copies)
    for s in range(2):
        if s == 0:
            kv_lines[0].take(kv_lines[0].order[1])
            kv_lines[0].take(kv_lines[0].order[2])
        else:
            kv_lines[1].take_all()
        for i in range(cuts[s], cuts[s + 1]):
            rows = slice(i * tok, (i + 1) * tok)
            term = dot(r.wide[0, rows, :], weight(0), NT)
            term = term + dot(r.wide[1, rows, :], weight(1), NT)
            mixer_in.put(i, 0, term + dot(r.wide[2, rows, :], weight(2), NT), i)
        for i in range(cuts[s], cuts[s + 1]):
            mixer_in.onward(i, 0, i)
    sums = r.s4[0]
    for k in range(1, 4 * nb):
        sums = sums + r.s4[k]
    inner_columns = jnp.transpose(sums)
    attn_part = jnp.zeros((1, part), f32)
    in_hops = []
    base_in = net.used
    net.used += nb

    def in_hop(d, slot):
        return pltpu.make_async_remote_copy(
            src_ref=r.out_half.at[d],
            dst_ref=r.gin.at[mine, own_lane],
            send_sem=r.send.at[base_in + d],
            recv_sem=r.recv.at[base_in + slot],
            device_id={"b": jnp.int32(d)},
            device_id_type=MESH,
        )

    drain(out_copies)
    for i in range(nb):
        d_in = mixer_in.total(i, 0)
        r_col = r.ids[i, mine, 0:1]
        inner = jnp.where(
            c == 0, inner_columns[:half, i : i + 1], inner_columns[half:, i : i + 1]
        )
        x = r.xc[i, mine, :].astype(f32)
        scaled = d_in * r_col
        grad = d_hidden[i] + scaled * gain_in - x * (r_col * r_col * inner / model)
        attn_part = attn_part + jnp.sum(scaled * x, axis=0, keepdims=True)
        r.out_half[i] = grad.astype(bf16)

        @pl.when(b == i)
        def _():
            r.gin[mine, own_lane] = r.out_half[i]

        @pl.when(b != i)
        def _():
            in_hop(i, b).start()

    r.extra_own[...] = jnp.where(which_row == experts + 2, attn_part, r.extra_own[...])
    tail_copy = ship(r.extra_own, r.extra_in, core)
    pending += weight_grad(1)
    pending += weight_grad(2)
    tail_copy.wait_recv()
    shared = (which_row == experts + 1) | (which_row == experts + 2)
    r.tail_all[a] = r.extra_own[...] + jnp.where(shared, r.extra_in[...], 0.0)
    r.tail_all[a, experts + 3 : experts + 5, 0:head] = sums[4:6, 0:head]
    tail_copies = over_a(r.tail_all.at[a], r.tail_all)
    in_more = []
    for k in range(1, nb):
        place = lax.rem(b + k, nb)
        lane = lane_of(place)
        pltpu.make_async_remote_copy(
            src_ref=r.gin.at[mine, lane],
            dst_ref=r.gin.at[mine, lane],
            send_sem=r.send.at[base_in + place],
            recv_sem=r.recv.at[base_in + place],
            device_id=core,
            device_id_type=MESH,
        ).wait_recv()
        in_more.append(ship(r.gin.at[mine, lane], r.gin.at[mine, lane], core))
    in_more.append(ship(r.gin.at[mine, own_lane], r.gin.at[mine, own_lane], core))
    arrive(out_more)
    results.append(move(r.block_out, r.out_rows))
    arrive(pending)
    for j in range(4):
        mine_here = r.gsend[j, a] if j < 3 else r.gout[a]
        total = mine_here.astype(f32)
        for k in range(na - 1):
            came = r.gin_w[j, k] if j < 3 else r.gout_in[k]
            total = total + came.astype(f32)
        r.proj[j] = total
    results.append(move(r.proj, r.proj_out))
    arrive(tail_copies)
    r.tail[...] = jnp.sum(r.tail_all[...], axis=0)
    arrive(in_more)
    results.append(move(r.gin, r.in_rows))
    mixer_in.finish()
    for line in [heads_sum, pay_line] + cd_sums + ho_lines + q_lines + kv_lines:
        line.finish()
    for d in range(nb):

        @pl.when(b != d)
        def _():
            in_hop(d, b).wait_send()

    drain(list(sent))
    for copy in results:
        copy.wait()
    assert net.used <= r.send.shape[0] and local_used[0] <= r.local.shape[0]


def layer(sizes, dims, ins):
    nb, na, head, heads, experts, ff, top = dims
    tok, model = ins[0].shape
    part, col, half = model // nb, nb * tok, tok // 2
    sub, width, wide = part // na, heads * head, experts * ff
    others = max(na - 1, 1)
    shape = jax.ShapeDtypeStruct
    vmem, hbm = pl.BlockSpec(memory_space=pltpu.VMEM), pl.BlockSpec(memory_space=pl.ANY)
    outs = [
        shape((tok, model), bf16),
        shape((tok, model), bf16),
        shape((sub, wide), bf16),
        shape((sub, wide), bf16),
        shape((sub, wide), bf16),
        shape((others, sub, wide), bf16),
        shape((others, sub, wide), bf16),
        shape((others, sub, wide), bf16),
        shape((4, sub, width), f32),
        shape((16, part), f32),
    ]
    work = dict(
        xc=((nb, tok, part), bf16),
        cotc=((nb, tok, part), bf16),
        rows_all=((na, nb, 8, tok), f32),
        rows_own=((8, tok), f32),
        cols_own=((16, sub), f32),
        cols_all=((na, 16, sub), f32),
        cols_sum=((16, part), f32),
        wqkv=((3, na, sub, width), bf16),
        wo=((na, sub, width), bf16),
        wg=((na, sub, wide), bf16),
        wu=((na, sub, wide), bf16),
        wd=((na, sub, wide), bf16),
        stage=((sub, experts, ff), bf16),
        hn=((nb, tok, part), bf16),
        raw=((col, 3 * head), f32),
        q_rot=((col, head), bf16),
        kv=((na, col, 2 * head), bf16),
        stat=((col, 128), f32),
        ho=((col, width), bf16),
        cos_tab=((col, head), f32),
        sin_tab=((col, head), f32),
        pkv=((nb, col, 2 * head), bf16),
        gkv=((nb, col, 2 * head), bf16),
        pq=((nb, col, head), bf16),
        gq=((nb, col, head), bf16),
        pcd=((top, nb, ff // head * tok, head), bf16),
        gcd=((top, nb, ff // head * tok, head), bf16),
        acc=((nb, half, part), f32),
        sendc=((nb, half, 2 * part), bf16),
        recvc=((nb, half, 2 * part), bf16),
        sendy=((nb, half, 2 * part), bf16),
        recvy=((nb, half, 2 * part), bf16),
        hidden=((nb, half, part), f32),
        scaled=((nb, tok, part), bf16),
        small=((nb, 16, tok), f32),
        small_in=((nb, 16, tok), f32),
        pay=((nb, tok, 3 * top * ff), bf16),
        wide=((3, col, width), bf16),
        pair=((4, 8, tok), f32),
        late_small=((nb, 16, tok), f32),
        extra_own=((16, part), f32),
        extra_in=((16, part), f32),
        d_attn=((nb, tok, part), bf16),
        out_half=((nb, half, part), bf16),
        block_out=((tok, model), bf16),
        head_acc=((col, head), f32),
        dkv_acc=((col, 2 * head), f32),
        dkv_send=((others, col, 2 * head), bf16),
        dkv_in=((others, col, 2 * head), bf16),
        gsend=((3, na, sub, width), bf16),
        gin_w=((3, others, sub, width), bf16),
        gout=((na, sub, width), bf16),
        gout_in=((others, sub, width), bf16),
        gin=((tok, model), bf16),
        s4=((4 * nb, 8, tok), f32),
        gain_acc=((8, head), f32),
        tail_all=((na, 16, part), f32),
        ids=((nb, tok, 8), f32),
        gains=((8, head), f32),
        docs=((na, 1, col), f32),
        proj=((4, sub, width), f32),
    )
    count = 160 + 26 * na
    scratch = [pltpu.VMEM(*work[name]) for name in WORK[:-3]] + [
        pltpu.SemaphoreType.DMA((count,)),
        pltpu.SemaphoreType.DMA((count,)),
        pltpu.SemaphoreType.DMA((24,)),
    ]
    return pl.pallas_call(
        functools.partial(layer_kernel, sizes, dims),
        out_shape=outs,
        in_specs=[hbm] * 9 + [vmem] * 8,
        out_specs=[hbm] * 9 + [vmem],
        scratch_shapes=scratch,
        compiler_params=pltpu.CompilerParams(
            collective_id=1, has_side_effects=True, vmem_limit_bytes=67043328
        ),
        name="layer",
    )(*ins)


def last_kernel(experts, ff, sub, *refs):
    out_rows, in_rows, owns, cames, proj = refs[0], refs[1], refs[2:5], refs[5:8], refs[8]
    tail, refs = refs[9], refs[10:]
    block_out, grad_in, grads, projections = refs[0], refs[1], refs[2:5], refs[5:9]
    router, gain_attn, gain_ffn, gain_q, gain_k = refs[9:]
    block_out[...] = out_rows[...]
    grad_in[...] = in_rows[...].astype(f32)
    for own, came, grad in zip(owns, cames, grads):
        for e in range(experts):
            lane = slice(e * ff, (e + 1) * ff)
            total = own[:, lane].astype(f32)
            for k in range(came.shape[0]):
                total = total + came[k, :, lane].astype(f32)
            grad[:, e, :] = total
    for j in range(4):
        projections[j][...] = proj[j]

    @pl.when(pl.program_id(0) == 0)
    def _():
        a = lax.axis_index("a")
        piece = tail[:, :sub]
        for k in range(1, tail.shape[1] // sub):
            piece = jnp.where(a == k, tail[:, k * sub : (k + 1) * sub], piece)
        router[...] = piece[:experts]
        gain_ffn[...] = piece[experts + 1 : experts + 2]
        gain_attn[...] = piece[experts + 2 : experts + 3]
        gain_q[...] = tail[experts + 3 : experts + 4, : gain_q.shape[1]]
        gain_k[...] = tail[experts + 4 : experts + 5, : gain_k.shape[1]]


def last(dims, ins):
    nb, na, head, heads, experts, ff, top = dims
    tok, model = ins[0].shape
    sub, wide = ins[2].shape
    others, width = ins[5].shape[0], ins[8].shape[2]
    steps = 4
    shape = jax.ShapeDtypeStruct
    rows = pl.BlockSpec((tok // steps, model), lambda i: (i, 0))
    own = pl.BlockSpec((sub // steps, wide), lambda i: (i, 0))
    came = pl.BlockSpec((others, sub // steps, wide), lambda i: (0, i, 0))
    grad = pl.BlockSpec((sub // steps, experts, ff), lambda i: (i, 0, 0))
    flat = pl.BlockSpec((sub // steps, width), lambda i: (i, 0))
    small = [shape((experts, sub), f32), shape((1, sub), f32), shape((1, sub), f32)]
    small += [shape((1, head), f32)] * 2
    return pl.pallas_call(
        functools.partial(last_kernel, experts, ff, sub),
        grid=(steps,),
        out_shape=[shape((tok, model), bf16), shape((tok, model), f32)]
        + [shape((sub, experts, ff), f32)] * 3
        + [shape((sub, width), f32)] * 4
        + small,
        in_specs=[rows, rows] + [own] * 3 + [came] * 3
        + [pl.BlockSpec((4, sub // steps, width), lambda i: (0, i, 0))]
        + [pl.BlockSpec(ins[9].shape, lambda i: (0, 0))],
        out_specs=[rows, rows] + [grad] * 3 + [flat] * 4
        + [pl.BlockSpec(item.shape, lambda i: (0, 0)) for item in small],
        name="last",
    )(*ins)


def on_device(
    sizes,
    tokens_in,
    doc_ids,
    expert_ids,
    attn_gain,
    q_gain,
    k_gain,
    w_query,
    w_key,
    w_value,
    w_output,
    ffn_gain,
    w_router,
    w_gate,
    w_up,
    w_down,
    cotangent,
):
    nb, na = sizes["b"], sizes["a"]
    tok, model = tokens_in.shape
    part = model // nb
    sub = part // na
    head = q_gain.shape[0]
    width = w_query.shape[1]
    heads = width // head
    experts, ff = w_gate.shape[1], w_gate.shape[2]
    top = expert_ids.shape[1]
    dims = (nb, na, head, heads, experts, ff, top)

    speed = theta ** (-2.0 * (np.arange(head) % (head // 2)) / head)
    parts = layer(
        sizes,
        dims,
        [
            tokens_in, cotangent, w_query, w_key, w_value, w_output, w_gate, w_up, w_down,
            expert_ids.T, doc_ids[None], w_router.T, attn_gain[None], ffn_gain[None], q_gain[None],
            k_gain[None], jnp.asarray(speed, f32)[None],
        ],
    )
    (
        block_out, grad_in, grad_gate, grad_up, grad_down, grad_query, grad_key, grad_value,
        grad_output, router, gain_attn, gain_ffn, gain_q, gain_k,
    ) = last(dims, parts)
    return (
        block_out,
        grad_in,
        gain_attn.reshape(sub),
        gain_q.reshape(head),
        gain_k.reshape(head),
        grad_query,
        grad_key,
        grad_value,
        grad_output,
        gain_ffn.reshape(sub),
        router.T,
        grad_gate,
        grad_up,
        grad_down,
    )


def solution(mesh):
    cp, tp = mesh.shape["cp"], mesh.shape["tp"]
    sizes = {"b": 4, "a": cp // 4, "y": 2, "c": tp // 2}
    split = Mesh(mesh.devices.reshape([sizes[axis] for axis in AXES]), AXES)
    cp, tp = ("b", "a"), ("y", "c")
    return jax.shard_map(
        functools.partial(on_device, sizes),
        mesh=split,
        in_specs=(
            P(cp, None),
            P(cp),
            P(cp, None),
            P(cp),
            P(),
            P(),
            P(cp, tp),
            P(cp, tp),
            P(cp, tp),
            P(cp, tp),
            P(cp),
            P(cp, None),
            P(cp, None, tp),
            P(cp, None, tp),
            P(cp, None, tp),
            P(cp, None),
        ),
        out_specs=(
            P(cp, None),
            P(cp, None),
            P(cp),
            P(),
            P(),
            P(cp, tp),
            P(cp, tp),
            P(cp, tp),
            P(cp, tp),
            P(cp),
            P(cp, None),
            P(cp, None, tp),
            P(cp, None, tp),
            P(cp, None, tp),
        ),
        check_vma=False,
    )
```

```python
import functools
import types

import jax
import jax.numpy as jnp
import numpy as np
from jax import lax
from jax.experimental import pallas as pl
from jax.experimental.pallas import tpu as pltpu
from jax.sharding import Mesh
from jax.sharding import PartitionSpec as P

eps = 1e-05
theta = 50000.0
negative = -1e30
AXES = ("b", "a", "y", "c")
MESH = pl.DeviceIdType.MESH
bf16 = jnp.bfloat16
f32 = jnp.float32


NT = (((1,), (1,)), ((), ()))
TN = (((0,), (0,)), ((), ()))


def dot(left, right, dims=(((1,), (0,)), ((), ()))):
    return lax.dot_general(left, right, dims, preferred_element_type=f32)


class Net:
    def __init__(self, sizes, send, recv):
        self.sizes, self.send, self.recv, self.used = sizes, send, recv, 0
        self.me = {axis: lax.axis_index(axis) for axis in AXES}

    def near(self, **offs):
        return {axis: lax.rem(self.me[axis] + off, self.sizes[axis]) for axis, off in offs.items()}

    def copy(self, source, target, place):
        slot = self.used
        self.used += 1
        return pltpu.make_async_remote_copy(
            src_ref=source,
            dst_ref=target,
            send_sem=self.send.at[slot],
            recv_sem=self.recv.at[slot],
            device_id=place,
            device_id_type=MESH,
        )

    def greet(self, places):
        barrier = pltpu.get_barrier_semaphore()
        for place in places:
            pl.semaphore_signal(barrier, inc=1, device_id=place, device_id_type=MESH)
        pl.semaphore_wait(barrier, len(places))

    def pick(self, *values):
        result = values[-1]
        for i in range(len(values) - 2, -1, -1):
            result = jnp.where(self.me["b"] == i, values[i], result)
        return result

    def reduce(self, *args):
        return Reduce(self, *args)

    def spread(self, *blocks, start=True):
        return Spread(self, blocks, start)


class Reduce:
    def __init__(self, net, parts, got, make=None):
        self.net, self.parts, self.got = net, parts, got
        self.b = b = net.me["b"]
        self.base = net.used
        net.used += 4
        self.order = [3 - b, net.pick(2, 0, 3, 1), net.pick(1, 3, 0, 2)]
        for k in range(2):
            if make is not None:
                make(self.order[k])
            self.hop(self.order[k]).start()
        if make is not None:
            make(self.order[2])

    def hop(self, d):
        net, b = self.net, self.b
        far = ((b == 0) & (d == 3)) | ((b == 3) & (d == 0))
        beside = jnp.where(b == 0, 1, 2)
        target, slot = jnp.where(far, beside, d), jnp.where(far, beside, b)
        return pltpu.make_async_remote_copy(
            src_ref=self.parts.at[d],
            dst_ref=self.got.at[slot],
            send_sem=net.send.at[self.base + d],
            recv_sem=net.recv.at[self.base + slot],
            device_id={"b": target},
            device_id_type=MESH,
        )

    def came(self, i):
        net = self.net
        return pltpu.make_async_remote_copy(
            src_ref=self.got.at[i],
            dst_ref=self.got.at[i],
            send_sem=net.send.at[self.base + i],
            recv_sem=net.recv.at[self.base + i],
            device_id=net.near(b=1),
            device_id_type=MESH,
        )

    def inner(self):
        b, d = self.b, self.order[2]

        @pl.when((b == 1) | (b == 2))
        def _():
            self.came(b).wait_recv()
            rows = self.parts.shape[1]
            step = 256 if rows % 256 == 0 else rows

            @pl.loop(0, rows // step)
            def _(i):
                sl = pl.ds(pl.multiple_of(i * step, step), step)
                total = self.parts[d, sl, :].astype(f32) + self.got[b, sl, :].astype(f32)
                self.parts[d, sl, :] = total.astype(bf16)

        self.hop(d).start()

    def wait(self):
        for i in range(4):

            @pl.when((self.b != i) & (jnp.abs(self.b - i) <= 2))
            def _():
                self.came(i).wait_recv()

    def total(self, *index):
        b = self.b
        value = self.parts[(b,) + index].astype(f32)
        for i in range(4):
            valid = (b != i) & (jnp.abs(b - i) <= 2)
            value = value + jnp.where(valid, self.got[(i,) + index].astype(f32), 0.0)
        return value

    def finish(self):
        for d in range(4):

            @pl.when(self.b != d)
            def _():
                self.hop(d).wait_send()


class Spread:
    def __init__(self, net, blocks, start):
        self.net, self.blocks = net, blocks
        self.b = b = net.me["b"]
        self.base = net.used
        net.used += 4 * len(blocks)
        self.targets = [net.pick(2, 3, 0, 1), net.pick(1, 0, 3, 2), net.pick(2, 2, 1, 1)]
        self.order = [net.pick(1, 3, 0, 2), net.pick(2, 0, 3, 1), net.pick(3, 2, 1, 0)]
        self.inner = (b == 1) | (b == 2)
        if start:
            self.begin()

    def begin(self):
        for k, target in enumerate(self.targets):
            if k < 2:
                for j in range(len(self.blocks)):
                    self.hop(self.b, target, target, j).start()
            else:

                @pl.when(self.inner)
                def _():
                    for j in range(len(self.blocks)):
                        self.hop(self.b, target, target, j).start()

    def after(self, other):
        @pl.when(jnp.logical_not(self.inner))
        def _():
            self.begin()

        other.take(other.order[0])

        @pl.when(self.inner)
        def _():
            self.begin()

    def hop(self, i, target, slot, j):
        net, count = self.net, len(self.blocks)
        return pltpu.make_async_remote_copy(
            src_ref=self.blocks[j](i),
            dst_ref=self.blocks[j](i),
            send_sem=net.send.at[self.base + slot * count + j],
            recv_sem=net.recv.at[self.base + i * count + j],
            device_id={"b": target},
            device_id_type=MESH,
        )

    def take(self, i):
        b = self.b
        onward = ((b == 1) & (i == 3)) | ((b == 2) & (i == 0))
        for j in range(len(self.blocks)):
            self.hop(i, self.net.near(b=1)["b"], b, j).wait_recv()

            @pl.when(onward)
            def _():
                self.hop(i, jnp.where(b == 1, 0, 3), b, j).start()

    def take_all(self):
        for i in self.order:
            self.take(i)

    def finish(self):
        b = self.b
        for k, target in enumerate(self.targets):
            for j in range(len(self.blocks)):
                if k < 2:
                    self.hop(b, target, target, j).wait_send()
                else:

                    @pl.when(self.inner)
                    def _():
                        self.hop(b, target, target, j).wait_send()
                        self.hop(b, jnp.where(b == 1, 0, 3), b, j).wait_send()


def rope(values, cos_tab, sin_tab):
    return values * cos_tab + pltpu.roll(values, values.shape[1] // 2, 1) * sin_tab


def head_norm(values):
    return lax.rsqrt(jnp.mean(values * values, axis=1, keepdims=True) + eps)


def unrope(grad, raw, gain, cos_tab, sin_tab):
    factor = head_norm(raw)
    normed = raw * factor
    turned = grad * cos_tab + pltpu.roll(grad * sin_tab, grad.shape[1] // 2, 1)
    gain_part = jnp.sum(turned * normed, axis=0, keepdims=True)
    inner = turned * gain
    slope = jnp.mean(raw * inner, axis=1, keepdims=True)
    return factor * inner - raw * (factor * factor * factor * slope), gain_part


class TwoLevel:
    def __init__(self, net, acc, sendc, recvc, sendy, recvy, used):
        self.net, self.acc = net, acc
        self.sendc, self.recvc, self.sendy, self.recvy = sendc, recvc, sendy, recvy
        self.used = used
        self.base = net.used
        net.used += 16
        self.part = acc.shape[2]
        self.half = acc.shape[1]

    def lane(self, j):
        return slice(j * self.part, (j + 1) * self.part)

    def hop(self, i, j, level):
        net = self.net
        source, target = ((self.sendc, self.recvc), (self.sendy, self.recvy))[level]
        slot = self.base + 8 * level + 2 * i + j
        lane = pl.ds(j * self.part, self.part)
        return pltpu.make_async_remote_copy(
            src_ref=source.at[i, :, lane],
            dst_ref=target.at[i, :, lane],
            send_sem=net.send.at[slot],
            recv_sem=net.recv.at[slot],
            device_id=net.near(c=1) if level == 0 else net.near(y=1),
            device_id_type=MESH,
        )

    def put(self, i, j, term, k):
        first = self.net.me["c"] == 0
        low, high = term[: self.half], term[self.half :]
        self.acc[k] = jnp.where(first, low, high)
        self.sendc[i, :, self.lane(j)] = jnp.where(first, high, low).astype(bf16)
        self.hop(i, j, 0).start()

    def onward(self, i, j, k):
        self.hop(i, j, 0).wait_recv()
        total = self.acc[k] + self.recvc[i, :, self.lane(j)].astype(f32)
        self.sendy[i, :, self.lane(j)] = total.astype(bf16)
        self.hop(i, j, 1).start()

    def total(self, i, j):
        self.hop(i, j, 1).wait_recv()
        lane = self.lane(j)
        return self.sendy[i, :, lane].astype(f32) + self.recvy[i, :, lane].astype(f32)

    def finish(self):
        for i in range(4):
            for j in range(self.used):
                self.hop(i, j, 0).wait_send()
                self.hop(i, j, 1).wait_send()


def transpose_columns(columns, rows):
    lane = lax.broadcasted_iota(jnp.int32, (rows, 128), 1)
    table = jnp.zeros((rows, 128), f32)
    for k, column in enumerate(columns):
        table = jnp.where(lane == k, column, table)
    return jnp.transpose(table)[:8, :]


INS = (
    "tok", "cot", "wq_in", "wk_in", "wv_in", "wo_in", "wg_in", "wu_in", "wd_in", "ids_in",
    "docs_in", "router_in", "gain_in_a", "gain_in_f", "gain_q", "gain_k", "speed_in",
)
OUTS = (
    "out_rows", "in_rows", "gate_own", "up_own", "down_own", "gate_in", "up_in", "down_in",
    "proj_out", "tail",
)
WORK = (
    "xc", "cotc", "rows_all", "rows_own", "cols_own", "cols_all", "cols_sum", "wqkv", "wo",
    "wg", "wu", "wd", "stage", "hn", "raw", "q_rot", "kv", "stat", "ho", "cos_tab", "sin_tab",
    "pkv", "gkv", "pq", "gq", "pcd", "gcd", "acc", "sendc", "recvc", "sendy", "recvy", "hidden", "d_hidden", "scaled",
    "small", "small_in", "pay", "wide", "pair", "late_small", "extra_own", "extra_in", "d_attn",
    "out_half", "block_out", "head_acc", "dkv_acc", "dkv_send", "dkv_in", "gsend", "gin_w",
    "gout", "gout_in", "gin", "s4", "gain_acc", "tail_all", "gains", "ids", "docs", "proj",
    "send", "recv", "local",
)


def layer_kernel(sizes, dims, *refs):
    r = types.SimpleNamespace(**dict(zip(INS + OUTS + WORK, refs)))
    nb, na, head, heads, experts, ff, top = dims
    net = Net(sizes, r.send, r.recv)
    me = net.me
    b, a, y, c = me["b"], me["a"], me["y"], me["c"]
    tok, part = r.xc.shape[1], r.xc.shape[2]
    half, col, model, width, sub = tok // 2, nb * tok, nb * part, heads * head, part // na
    scale = head**-0.5
    mine = pl.ds(pl.multiple_of(c * half, half), half)
    own_lane = pl.ds(pl.multiple_of(b * part, part), part)
    head_lane = pl.ds(pl.multiple_of(b * head, head), head)
    core, across = net.near(c=1), net.near(y=1)
    b_peers = [net.near(b=k) for k in range(1, nb)]
    a_peers = [net.near(a=k) for k in range(1, na)]
    group = [
        net.near(b=i, y=j, c=k)
        for i in range(nb) for j in range(2) for k in range(2) if i or j or k
    ]
    tp_peers = [net.near(y=j, c=k) for j in range(2) for k in range(2) if j or k]
    sent = []
    local_used = [0]

    def rows_of(i):
        return pl.ds(pl.multiple_of(i * tok, tok), tok)

    def lane_of(place):
        return pl.ds(pl.multiple_of(place * part, part), part)

    def move(source, target):
        copy = pltpu.make_async_copy(source, target, r.local.at[local_used[0]])
        local_used[0] += 1
        copy.start()
        return copy

    def ship(source, target, place):
        copy = net.copy(source, target, place)
        copy.start()
        sent.append(copy)
        return copy

    def arrive(copies):
        for copy in copies:
            copy.wait_recv()

    def drain(copies):
        for copy in copies:
            copy.wait_send()
            sent[:] = [other for other in sent if other is not copy]

    tok_here = move(r.tok, r.gin)
    w_here = [move(w, r.wqkv.at[j, a]) for j, w in ((1, r.wk_in), (2, r.wv_in), (0, r.wq_in))]
    stage_copy = move(r.wd_in, r.stage)
    late_here = [move(r.wo_in, r.wo.at[a]), move(r.cot.at[:, own_lane], r.cotc.at[b])]
    net.greet(group + [net.near(b=j, a=k) for j in range(nb) for k in range(1, na)])

    r.cols_own[...] = jnp.zeros_like(r.cols_own)
    r.cols_own[0:experts, :] = r.router_in[...].astype(f32)
    r.cols_own[experts : experts + 1, :] = r.gain_in_a[...].astype(f32).reshape(1, sub)
    r.cols_own[experts + 1 : experts + 2, :] = r.gain_in_f[...].astype(f32).reshape(1, sub)
    r.gains[0:1, :] = r.gain_q[...].astype(f32)
    r.gains[1:2, :] = r.gain_k[...].astype(f32)
    r.gains[2:3, :] = r.speed_in[...]
    r.rows_own[...] = jnp.zeros_like(r.rows_own)
    r.rows_own[1 : 1 + top, :] = r.ids_in[...].astype(f32)
    r.rows_own[3:4, :] = r.docs_in[...].astype(f32)

    exchange = [net.pick(2, 3, 0, 1), net.pick(3, 2, 1, 0), net.pick(1, 0, 3, 2)]

    quarter = half // 2
    fourth = pl.ds(pl.multiple_of(c * half + y * quarter, quarter), quarter)

    def to_quarters(source, target):
        return [
            ship(source.at[fourth, lane_of(d)], target.at[b, fourth, :], {"b": d})
            for d in exchange
        ]

    def over_a(source, target):
        return [ship(source, target.at[a], place) for place in a_peers]

    def onward(copies, target, rows, place):
        more = []
        for source_b, copy in zip(exchange, copies):
            copy.wait_recv()
            block = target.at[source_b, rows, :]
            more.append(ship(block, block, place))
        return more

    x_copies = to_quarters(r.tok, r.xc)
    cols_copies = over_a(r.cols_own, r.cols_all)
    r.cols_all[a] = r.cols_own[...]
    kv_weights = over_a(r.wk_in, r.wqkv.at[1]) + over_a(r.wv_in, r.wqkv.at[2])
    q_weights = over_a(r.wq_in, r.wqkv.at[0])
    tok_here.wait()
    square_columns = []
    for s in range(tok // 64):
        piece = r.gin[s * 64 : (s + 1) * 64, :].astype(f32)
        square_columns.append(jnp.sum(piece * piece, axis=1, keepdims=True))
    squares = transpose_columns([jnp.concatenate(square_columns, axis=0)], tok)[0:1, :]
    which8 = lax.broadcasted_iota(jnp.int32, (8, tok), 0)
    r.rows_own[0:1, :] = lax.rsqrt(squares / model + eps)
    rows_copies = [ship(r.rows_own, r.rows_all.at[a, b], place) for place in b_peers]
    rows_far = [
        ship(r.rows_own, r.rows_all.at[a, b], net.near(b=j, a=k))
        for j in range(nb) for k in range(1, na)
    ]
    r.rows_all[a, b] = r.rows_own[...]
    r.xc[b] = r.gin[:, own_lane]
    cot_copies = to_quarters(r.cot, r.cotc)
    wo_copies = over_a(r.wo_in, r.wo)

    def relayout(target):
        step = 32

        @pl.loop(0, sub // step)
        def _(n):
            rows = pl.ds(pl.multiple_of(n * step, step), step)
            turned = jnp.swapaxes(r.stage[rows].astype(f32), 0, 1)
            for e in range(experts):
                target[a, rows, e * ff : (e + 1) * ff] = turned[e].astype(bf16)

    stage_copy.wait()
    relayout(r.wd)
    wd_copies = over_a(r.wd.at[a], r.wd)
    stage_copy = move(r.wg_in, r.stage)

    lane_index = lax.broadcasted_iota(jnp.int32, (tok, head), 1)
    row_index = lax.broadcasted_iota(jnp.int32, (tok, head), 0)

    @pl.loop(0, nb)
    def _(i):
        place = ((i * na + a) * tok + row_index).astype(f32)
        angle = place * r.gains[2:3, :]
        r.cos_tab[rows_of(i), :] = jnp.cos(angle)
        turned = jnp.sin(angle)
        r.sin_tab[rows_of(i), :] = jnp.where(lane_index < head // 2, -turned, turned)

    x_y = onward(x_copies, r.xc, fourth, across)
    x_more = onward(x_y, r.xc, mine, core)
    arrive(rows_copies + cols_copies + x_more)
    arrive(kv_weights)
    for copy in w_here:
        copy.wait()
    for k in range(na):
        r.cols_sum[:, k * sub : (k + 1) * sub] = r.cols_all[k]
    gain_in = r.cols_sum[experts : experts + 1, :]
    for i in range(nb):
        columns = jnp.transpose(r.rows_all[a, i])
        r.ids[i] = columns
        r.hn[i] = (r.xc[i].astype(f32) * columns[:, 0:1] * gain_in).astype(bf16)

    def weight(j):
        return r.wqkv[j].reshape(part, width)

    @pl.loop(0, nb)
    def _(i):
        for j in (1, 2):
            term = dot(r.hn[i], weight(j)).astype(bf16)
            for h in range(heads):
                piece = term[:, h * head : (h + 1) * head]
                r.pkv[h, rows_of(i), (j - 1) * head : j * head] = piece

    kv_sum = net.reduce(r.pkv, r.gkv)
    cot_y = onward(cot_copies, r.cotc, fourth, across)
    arrive(q_weights)

    @pl.loop(0, nb)
    def _(i):
        term = dot(r.hn[i], weight(0)).astype(bf16)
        for h in range(heads):
            r.pq[h, rows_of(i), :] = term[:, h * head : (h + 1) * head]

    stage_copy.wait()
    relayout(r.wg)
    low, high = (pl.ds(k * experts * ff // 2, experts * ff // 2) for k in range(2))

    def half_over_a(array, lane):
        return [ship(array.at[a, :, lane], array.at[a, :, lane], place) for place in a_peers]

    wg_copies = half_over_a(r.wg, low)
    stage_copy = move(r.wu_in, r.stage)
    kv_sum.inner()
    q_sum = net.reduce(r.pq, r.gq)
    stage_copy.wait()
    relayout(r.wu)
    q_sum.inner()
    cot_more = onward(cot_y, r.cotc, mine, core)
    kv_sum.wait()

    @pl.loop(0, nb)
    def _(i):
        rows = rows_of(i)
        both = kv_sum.total(rows)
        r.raw[rows, head:] = both
        keys = both[:, :head]
        normed = keys * head_norm(keys) * r.gains[1:2, :]
        r.kv[a, rows, :head] = rope(normed, r.cos_tab[rows, :], r.sin_tab[rows, :]).astype(bf16)
        r.kv[a, rows, head:] = both[:, head:].astype(bf16)

    kv_copies = over_a(r.kv.at[a], r.kv)
    wg_copies += half_over_a(r.wg, high)
    wu_copies = over_a(r.wu.at[a], r.wu)
    arrive(wd_copies + cot_more)
    for copy in late_here:
        copy.wait()

    def chosen(left, weights, d, put):
        columns = r.ids[d]
        values = [jnp.zeros((tok, ff), f32) for k in range(top)]
        for e in range(experts):
            term = dot(left, weights[:, :, e * ff : (e + 1) * ff].reshape(part, ff))
            for k in range(top):
                values[k] = jnp.where(columns[:, 1 + k : 2 + k] == e, term, values[k])
        for k in range(top):
            put(k, values[k].astype(bf16))

    groups = ff // head

    @pl.loop(0, nb)
    def _(i):
        def put(k, value):
            for g in range(groups):
                r.pcd[k, i, g * tok : (g + 1) * tok, :] = value[:, g * head : (g + 1) * head]

        chosen(r.cotc[i], r.wd, i, put)

    cd_sums = [net.reduce(r.pcd.at[0], r.gcd.at[0])]
    arrive(rows_far)
    for i in range(nb):
        for j in range(na):
            r.docs[j, :, i * tok : (i + 1) * tok] = r.rows_all[j, i][3:4, :]
    q_sum.wait()

    @pl.loop(0, nb)
    def _(i):
        rows = rows_of(i)
        query = q_sum.total(rows)
        r.raw[rows, :head] = query
        normed = query * head_norm(query) * r.gains[0:1, :]
        r.q_rot[rows, :] = rope(normed, r.cos_tab[rows, :], r.sin_tab[rows, :]).astype(bf16)

    cd_sums[0].inner()

    deep = 2 if na <= 2 else 1

    def deep_rows(i):
        return pl.ds(pl.multiple_of(i * deep * tok, deep * tok), deep * tok)

    def deep_ids(i):
        return r.ids[pl.ds(i * deep, deep)].reshape(deep * tok, 8)

    def attend(block, first, last):
        @pl.loop(0, nb)
        def _(i):
            rows = rows_of(i)
            columns = r.ids[i]
            scores = dot(r.q_rot[rows, :], r.kv[block, :, :head], NT) * scale
            scores = jnp.where(columns[:, 3:4] == r.docs[block], scores, negative)
            most = jnp.max(scores, axis=1, keepdims=True)
            if not first:
                before = r.stat[rows, 0:1]
                most = jnp.maximum(before, most)
            terms = jnp.exp(scores - most)
            total = jnp.sum(terms, axis=1, keepdims=True)
            mixed = dot(terms.astype(bf16), r.kv[block, :, head:])
            if not first:
                fade = jnp.exp(before - most)
                total = r.stat[rows, 1:2] * fade + total
                mixed = r.head_acc[rows, :] * fade + mixed
            if last:
                r.ho[rows, head_lane] = (mixed * (1.0 / total)).astype(bf16)
                r.stat[rows, 2:3] = most + jnp.log(total)
            else:
                r.stat[rows, 0:1] = most
                r.stat[rows, 1:2] = total
                r.head_acc[rows, :] = mixed

    attend(a, True, na == 1)
    for k in range(1, na):
        kv_copies[k - 1].wait_recv()
        attend(lax.rem(a + na - k, na), False, k == na - 1)

    def head_block(array, i, start, size):
        return array.at[pl.ds(start, size), pl.ds(pl.multiple_of(i * head, head), head)]

    cuts = [0, nb - 1, nb]

    def ho_half(s):
        start, size = cuts[s] * tok, (cuts[s + 1] - cuts[s]) * tok
        return net.spread(lambda i: head_block(r.ho, i, start, size), start=s == 0)

    ho_lines = [ho_half(0)]
    arrive(wo_copies)
    ho_lines.append(ho_half(1))
    ho_lines[1].after(ho_lines[0])

    mixer = TwoLevel(net, r.acc, r.sendc, r.recvc, r.sendy, r.recvy, 1)
    for s in range(2):
        if s == 0:
            ho_lines[0].take(ho_lines[0].order[1])
            ho_lines[0].take(ho_lines[0].order[2])
        else:
            ho_lines[1].take_all()
            for k in range(1, top):
                cd_sums.append(net.reduce(r.pcd.at[k], r.gcd.at[k]))
        for i in range(cuts[s], cuts[s + 1]):
            term = dot(r.ho[i * tok : (i + 1) * tok, :], r.wo[...].reshape(part, width), NT)
            mixer.put(i, 0, term, i)
        for i in range(cuts[s], cuts[s + 1]):
            mixer.onward(i, 0, i)
    for group_sum in cd_sums[1:]:
        group_sum.inner()
    gain_mid = r.cols_sum[experts + 1 : experts + 2, :]
    router = r.cols_sum[...].astype(bf16)
    last_copies = []
    for i in range(nb):
        value = r.xc[i, mine, :].astype(f32) + mixer.total(i, 0)
        r.hidden[i] = value
        piece = (value * gain_mid).astype(bf16)
        r.scaled[i, mine, :] = piece
        logits = dot(router, piece, NT)
        squares = jnp.sum(value * value, axis=1, keepdims=True)
        squares = jnp.transpose(jnp.broadcast_to(squares, (half, 128)))[:1, :]
        which = lax.broadcasted_iota(jnp.int32, logits.shape, 0)
        r.small[i, :, mine] = jnp.where(which == experts, squares, logits)
        for array in (r.scaled.at[i, mine, :], r.small.at[i, :, mine]):
            last_copies.append(ship(array, array, core))
    arrive(wg_copies + wu_copies + last_copies)
    mixer.finish()
    kv_sum.finish()
    q_sum.finish()

    small_copies = [ship(r.small.at[p["b"]], r.small_in.at[b], p) for p in b_peers]
    r.small_in[b] = r.small[b]

    def make(d):
        for j, w in enumerate((r.wg, r.wu)):

            def put(k, value, j=j):
                r.pkv[d, (2 * k + j) * tok : (2 * k + j + 1) * tok, :] = value

            chosen(r.scaled[d], w, d, put)

    gu_sum = net.reduce(r.pkv, r.gkv, make)
    gu_sum.inner()
    make(b)
    arrive(small_copies)
    for group_sum in cd_sums:
        group_sum.wait()
    gu_sum.wait()
    total = jnp.sum(r.small_in[...], axis=0)
    r_mid = lax.rsqrt(total[experts : experts + 1] / model + eps)
    logits = total[:experts] * r_mid
    terms = jnp.exp(logits - jnp.max(logits, axis=0, keepdims=True))
    probs = terms / jnp.sum(terms, axis=0, keepdims=True)
    which = lax.broadcasted_iota(jnp.int32, probs.shape, 0).astype(f32)
    picks = [r.rows_own[1 + k : 2 + k] == which for k in range(top)]
    combine = [jnp.sum(jnp.where(pick, probs, 0.0), axis=0, keepdims=True) for pick in picks]
    table = jnp.where(which8 == 0, r_mid, 0.0)
    for k in range(top):
        table = jnp.where(which8 == 1 + k, combine[k], table)
    columns = jnp.transpose(table)
    r_col = columns[:, 0:1]
    columns_back = []
    inner = jnp.zeros((tok, 1), f32)
    for k in range(top):
        gate = gu_sum.total(slice((2 * k) * tok, (2 * k + 1) * tok)) * r_col
        up = gu_sum.total(slice((2 * k + 1) * tok, (2 * k + 2) * tok)) * r_col
        back = jnp.concatenate(
            [
                cd_sums[k].total(slice(g * tok, (g + 1) * tok))
                for g in range(groups)
            ],
            axis=1,
        )
        sig = 1.0 / (1.0 + jnp.exp(-gate))
        silu = gate * sig
        act = silu * up
        weighed = columns[:, 1 + k : 2 + k]
        d_act = weighed * back
        d_gate = d_act * up * (sig * (1.0 + gate * (1.0 - sig)))
        d_up = d_act * silu
        for j, value in enumerate((weighed * act, d_gate * r_col, d_up * r_col)):
            r.pay[b, :, (top * j + k) * ff : (top * j + k + 1) * ff] = value.astype(bf16)
        columns_back.append(jnp.sum(act * back, axis=1, keepdims=True))
        inner = inner + jnp.sum(d_gate * gate + d_up * up, axis=1, keepdims=True)

    pay_line = net.spread(lambda i: r.pay.at[i, :, pl.ds(top * ff, 2 * top * ff)])
    act_line = net.spread(lambda i: r.pay.at[i, :, pl.ds(0, top * ff)], start=False)
    rank = y * sizes["c"] + c
    r.pair[rank] = transpose_columns(columns_back + [inner], tok)
    arrive([ship(r.pair.at[rank], r.pair.at[rank], place) for place in tp_peers])
    sums = r.pair[0] + r.pair[1] + r.pair[2] + r.pair[3]
    d_probs = jnp.zeros_like(probs)
    for k in range(top):
        d_probs = d_probs + jnp.where(picks[k], sums[k : k + 1], 0.0)
    d_logits = probs * (d_probs - jnp.sum(probs * d_probs, axis=0, keepdims=True))
    inner_row = sums[top : top + 1] + jnp.sum(d_logits * logits, axis=0, keepdims=True)
    r.late_small[b, 0:8, :] = d_logits * r_mid
    r.late_small[b, 8:16, :] = jnp.broadcast_to(r_mid * r_mid * inner_row / model, (8, tok))
    late_copies = [ship(r.late_small.at[b], r.late_small.at[b], place) for place in b_peers]

    mixer = TwoLevel(net, r.acc, r.sendc, r.recvc, r.sendy, r.recvy, 2)
    pieces = experts * ff // width
    by_piece = width // ff

    def expand(j, i, e):
        columns = r.ids[i]
        value = jnp.zeros((tok, ff), f32)
        for k in range(top):
            taken = r.pay[i, :, (top * j + k) * ff : (top * j + k + 1) * ff].astype(f32)
            value = jnp.where(columns[:, 1 + k : 2 + k] == e, taken, value)
        return value.astype(bf16)

    def use(i):
        def widen(j):
            for e in range(experts):
                g, h = e // by_piece, e % by_piece
                r.wide[j, g * tok : (g + 1) * tok, h * ff : (h + 1) * ff] = expand(j, i, e)

        def times(j, w):
            total = 0.0
            for g in range(pieces):
                piece = w[:, :, g * width : (g + 1) * width].reshape(part, width)
                total = total + dot(r.wide[j, g * tok : (g + 1) * tok, :], piece, NT)
            return total

        widen(1)
        widen(2)
        mixer.put(i, 0, times(1, r.wg) + times(2, r.wu), 0)
        mixer.onward(i, 0, 0)

    @pl.loop(0, nb)
    def _(n):
        index = b
        for k in range(nb - 1):
            index = jnp.where(n == k + 1, pay_line.order[k], index)

        @pl.when(n > 0)
        def _():
            pay_line.take(index)

        @pl.when(n == jnp.where(act_line.inner, 1, 2))
        def _():
            act_line.begin()

        use(index)

    drain(wd_copies + wg_copies + wu_copies)
    gu_sum.finish()

    def to_a(source, target):
        return [ship(source.at[p["a"]], target.at[k], p) for k, p in enumerate(a_peers)]

    def expert_grad(j, left, target):
        @pl.loop(0, experts)
        def _(e):
            for i in range(nb):
                r.pkv[0, i * tok : (i + 1) * tok, :] = expand(j, i, e)
            grad = dot(left[...].reshape(col, part), r.pkv[0], TN).astype(bf16)
            lane = pl.ds(pl.multiple_of(e * ff, ff), ff)
            for k in range(na):
                target[k, :, lane] = grad[k * sub : (k + 1) * sub, :]

    expert_grad(1, r.scaled, r.wg)
    pending = to_a(r.wg, r.gate_in)
    results = [move(r.wg.at[a], r.gate_own)]
    arrive(late_copies)
    which16 = lax.broadcasted_iota(jnp.int32, (16, tok), 0)
    ffn_part = jnp.zeros((1, part), f32)
    attn_copies = []
    for i in range(nb):
        columns = jnp.transpose(r.late_small[i, :, mine])
        d_log = jnp.where(which16[:, :half] < experts, r.late_small[i, :, mine], 0.0).astype(bf16)
        mid = mixer.total(i, 0) + dot(d_log, router, TN)
        value = r.hidden[i]
        grad = r.cotc[i, mine, :].astype(f32) + gain_mid * mid - value * columns[:, 8:9]
        r.d_attn[i, mine, :] = grad.astype(bf16)
        attn_copies.append(ship(r.d_attn.at[i, mine, :], r.d_attn.at[i, mine, :], core))
        ffn_part = ffn_part + jnp.sum(mid * value, axis=0, keepdims=True)
        r.d_hidden[i] = grad
    act_line.take(act_line.order[0])
    arrive(attn_copies)

    @pl.loop(0, nb)
    def _(i):
        term = dot(r.d_attn[i], r.wo[...].reshape(part, width)).astype(bf16)
        for h in range(heads):
            r.pq[h, rows_of(i), :] = term[:, h * head : (h + 1) * head]

    heads_sum = net.reduce(r.pq, r.gq)

    expert_grad(2, r.scaled, r.wu)
    heads_sum.inner()

    act_line.take(act_line.order[1])
    act_line.take(act_line.order[2])

    @pl.loop(0, nb)
    def _(i):
        total = 0.0
        for e in range(experts):
            r.pkv[1, 0:tok, :] = expand(0, i, e)
            piece = r.wd[:, :, e * ff : (e + 1) * ff].reshape(part, ff)
            total = total + dot(r.pkv[1, 0:tok, :], piece, NT)
        mixer.put(i, 1, total, 1)
        mixer.onward(i, 1, 1)

    term = dot(r.d_attn[...].reshape(col, part), r.ho[...], TN).astype(bf16)
    r.gout[...] = term.reshape(na, sub, width)
    pending += to_a(r.gout, r.gout_in)
    extra = 0.0
    for i in range(nb):
        d_log = jnp.where(which16 < experts, r.late_small[i], 0.0).astype(bf16)
        extra = extra + dot(d_log, r.scaled[i])
    which_row = lax.broadcasted_iota(jnp.int32, (16, part), 0)
    r.extra_own[...] = jnp.where(which_row == experts + 1, ffn_part, extra)
    for i in range(nb):
        r.out_half[i] = (r.hidden[i] + mixer.total(i, 1)).astype(bf16)
    heads_sum.wait()
    out_copies = [
        ship(r.out_half.at[p["b"]], r.block_out.at[mine, own_lane], p) for p in b_peers
    ]
    r.block_out[mine, own_lane] = r.out_half[b]

    r.gain_acc[...] = jnp.zeros_like(r.gain_acc)

    @pl.loop(0, nb)
    def _(i):
        rows = rows_of(i)
        cot = heads_sum.total(rows).astype(bf16)
        r.pq[b, rows, :] = cot
        delta = jnp.sum(cot.astype(f32) * r.ho[rows, head_lane].astype(f32), axis=1, keepdims=True)
        r.stat[rows, 4:5] = delta

    def attend_back(block, first, last, start, stop):
        @pl.loop(start // deep, stop // deep)
        def _(i):
            rows = deep_rows(i)
            columns = deep_ids(i)
            query, cot = r.q_rot[rows, :], r.pq[b, rows, :]
            keys, values = r.kv[block, :, :head], r.kv[block, :, head:]
            scores = dot(query, keys, NT) * scale
            keep = columns[:, 3:4] == r.docs[block]
            probs = jnp.where(keep, jnp.exp(scores - r.stat[rows, 2:3]), 0.0)
            d_scores = (probs * (dot(cot, values, NT) - r.stat[rows, 4:5])).astype(bf16)
            key_term = dot(d_scores, query, TN) * scale
            value_term = dot(probs.astype(bf16), cot, TN)

            @pl.when(i == 0)
            def _():
                r.dkv_acc[:, :head] = key_term
                r.dkv_acc[:, head:] = value_term

            @pl.when(i > 0)
            def _():
                r.dkv_acc[:, :head] += key_term
                r.dkv_acc[:, head:] += value_term

            grad = dot(d_scores, keys) * scale
            if not first:
                grad = r.head_acc[rows, :] + grad
            if not last:
                r.head_acc[rows, :] = grad
            else:
                source = r.raw[rows, :head]
                grad, gain_part = unrope(
                    grad, source, r.gains[0:1, :], r.cos_tab[rows, :], r.sin_tab[rows, :]
                )
                r.gain_acc[0:1, :] += gain_part
                r.wide[0, rows, head_lane] = grad.astype(bf16)
                r.stat[rows, 3:4] = jnp.sum(grad * source, axis=1, keepdims=True)

    kv_back = []
    for k in range(1, na):
        attend_back(lax.rem(a + k, na), k == 1, False, 0, nb)
        r.dkv_send[k - 1] = r.dkv_acc[...].astype(bf16)
        kv_back.append(ship(r.dkv_send.at[k - 1], r.dkv_in.at[k - 1], a_peers[k - 1]))
    pending += to_a(r.wu, r.up_in)
    results.append(move(r.wu.at[a], r.up_own))
    q_lines = []
    for s in range(2):
        attend_back(a, na == 1, True, s * (nb // 2), (s + 1) * (nb // 2))
        q_lines.append(
            net.spread(lambda i, s=s: head_block(r.wide.at[0], i, s * (col // 2), col // 2))
        )
    out_more = []
    for k, copy in zip(range(1, nb), out_copies):
        lane = lane_of(lax.rem(b + nb - k, nb))
        copy.wait_recv()
        out_more.append(ship(r.block_out.at[mine, lane], r.block_out.at[mine, lane], core))
    out_more.append(ship(r.block_out.at[mine, own_lane], r.block_out.at[mine, own_lane], core))
    for line in q_lines:
        line.take(line.order[0])
    arrive(kv_back)

    @pl.loop(0, nb)
    def _(i):
        rows = rows_of(i)
        both = r.dkv_acc[rows, :]
        for k in range(na - 1):
            both = both + r.dkv_in[k, rows, :].astype(f32)
        source = r.raw[rows, head : 2 * head]
        grad, gain_part = unrope(
            both[:, :head], source, r.gains[1:2, :], r.cos_tab[rows, :], r.sin_tab[rows, :]
        )
        r.gain_acc[1:2, :] += gain_part
        value_grad = both[:, head:]
        r.wide[1, rows, head_lane] = grad.astype(bf16)
        r.wide[2, rows, head_lane] = value_grad.astype(bf16)
        r.stat[rows, 3:4] += jnp.sum(
            grad * source + value_grad * r.raw[rows, 2 * head :], axis=1, keepdims=True
        )

    def kv_piece(s):
        return net.spread(
            lambda i: head_block(r.wide.at[1], i, s * tok, tok),
            lambda i: head_block(r.wide.at[2], i, s * tok, tok),
            start=s == 0,
        )

    kv_lines = [kv_piece(s) for s in range(nb)]
    place16 = (b * 2 + y) * 2 + c
    r.s4[place16] = transpose_columns([r.stat[i * tok : (i + 1) * tok, 3:4] for i in range(nb)], tok)
    r.s4[place16, 4:6, 0:head] = r.gain_acc[0:2, :]
    s4_copies = [ship(r.s4.at[place16], r.s4.at[place16], place) for place in group]

    def weight_grad(j):
        grad = dot(r.hn[...].reshape(col, part), r.wide[j], TN).astype(bf16)
        r.gsend[j] = grad.reshape(na, sub, width)
        return to_a(r.gsend.at[j], r.gin_w.at[j])

    expert_grad(0, r.cotc, r.wd)
    pending += to_a(r.wd, r.down_in)
    results.append(move(r.wd.at[a], r.down_own))
    for line in q_lines:
        line.take(line.order[1])
        line.take(line.order[2])
    pending += weight_grad(0)
    mixer_in = TwoLevel(net, r.acc, r.sendc, r.recvc, r.sendy, r.recvy, 1)
    mixer.finish()
    arrive(s4_copies)
    for i in range(nb):
        if i < nb - 1:
            kv_lines[i + 1].after(kv_lines[i])
        else:
            kv_lines[i].take(kv_lines[i].order[0])
        kv_lines[i].take(kv_lines[i].order[1])
        kv_lines[i].take(kv_lines[i].order[2])
        rows = slice(i * tok, (i + 1) * tok)
        term = dot(r.wide[0, rows, :], weight(0), NT) + dot(r.wide[1, rows, :], weight(1), NT)
        mixer_in.put(i, 0, term + dot(r.wide[2, rows, :], weight(2), NT), i)
        mixer_in.onward(i, 0, i)
    sums = r.s4[0]
    for k in range(1, 4 * nb):
        sums = sums + r.s4[k]
    inner_columns = jnp.transpose(sums)
    attn_part = jnp.zeros((1, part), f32)
    in_hops = []
    base_in = net.used
    net.used += nb

    def in_hop(d, slot):
        return pltpu.make_async_remote_copy(
            src_ref=r.out_half.at[d],
            dst_ref=r.gin.at[mine, own_lane],
            send_sem=r.send.at[base_in + d],
            recv_sem=r.recv.at[base_in + slot],
            device_id={"b": jnp.int32(d)},
            device_id_type=MESH,
        )

    drain(out_copies)
    for i in range(nb):
        d_in = mixer_in.total(i, 0)
        r_col = r.ids[i, mine, 0:1]
        inner = jnp.where(
            c == 0, inner_columns[:half, i : i + 1], inner_columns[half:, i : i + 1]
        )
        x = r.xc[i, mine, :].astype(f32)
        scaled = d_in * r_col
        grad = r.d_hidden[i] + scaled * gain_in - x * (r_col * r_col * inner / model)
        attn_part = attn_part + jnp.sum(scaled * x, axis=0, keepdims=True)
        r.out_half[i] = grad.astype(bf16)

        @pl.when(b == i)
        def _():
            r.gin[mine, own_lane] = r.out_half[i]

        @pl.when(b != i)
        def _():
            in_hop(i, b).start()

    r.extra_own[...] = jnp.where(which_row == experts + 2, attn_part, r.extra_own[...])
    tail_copy = ship(r.extra_own, r.extra_in, core)
    pending += weight_grad(1)
    pending += weight_grad(2)
    tail_copy.wait_recv()
    shared = (which_row == experts + 1) | (which_row == experts + 2)
    r.tail_all[a] = r.extra_own[...] + jnp.where(shared, r.extra_in[...], 0.0)
    r.tail_all[a, experts + 3 : experts + 5, 0:head] = sums[4:6, 0:head]
    tail_copies = over_a(r.tail_all.at[a], r.tail_all)
    in_more = []
    for k in range(1, nb):
        place = lax.rem(b + k, nb)
        lane = lane_of(place)
        pltpu.make_async_remote_copy(
            src_ref=r.gin.at[mine, lane],
            dst_ref=r.gin.at[mine, lane],
            send_sem=r.send.at[base_in + place],
            recv_sem=r.recv.at[base_in + place],
            device_id=core,
            device_id_type=MESH,
        ).wait_recv()
        in_more.append(ship(r.gin.at[mine, lane], r.gin.at[mine, lane], core))
    in_more.append(ship(r.gin.at[mine, own_lane], r.gin.at[mine, own_lane], core))
    arrive(out_more)
    results.append(move(r.block_out, r.out_rows))
    arrive(pending)
    for j in range(4):
        mine_here = r.gsend[j, a] if j < 3 else r.gout[a]
        total = mine_here.astype(f32)
        for k in range(na - 1):
            came = r.gin_w[j, k] if j < 3 else r.gout_in[k]
            total = total + came.astype(f32)
        r.proj[j] = total
    results.append(move(r.proj, r.proj_out))
    arrive(tail_copies)
    r.tail[...] = jnp.sum(r.tail_all[...], axis=0)
    arrive(in_more)
    results.append(move(r.gin, r.in_rows))
    mixer_in.finish()
    for line in [heads_sum, pay_line, act_line] + cd_sums + ho_lines + q_lines + kv_lines:
        line.finish()
    for d in range(nb):

        @pl.when(b != d)
        def _():
            in_hop(d, b).wait_send()

    drain(list(sent))
    for copy in results:
        copy.wait()
    assert net.used <= r.send.shape[0] and local_used[0] <= r.local.shape[0]


def layer(sizes, dims, ins):
    nb, na, head, heads, experts, ff, top = dims
    tok, model = ins[0].shape
    part, col, half = model // nb, nb * tok, tok // 2
    sub, width, wide = part // na, heads * head, experts * ff
    others = max(na - 1, 1)
    shape = jax.ShapeDtypeStruct
    vmem, hbm = pl.BlockSpec(memory_space=pltpu.VMEM), pl.BlockSpec(memory_space=pl.ANY)
    outs = [
        shape((tok, model), bf16),
        shape((tok, model), bf16),
        shape((sub, wide), bf16),
        shape((sub, wide), bf16),
        shape((sub, wide), bf16),
        shape((others, sub, wide), bf16),
        shape((others, sub, wide), bf16),
        shape((others, sub, wide), bf16),
        shape((4, sub, width), f32),
        shape((16, part), f32),
    ]
    work = dict(
        xc=((nb, tok, part), bf16),
        cotc=((nb, tok, part), bf16),
        rows_all=((na, nb, 8, tok), f32),
        rows_own=((8, tok), f32),
        cols_own=((16, sub), f32),
        cols_all=((na, 16, sub), f32),
        cols_sum=((16, part), f32),
        wqkv=((3, na, sub, width), bf16),
        wo=((na, sub, width), bf16),
        wg=((na, sub, wide), bf16),
        wu=((na, sub, wide), bf16),
        wd=((na, sub, wide), bf16),
        stage=((sub, experts, ff), bf16),
        hn=((nb, tok, part), bf16),
        raw=((col, 3 * head), f32),
        q_rot=((col, head), bf16),
        kv=((na, col, 2 * head), bf16),
        stat=((col, 128), f32),
        ho=((col, width), bf16),
        cos_tab=((col, head), f32),
        sin_tab=((col, head), f32),
        pkv=((nb, col, 2 * head), bf16),
        gkv=((nb, col, 2 * head), bf16),
        pq=((nb, col, head), bf16),
        gq=((nb, col, head), bf16),
        pcd=((top, nb, ff // head * tok, head), bf16),
        gcd=((top, nb, ff // head * tok, head), bf16),
        acc=((nb, half, part), f32),
        sendc=((nb, half, 2 * part), bf16),
        recvc=((nb, half, 2 * part), bf16),
        sendy=((nb, half, 2 * part), bf16),
        recvy=((nb, half, 2 * part), bf16),
        hidden=((nb, half, part), f32),
        d_hidden=((nb, half, part), f32),
        scaled=((nb, tok, part), bf16),
        small=((nb, 16, tok), f32),
        small_in=((nb, 16, tok), f32),
        pay=((nb, tok, 3 * top * ff), bf16),
        wide=((3, col, width), bf16),
        pair=((4, 8, tok), f32),
        late_small=((nb, 16, tok), f32),
        extra_own=((16, part), f32),
        extra_in=((16, part), f32),
        d_attn=((nb, tok, part), bf16),
        out_half=((nb, half, part), bf16),
        block_out=((tok, model), bf16),
        head_acc=((col, head), f32),
        dkv_acc=((col, 2 * head), f32),
        dkv_send=((others, col, 2 * head), bf16),
        dkv_in=((others, col, 2 * head), bf16),
        gsend=((3, na, sub, width), bf16),
        gin_w=((3, others, sub, width), bf16),
        gout=((na, sub, width), bf16),
        gout_in=((others, sub, width), bf16),
        gin=((tok, model), bf16),
        s4=((4 * nb, 8, tok), f32),
        gain_acc=((8, head), f32),
        tail_all=((na, 16, part), f32),
        ids=((nb, tok, 8), f32),
        gains=((8, head), f32),
        docs=((na, 1, col), f32),
        proj=((4, sub, width), f32),
    )
    count = 224 + 28 * na
    scratch = [pltpu.VMEM(*work[name]) for name in WORK[:-3]] + [
        pltpu.SemaphoreType.DMA((count,)),
        pltpu.SemaphoreType.DMA((count,)),
        pltpu.SemaphoreType.DMA((24,)),
    ]
    return pl.pallas_call(
        functools.partial(layer_kernel, sizes, dims),
        out_shape=outs,
        in_specs=[hbm] * 9 + [vmem] * 8,
        out_specs=[hbm] * 9 + [vmem],
        scratch_shapes=scratch,
        compiler_params=pltpu.CompilerParams(
            collective_id=1, has_side_effects=True, vmem_limit_bytes=67043328
        ),
        name="layer",
    )(*ins)


def last_kernel(experts, ff, sub, *refs):
    out_rows, in_rows, owns, cames, proj = refs[0], refs[1], refs[2:5], refs[5:8], refs[8]
    tail, refs = refs[9], refs[10:]
    block_out, grad_in, grads, projections = refs[0], refs[1], refs[2:5], refs[5:9]
    router, gain_attn, gain_ffn, gain_q, gain_k = refs[9:]
    block_out[...] = out_rows[...]
    grad_in[...] = in_rows[...].astype(f32)
    for own, came, grad in zip(owns, cames, grads):
        for e in range(experts):
            lane = slice(e * ff, (e + 1) * ff)
            total = own[:, lane].astype(f32)
            for k in range(came.shape[0]):
                total = total + came[k, :, lane].astype(f32)
            grad[:, e, :] = total
    for j in range(4):
        projections[j][...] = proj[j]

    @pl.when(pl.program_id(0) == 0)
    def _():
        a = lax.axis_index("a")
        piece = tail[:, :sub]
        for k in range(1, tail.shape[1] // sub):
            piece = jnp.where(a == k, tail[:, k * sub : (k + 1) * sub], piece)
        router[...] = piece[:experts]
        gain_ffn[...] = piece[experts + 1 : experts + 2]
        gain_attn[...] = piece[experts + 2 : experts + 3]
        gain_q[...] = tail[experts + 3 : experts + 4, : gain_q.shape[1]]
        gain_k[...] = tail[experts + 4 : experts + 5, : gain_k.shape[1]]


def last(dims, ins):
    nb, na, head, heads, experts, ff, top = dims
    tok, model = ins[0].shape
    sub, wide = ins[2].shape
    others, width = ins[5].shape[0], ins[8].shape[2]
    steps = 4
    shape = jax.ShapeDtypeStruct
    rows = pl.BlockSpec((tok // steps, model), lambda i: (i, 0))
    own = pl.BlockSpec((sub // steps, wide), lambda i: (i, 0))
    came = pl.BlockSpec((others, sub // steps, wide), lambda i: (0, i, 0))
    grad = pl.BlockSpec((sub // steps, experts, ff), lambda i: (i, 0, 0))
    flat = pl.BlockSpec((sub // steps, width), lambda i: (i, 0))
    small = [shape((experts, sub), f32), shape((1, sub), f32), shape((1, sub), f32)]
    small += [shape((1, head), f32)] * 2
    return pl.pallas_call(
        functools.partial(last_kernel, experts, ff, sub),
        grid=(steps,),
        out_shape=[shape((tok, model), bf16), shape((tok, model), f32)]
        + [shape((sub, experts, ff), f32)] * 3
        + [shape((sub, width), f32)] * 4
        + small,
        in_specs=[rows, rows] + [own] * 3 + [came] * 3
        + [pl.BlockSpec((4, sub // steps, width), lambda i: (0, i, 0))]
        + [pl.BlockSpec(ins[9].shape, lambda i: (0, 0))],
        out_specs=[rows, rows] + [grad] * 3 + [flat] * 4
        + [pl.BlockSpec(item.shape, lambda i: (0, 0)) for item in small],
        name="last",
    )(*ins)


def on_device(
    sizes,
    tokens_in,
    doc_ids,
    expert_ids,
    attn_gain,
    q_gain,
    k_gain,
    w_query,
    w_key,
    w_value,
    w_output,
    ffn_gain,
    w_router,
    w_gate,
    w_up,
    w_down,
    cotangent,
):
    nb, na = sizes["b"], sizes["a"]
    tok, model = tokens_in.shape
    part = model // nb
    sub = part // na
    head = q_gain.shape[0]
    width = w_query.shape[1]
    heads = width // head
    experts, ff = w_gate.shape[1], w_gate.shape[2]
    top = expert_ids.shape[1]
    dims = (nb, na, head, heads, experts, ff, top)

    speed = theta ** (-2.0 * (np.arange(head) % (head // 2)) / head)
    parts = layer(
        sizes,
        dims,
        [
            tokens_in, cotangent, w_query, w_key, w_value, w_output, w_gate, w_up, w_down,
            expert_ids.T, doc_ids[None], w_router.T, attn_gain, ffn_gain, q_gain[None],
            k_gain[None], jnp.asarray(speed, f32)[None],
        ],
    )
    (
        block_out, grad_in, grad_gate, grad_up, grad_down, grad_query, grad_key, grad_value,
        grad_output, router, gain_attn, gain_ffn, gain_q, gain_k,
    ) = last(dims, parts)
    return (
        block_out,
        grad_in,
        gain_attn.reshape(sub),
        gain_q.reshape(head),
        gain_k.reshape(head),
        grad_query,
        grad_key,
        grad_value,
        grad_output,
        gain_ffn.reshape(sub),
        router.T,
        grad_gate,
        grad_up,
        grad_down,
    )


def solution(mesh):
    cp, tp = mesh.shape["cp"], mesh.shape["tp"]
    sizes = {"b": 4, "a": cp // 4, "y": 2, "c": tp // 2}
    split = Mesh(mesh.devices.reshape([sizes[axis] for axis in AXES]), AXES)
    cp, tp = ("b", "a"), ("y", "c")
    return jax.shard_map(
        functools.partial(on_device, sizes),
        mesh=split,
        in_specs=(
            P(cp, None),
            P(cp),
            P(cp, None),
            P(cp),
            P(),
            P(),
            P(cp, tp),
            P(cp, tp),
            P(cp, tp),
            P(cp, tp),
            P(cp),
            P(cp, None),
            P(cp, None, tp),
            P(cp, None, tp),
            P(cp, None, tp),
            P(cp, None),
        ),
        out_specs=(
            P(cp, None),
            P(cp, None),
            P(cp),
            P(),
            P(),
            P(cp, tp),
            P(cp, tp),
            P(cp, tp),
            P(cp, tp),
            P(cp),
            P(cp, None),
            P(cp, None, tp),
            P(cp, None, tp),
            P(cp, None, tp),
        ),
        check_vma=False,
    )
```

```python
import functools
import types

import jax
import jax.numpy as jnp
import numpy as np
from jax import lax
from jax.experimental import pallas as pl
from jax.experimental.pallas import tpu as pltpu
from jax.sharding import Mesh
from jax.sharding import PartitionSpec as P

eps = 1e-05
theta = 50000.0
negative = -1e30
AXES = ("b", "a", "y", "c")
MESH = pl.DeviceIdType.MESH
bf16 = jnp.bfloat16
f32 = jnp.float32


NT = (((1,), (1,)), ((), ()))
TN = (((0,), (0,)), ((), ()))


def dot(left, right, dims=(((1,), (0,)), ((), ()))):
    return lax.dot_general(left, right, dims, preferred_element_type=f32)


class Net:
    def __init__(self, sizes, send, recv):
        self.sizes, self.send, self.recv, self.used = sizes, send, recv, 0
        self.me = {axis: lax.axis_index(axis) for axis in AXES}

    def near(self, **offs):
        return {axis: lax.rem(self.me[axis] + off, self.sizes[axis]) for axis, off in offs.items()}

    def copy(self, source, target, place):
        slot = self.used
        self.used += 1
        return pltpu.make_async_remote_copy(
            src_ref=source,
            dst_ref=target,
            send_sem=self.send.at[slot],
            recv_sem=self.recv.at[slot],
            device_id=place,
            device_id_type=MESH,
        )

    def greet(self, places):
        barrier = pltpu.get_barrier_semaphore()
        for place in places:
            pl.semaphore_signal(barrier, inc=1, device_id=place, device_id_type=MESH)
        pl.semaphore_wait(barrier, len(places))

    def pick(self, *values):
        result = values[-1]
        for i in range(len(values) - 2, -1, -1):
            result = jnp.where(self.me["b"] == i, values[i], result)
        return result

    def reduce(self, *args):
        return Reduce(self, *args)

    def spread(self, *blocks, start=True):
        return Spread(self, blocks, start)


class Reduce:
    def __init__(self, net, parts, got, make=None):
        self.net, self.parts, self.got = net, parts, got
        self.b = b = net.me["b"]
        self.base = net.used
        net.used += 4
        self.order = [3 - b, net.pick(2, 0, 3, 1), net.pick(1, 3, 0, 2)]
        for k in range(2):
            if make is not None:
                make(self.order[k])
            self.hop(self.order[k]).start()
        if make is not None:
            make(self.order[2])

    def hop(self, d):
        net, b = self.net, self.b
        far = ((b == 0) & (d == 3)) | ((b == 3) & (d == 0))
        beside = jnp.where(b == 0, 1, 2)
        target, slot = jnp.where(far, beside, d), jnp.where(far, beside, b)
        return pltpu.make_async_remote_copy(
            src_ref=self.parts.at[d],
            dst_ref=self.got.at[slot],
            send_sem=net.send.at[self.base + d],
            recv_sem=net.recv.at[self.base + slot],
            device_id={"b": target},
            device_id_type=MESH,
        )

    def came(self, i):
        net = self.net
        return pltpu.make_async_remote_copy(
            src_ref=self.got.at[i],
            dst_ref=self.got.at[i],
            send_sem=net.send.at[self.base + i],
            recv_sem=net.recv.at[self.base + i],
            device_id=net.near(b=1),
            device_id_type=MESH,
        )

    def inner(self):
        b, d = self.b, self.order[2]

        @pl.when((b == 1) | (b == 2))
        def _():
            self.came(b).wait_recv()
            rows = self.parts.shape[1]
            step = 256 if rows % 256 == 0 else rows

            @pl.loop(0, rows // step)
            def _(i):
                sl = pl.ds(pl.multiple_of(i * step, step), step)
                total = self.parts[d, sl, :].astype(f32) + self.got[b, sl, :].astype(f32)
                self.parts[d, sl, :] = total.astype(bf16)

        self.hop(d).start()

    def wait(self):
        for i in range(4):

            @pl.when((self.b != i) & (jnp.abs(self.b - i) <= 2))
            def _():
                self.came(i).wait_recv()

    def total(self, *index):
        b = self.b
        value = self.parts[(b,) + index].astype(f32)
        for i in range(4):
            valid = (b != i) & (jnp.abs(b - i) <= 2)
            value = value + jnp.where(valid, self.got[(i,) + index].astype(f32), 0.0)
        return value

    def finish(self):
        for d in range(4):

            @pl.when(self.b != d)
            def _():
                self.hop(d).wait_send()


class Spread:
    def __init__(self, net, blocks, start):
        self.net, self.blocks = net, blocks
        self.b = b = net.me["b"]
        self.base = net.used
        net.used += 4 * len(blocks)
        self.targets = [net.pick(2, 3, 0, 1), net.pick(1, 0, 3, 2), net.pick(2, 2, 1, 1)]
        self.order = [net.pick(1, 3, 0, 2), net.pick(2, 0, 3, 1), net.pick(3, 2, 1, 0)]
        self.inner = (b == 1) | (b == 2)
        if start:
            self.begin()

    def begin(self):
        for k, target in enumerate(self.targets):
            if k < 2:
                for j in range(len(self.blocks)):
                    self.hop(self.b, target, target, j).start()
            else:

                @pl.when(self.inner)
                def _():
                    for j in range(len(self.blocks)):
                        self.hop(self.b, target, target, j).start()

    def hop(self, i, target, slot, j):
        net, count = self.net, len(self.blocks)
        return pltpu.make_async_remote_copy(
            src_ref=self.blocks[j](i),
            dst_ref=self.blocks[j](i),
            send_sem=net.send.at[self.base + slot * count + j],
            recv_sem=net.recv.at[self.base + i * count + j],
            device_id={"b": target},
            device_id_type=MESH,
        )

    def take(self, i):
        b = self.b
        onward = ((b == 1) & (i == 3)) | ((b == 2) & (i == 0))
        for j in range(len(self.blocks)):
            self.hop(i, self.net.near(b=1)["b"], b, j).wait_recv()

            @pl.when(onward)
            def _():
                self.hop(i, jnp.where(b == 1, 0, 3), b, j).start()

    def take_all(self):
        for i in self.order:
            self.take(i)

    def finish(self):
        b = self.b
        for k, target in enumerate(self.targets):
            for j in range(len(self.blocks)):
                if k < 2:
                    self.hop(b, target, target, j).wait_send()
                else:

                    @pl.when(self.inner)
                    def _():
                        self.hop(b, target, target, j).wait_send()
                        self.hop(b, jnp.where(b == 1, 0, 3), b, j).wait_send()


def rope(values, cos_tab, sin_tab):
    return values * cos_tab + pltpu.roll(values, values.shape[1] // 2, 1) * sin_tab


def head_norm(values):
    return lax.rsqrt(jnp.mean(values * values, axis=1, keepdims=True) + eps)


def unrope(grad, raw, gain, cos_tab, sin_tab):
    factor = head_norm(raw)
    normed = raw * factor
    turned = grad * cos_tab + pltpu.roll(grad * sin_tab, grad.shape[1] // 2, 1)
    gain_part = jnp.sum(turned * normed, axis=0, keepdims=True)
    inner = turned * gain
    slope = jnp.mean(raw * inner, axis=1, keepdims=True)
    return factor * inner - raw * (factor * factor * factor * slope), gain_part


class TwoLevel:
    def __init__(self, net, acc, sendc, recvc, sendy, recvy):
        self.net, self.acc = net, acc
        self.sendc, self.recvc, self.sendy, self.recvy = sendc, recvc, sendy, recvy
        self.base = net.used
        net.used += 16
        self.part = acc.shape[2]
        self.half = acc.shape[1]

    def lane(self, j):
        return slice(j * self.part, (j + 1) * self.part)

    def hop(self, i, j, level):
        net = self.net
        source, target = ((self.sendc, self.recvc), (self.sendy, self.recvy))[level]
        slot = self.base + 8 * level + 2 * i + j
        lane = pl.ds(j * self.part, self.part)
        return pltpu.make_async_remote_copy(
            src_ref=source.at[i, :, lane],
            dst_ref=target.at[i, :, lane],
            send_sem=net.send.at[slot],
            recv_sem=net.recv.at[slot],
            device_id=net.near(c=1) if level == 0 else net.near(y=1),
            device_id_type=MESH,
        )

    def put(self, i, j, term, k):
        first = self.net.me["c"] == 0
        low, high = term[: self.half], term[self.half :]
        self.acc[k] = jnp.where(first, low, high)
        self.sendc[i, :, self.lane(j)] = jnp.where(first, high, low).astype(bf16)
        self.hop(i, j, 0).start()

    def onward(self, i, j, k):
        self.hop(i, j, 0).wait_recv()
        total = self.acc[k] + self.recvc[i, :, self.lane(j)].astype(f32)
        self.sendy[i, :, self.lane(j)] = total.astype(bf16)
        self.hop(i, j, 1).start()

    def total(self, i, j):
        self.hop(i, j, 1).wait_recv()
        lane = self.lane(j)
        return self.sendy[i, :, lane].astype(f32) + self.recvy[i, :, lane].astype(f32)

    def finish(self, kinds=(0,)):
        for i in range(4):
            for j in kinds:
                self.hop(i, j, 0).wait_send()
                self.hop(i, j, 1).wait_send()


def transpose_columns(columns, rows):
    lane = lax.broadcasted_iota(jnp.int32, (rows, 128), 1)
    table = jnp.zeros((rows, 128), f32)
    for k, column in enumerate(columns):
        table = jnp.where(lane == k, column, table)
    return jnp.transpose(table)[:8, :]


INS = (
    "tok", "cot", "wq_in", "wk_in", "wv_in", "wo_in", "wg_in", "wu_in", "wd_in", "ids_in",
    "docs_in", "router_in", "gain_in_a", "gain_in_f", "gain_q", "gain_k", "speed_in",
)
OUTS = (
    "out_rows", "in_rows", "gate_own", "up_own", "down_own", "gate_in", "up_in", "down_in",
    "proj_out", "tail",
)
WORK = (
    "xc", "cotc", "rows_all", "rows_own", "cols_own", "cols_all", "cols_sum", "wqkv", "wo",
    "wg", "wu", "wd", "stage", "hn", "raw", "q_rot", "kv", "stat", "ho", "cos_tab", "sin_tab",
    "pkv", "gkv", "pq", "gq", "pcd", "gcd", "acc", "sendc", "recvc", "sendy", "recvy", "hidden", "d_hidden", "scaled",
    "small", "small_in", "pay", "wide", "pair", "late_small", "extra_own", "extra_in", "d_attn",
    "out_half", "block_out", "head_acc", "dkv_acc", "dkv_send", "dkv_in", "gsend", "gin_w",
    "gout", "gout_in", "gin", "s4", "gain_acc", "tail_all", "gains", "ids", "docs", "proj",
    "send", "recv", "local",
)


def layer_kernel(sizes, dims, *refs):
    r = types.SimpleNamespace(**dict(zip(INS + OUTS + WORK, refs)))
    nb, na, head, heads, experts, ff, top = dims
    net = Net(sizes, r.send, r.recv)
    me = net.me
    b, a, y, c = me["b"], me["a"], me["y"], me["c"]
    tok, part = r.xc.shape[1], r.xc.shape[2]
    half, col, model, width, sub = tok // 2, nb * tok, nb * part, heads * head, part // na
    scale = head**-0.5
    mine = pl.ds(pl.multiple_of(c * half, half), half)
    own_lane = pl.ds(pl.multiple_of(b * part, part), part)
    head_lane = pl.ds(pl.multiple_of(b * head, head), head)
    core, across = net.near(c=1), net.near(y=1)
    b_peers = [net.near(b=k) for k in range(1, nb)]
    a_peers = [net.near(a=k) for k in range(1, na)]
    group = [
        net.near(b=i, y=j, c=k)
        for i in range(nb) for j in range(2) for k in range(2) if i or j or k
    ]
    tp_peers = [net.near(y=j, c=k) for j in range(2) for k in range(2) if j or k]
    sent = []
    local_used = [0]

    def rows_of(i):
        return pl.ds(pl.multiple_of(i * tok, tok), tok)

    def lane_of(place):
        return pl.ds(pl.multiple_of(place * part, part), part)

    def move(source, target):
        copy = pltpu.make_async_copy(source, target, r.local.at[local_used[0]])
        local_used[0] += 1
        copy.start()
        return copy

    def ship(source, target, place):
        copy = net.copy(source, target, place)
        copy.start()
        sent.append(copy)
        return copy

    def arrive(copies):
        for copy in copies:
            copy.wait_recv()

    def drain(copies):
        for copy in copies:
            copy.wait_send()
            sent[:] = [other for other in sent if other is not copy]

    tok_here = move(r.tok, r.gin)
    w_here = [move(w, r.wqkv.at[j, a]) for j, w in ((1, r.wk_in), (2, r.wv_in), (0, r.wq_in))]
    stage_copy = move(r.wd_in, r.stage)
    late_here = [move(r.wo_in, r.wo.at[a]), move(r.cot.at[:, own_lane], r.cotc.at[b])]
    net.greet(group + [net.near(b=j, a=k) for j in range(nb) for k in range(1, na)])

    r.cols_own[...] = jnp.zeros_like(r.cols_own)
    r.cols_own[0:experts, :] = r.router_in[...].astype(f32)
    r.cols_own[experts : experts + 1, :] = r.gain_in_a[...].astype(f32).reshape(1, sub)
    r.cols_own[experts + 1 : experts + 2, :] = r.gain_in_f[...].astype(f32).reshape(1, sub)
    r.gains[0:1, :] = r.gain_q[...].astype(f32)
    r.gains[1:2, :] = r.gain_k[...].astype(f32)
    r.gains[2:3, :] = r.speed_in[...]
    r.rows_own[...] = jnp.zeros_like(r.rows_own)
    r.rows_own[1 : 1 + top, :] = r.ids_in[...].astype(f32)
    r.rows_own[3:4, :] = r.docs_in[...].astype(f32)

    exchange = [net.pick(2, 3, 0, 1), net.pick(3, 2, 1, 0), net.pick(1, 0, 3, 2)]

    quarter = half // 2
    fourth = pl.ds(pl.multiple_of(c * half + y * quarter, quarter), quarter)

    def to_quarters(source, target):
        return [
            ship(source.at[fourth, lane_of(d)], target.at[b, fourth, :], {"b": d})
            for d in exchange
        ]

    def over_a(source, target):
        return [ship(source, target.at[a], place) for place in a_peers]

    def onward(copies, target, rows, place):
        more = []
        for source_b, copy in zip(exchange, copies):
            copy.wait_recv()
            block = target.at[source_b, rows, :]
            more.append(ship(block, block, place))
        return more

    x_copies = to_quarters(r.tok, r.xc)
    cols_copies = over_a(r.cols_own, r.cols_all)
    r.cols_all[a] = r.cols_own[...]
    kv_weights = over_a(r.wk_in, r.wqkv.at[1]) + over_a(r.wv_in, r.wqkv.at[2])
    q_weights = over_a(r.wq_in, r.wqkv.at[0])
    tok_here.wait()
    square_columns = []
    for s in range(tok // 64):
        piece = r.gin[s * 64 : (s + 1) * 64, :].astype(f32)
        square_columns.append(jnp.sum(piece * piece, axis=1, keepdims=True))
    squares = transpose_columns([jnp.concatenate(square_columns, axis=0)], tok)[0:1, :]
    which8 = lax.broadcasted_iota(jnp.int32, (8, tok), 0)
    r.rows_own[0:1, :] = lax.rsqrt(squares / model + eps)
    rows_copies = [ship(r.rows_own, r.rows_all.at[a, b], place) for place in b_peers]
    rows_far = [
        ship(r.rows_own, r.rows_all.at[a, b], net.near(b=j, a=k))
        for j in range(nb) for k in range(1, na)
    ]
    r.rows_all[a, b] = r.rows_own[...]
    r.xc[b] = r.gin[:, own_lane]
    cot_copies = to_quarters(r.cot, r.cotc)
    wo_copies = over_a(r.wo_in, r.wo)

    def relayout(target):
        step = 32

        @pl.loop(0, sub // step)
        def _(n):
            rows = pl.ds(pl.multiple_of(n * step, step), step)
            turned = jnp.swapaxes(r.stage[rows].astype(f32), 0, 1)
            for e in range(experts):
                target[a, rows, e * ff : (e + 1) * ff] = turned[e].astype(bf16)

    stage_copy.wait()
    relayout(r.wd)
    wd_copies = over_a(r.wd.at[a], r.wd)
    stage_copy = move(r.wg_in, r.stage)

    lane_index = lax.broadcasted_iota(jnp.int32, (tok, head), 1)
    row_index = lax.broadcasted_iota(jnp.int32, (tok, head), 0)

    @pl.loop(0, nb)
    def _(i):
        place = ((i * na + a) * tok + row_index).astype(f32)
        angle = place * r.gains[2:3, :]
        r.cos_tab[rows_of(i), :] = jnp.cos(angle)
        turned = jnp.sin(angle)
        r.sin_tab[rows_of(i), :] = jnp.where(lane_index < head // 2, -turned, turned)

    x_y = onward(x_copies, r.xc, fourth, across)
    x_more = onward(x_y, r.xc, mine, core)
    arrive(rows_copies + cols_copies + x_more)
    arrive(kv_weights)
    for copy in w_here:
        copy.wait()
    for k in range(na):
        r.cols_sum[:, k * sub : (k + 1) * sub] = r.cols_all[k]
    gain_in = r.cols_sum[experts : experts + 1, :]
    for i in range(nb):
        columns = jnp.transpose(r.rows_all[a, i])
        r.ids[i] = columns
        r.hn[i] = (r.xc[i].astype(f32) * columns[:, 0:1] * gain_in).astype(bf16)

    def weight(j):
        return r.wqkv[j].reshape(part, width)

    @pl.loop(0, nb)
    def _(i):
        for j in (1, 2):
            term = dot(r.hn[i], weight(j)).astype(bf16)
            for h in range(heads):
                piece = term[:, h * head : (h + 1) * head]
                r.pkv[h, rows_of(i), (j - 1) * head : j * head] = piece

    kv_sum = net.reduce(r.pkv, r.gkv)
    cot_y = onward(cot_copies, r.cotc, fourth, across)
    arrive(q_weights)

    @pl.loop(0, nb)
    def _(i):
        term = dot(r.hn[i], weight(0)).astype(bf16)
        for h in range(heads):
            r.pq[h, rows_of(i), :] = term[:, h * head : (h + 1) * head]

    stage_copy.wait()
    relayout(r.wg)
    low, high = (pl.ds(k * experts * ff // 2, experts * ff // 2) for k in range(2))

    def half_over_a(array, lane):
        return [ship(array.at[a, :, lane], array.at[a, :, lane], place) for place in a_peers]

    wg_copies = half_over_a(r.wg, low)
    stage_copy = move(r.wu_in, r.stage)
    kv_sum.inner()
    q_sum = net.reduce(r.pq, r.gq)
    stage_copy.wait()
    relayout(r.wu)
    q_sum.inner()
    cot_more = onward(cot_y, r.cotc, mine, core)
    kv_sum.wait()

    @pl.loop(0, nb)
    def _(i):
        rows = rows_of(i)
        both = kv_sum.total(rows)
        r.raw[rows, head:] = both
        keys = both[:, :head]
        normed = keys * head_norm(keys) * r.gains[1:2, :]
        r.kv[a, rows, :head] = rope(normed, r.cos_tab[rows, :], r.sin_tab[rows, :]).astype(bf16)
        r.kv[a, rows, head:] = both[:, head:].astype(bf16)

    kv_copies = over_a(r.kv.at[a], r.kv)
    wg_copies += half_over_a(r.wg, high)
    wu_copies = over_a(r.wu.at[a], r.wu)
    arrive(wd_copies + cot_more)
    for copy in late_here:
        copy.wait()

    def chosen(left, weights, d, put):
        columns = r.ids[d]
        values = [jnp.zeros((tok, ff), f32) for k in range(top)]
        for e in range(experts):
            term = dot(left, weights[:, :, e * ff : (e + 1) * ff].reshape(part, ff))
            for k in range(top):
                values[k] = jnp.where(columns[:, 1 + k : 2 + k] == e, term, values[k])
        for k in range(top):
            put(k, values[k].astype(bf16))

    groups = ff // head

    @pl.loop(0, nb)
    def _(i):
        def put(k, value):
            for g in range(groups):
                r.pcd[k, i, g * tok : (g + 1) * tok, :] = value[:, g * head : (g + 1) * head]

        chosen(r.cotc[i], r.wd, i, put)

    cd_sums = [net.reduce(r.pcd.at[0], r.gcd.at[0])]
    arrive(rows_far)
    for i in range(nb):
        for j in range(na):
            r.docs[j, :, i * tok : (i + 1) * tok] = r.rows_all[j, i][3:4, :]
    q_sum.wait()

    @pl.loop(0, nb)
    def _(i):
        rows = rows_of(i)
        query = q_sum.total(rows)
        r.raw[rows, :head] = query
        normed = query * head_norm(query) * r.gains[0:1, :]
        r.q_rot[rows, :] = rope(normed, r.cos_tab[rows, :], r.sin_tab[rows, :]).astype(bf16)

    cd_sums[0].inner()

    deep = 2 if na <= 2 else 1

    def deep_rows(i):
        return pl.ds(pl.multiple_of(i * deep * tok, deep * tok), deep * tok)

    def deep_ids(i):
        return r.ids[pl.ds(i * deep, deep)].reshape(deep * tok, 8)

    def attend(block, first, last):
        @pl.loop(0, nb)
        def _(i):
            rows = rows_of(i)
            columns = r.ids[i]
            scores = dot(r.q_rot[rows, :], r.kv[block, :, :head], NT) * scale
            scores = jnp.where(columns[:, 3:4] == r.docs[block], scores, negative)
            most = jnp.max(scores, axis=1, keepdims=True)
            if not first:
                before = r.stat[rows, 0:1]
                most = jnp.maximum(before, most)
            terms = jnp.exp(scores - most)
            total = jnp.sum(terms, axis=1, keepdims=True)
            mixed = dot(terms.astype(bf16), r.kv[block, :, head:])
            if not first:
                fade = jnp.exp(before - most)
                total = r.stat[rows, 1:2] * fade + total
                mixed = r.head_acc[rows, :] * fade + mixed
            if last:
                r.ho[rows, head_lane] = (mixed * (1.0 / total)).astype(bf16)
                r.stat[rows, 2:3] = most + jnp.log(total)
            else:
                r.stat[rows, 0:1] = most
                r.stat[rows, 1:2] = total
                r.head_acc[rows, :] = mixed

    attend(a, True, na == 1)
    for k in range(1, na):
        kv_copies[k - 1].wait_recv()
        attend(lax.rem(a + na - k, na), False, k == na - 1)

    def head_block(array, i, start, size):
        return array.at[pl.ds(start, size), pl.ds(pl.multiple_of(i * head, head), head)]

    def chain(lines, i):
        lines[i].take(lines[i].order[0])
        if i + 2 < len(lines):
            lines[i + 2].begin()

    def rest(line):
        line.take(line.order[1])
        line.take(line.order[2])

    ho_lines = [
        net.spread(lambda i, s=s: head_block(r.ho, i, s * tok, tok), start=s < 2)
        for s in range(nb)
    ]
    arrive(wo_copies)

    mixer = TwoLevel(net, r.acc, r.sendc, r.recvc, r.sendy, r.recvy)
    for i in range(nb):
        chain(ho_lines, i)
        rest(ho_lines[i])
        if i == nb - 1:
            for k in range(1, top):
                cd_sums.append(net.reduce(r.pcd.at[k], r.gcd.at[k]))
        term = dot(r.ho[i * tok : (i + 1) * tok, :], r.wo[...].reshape(part, width), NT)
        mixer.put(i, 0, term, i)
        if i:
            mixer.onward(i - 1, 0, i - 1)
    mixer.onward(nb - 1, 0, nb - 1)
    for group_sum in cd_sums[1:]:
        group_sum.inner()
    gain_mid = r.cols_sum[experts + 1 : experts + 2, :]
    router = r.cols_sum[...].astype(bf16)
    last_copies = []
    for i in range(nb):
        value = r.xc[i, mine, :].astype(f32) + mixer.total(i, 0)
        r.hidden[i] = value
        piece = (value * gain_mid).astype(bf16)
        r.scaled[i, mine, :] = piece
        logits = dot(router, piece, NT)
        squares = jnp.sum(value * value, axis=1, keepdims=True)
        squares = jnp.transpose(jnp.broadcast_to(squares, (half, 128)))[:1, :]
        which = lax.broadcasted_iota(jnp.int32, logits.shape, 0)
        r.small[i, :, mine] = jnp.where(which == experts, squares, logits)
        for array in (r.scaled.at[i, mine, :], r.small.at[i, :, mine]):
            last_copies.append(ship(array, array, core))
    arrive(wg_copies + wu_copies + last_copies)
    mixer.finish()
    kv_sum.finish()
    q_sum.finish()

    small_copies = [ship(r.small.at[p["b"]], r.small_in.at[b], p) for p in b_peers]
    r.small_in[b] = r.small[b]

    def make(d):
        for j, w in enumerate((r.wg, r.wu)):

            def put(k, value, j=j):
                r.pkv[d, (2 * k + j) * tok : (2 * k + j + 1) * tok, :] = value

            chosen(r.scaled[d], w, d, put)

    gu_sum = net.reduce(r.pkv, r.gkv, make)
    gu_sum.inner()
    make(b)
    arrive(small_copies)
    for group_sum in cd_sums:
        group_sum.wait()
    gu_sum.wait()
    total = jnp.sum(r.small_in[...], axis=0)
    r_mid = lax.rsqrt(total[experts : experts + 1] / model + eps)
    logits = total[:experts] * r_mid
    terms = jnp.exp(logits - jnp.max(logits, axis=0, keepdims=True))
    probs = terms / jnp.sum(terms, axis=0, keepdims=True)
    which = lax.broadcasted_iota(jnp.int32, probs.shape, 0).astype(f32)
    picks = [r.rows_own[1 + k : 2 + k] == which for k in range(top)]
    combine = [jnp.sum(jnp.where(pick, probs, 0.0), axis=0, keepdims=True) for pick in picks]
    table = jnp.where(which8 == 0, r_mid, 0.0)
    for k in range(top):
        table = jnp.where(which8 == 1 + k, combine[k], table)
    columns = jnp.transpose(table)
    r_col = columns[:, 0:1]
    columns_back = []
    inner = jnp.zeros((tok, 1), f32)
    for k in range(top):
        gate = gu_sum.total(slice((2 * k) * tok, (2 * k + 1) * tok)) * r_col
        up = gu_sum.total(slice((2 * k + 1) * tok, (2 * k + 2) * tok)) * r_col
        back = jnp.concatenate(
            [
                cd_sums[k].total(slice(g * tok, (g + 1) * tok))
                for g in range(groups)
            ],
            axis=1,
        )
        sig = 1.0 / (1.0 + jnp.exp(-gate))
        silu = gate * sig
        act = silu * up
        weighed = columns[:, 1 + k : 2 + k]
        d_act = weighed * back
        d_gate = d_act * up * (sig * (1.0 + gate * (1.0 - sig)))
        d_up = d_act * silu
        for j, value in enumerate((weighed * act, d_gate * r_col, d_up * r_col)):
            r.pay[b, :, (top * j + k) * ff : (top * j + k + 1) * ff] = value.astype(bf16)
        columns_back.append(jnp.sum(act * back, axis=1, keepdims=True))
        inner = inner + jnp.sum(d_gate * gate + d_up * up, axis=1, keepdims=True)

    pay_line = net.spread(lambda i: r.pay.at[i, :, pl.ds(top * ff, 2 * top * ff)])
    act_lines = [
        net.spread(lambda i, k=k: r.pay.at[i, :, pl.ds(k * ff, ff)], start=False)
        for k in range(top)
    ]
    rank = y * sizes["c"] + c
    r.pair[rank] = transpose_columns(columns_back + [inner], tok)
    arrive([ship(r.pair.at[rank], r.pair.at[rank], place) for place in tp_peers])
    sums = r.pair[0] + r.pair[1] + r.pair[2] + r.pair[3]
    d_probs = jnp.zeros_like(probs)
    for k in range(top):
        d_probs = d_probs + jnp.where(picks[k], sums[k : k + 1], 0.0)
    d_logits = probs * (d_probs - jnp.sum(probs * d_probs, axis=0, keepdims=True))
    inner_row = sums[top : top + 1] + jnp.sum(d_logits * logits, axis=0, keepdims=True)
    r.late_small[b, 0:8, :] = d_logits * r_mid
    r.late_small[b, 8:16, :] = jnp.broadcast_to(r_mid * r_mid * inner_row / model, (8, tok))
    late_copies = [ship(r.late_small.at[b], r.late_small.at[b], place) for place in b_peers]

    mixer = TwoLevel(net, r.acc, r.sendc, r.recvc, r.sendy, r.recvy)
    pieces = experts * ff // width
    by_piece = width // ff

    def expand(j, i, e):
        columns = r.ids[i]
        value = jnp.zeros((tok, ff), f32)
        for k in range(top):
            taken = r.pay[i, :, (top * j + k) * ff : (top * j + k + 1) * ff].astype(f32)
            value = jnp.where(columns[:, 1 + k : 2 + k] == e, taken, value)
        return value.astype(bf16)

    def use(i):
        def widen(j):
            for e in range(experts):
                g, h = e // by_piece, e % by_piece
                r.wide[j, g * tok : (g + 1) * tok, h * ff : (h + 1) * ff] = expand(j, i, e)

        def times(j, w):
            total = 0.0
            for g in range(pieces):
                piece = w[:, :, g * width : (g + 1) * width].reshape(part, width)
                total = total + dot(r.wide[j, g * tok : (g + 1) * tok, :], piece, NT)
            return total

        widen(1)
        widen(2)
        mixer.put(i, 0, times(1, r.wg) + times(2, r.wu), 0)
        mixer.onward(i, 0, 0)

    @pl.loop(0, nb)
    def _(n):
        index = b
        for k in range(nb - 1):
            index = jnp.where(n == k + 1, pay_line.order[k], index)

        @pl.when(n > 0)
        def _():
            pay_line.take(index)

        @pl.when(n == jnp.where(pay_line.inner, 1, 3))
        def _():
            act_lines[0].begin()

        use(index)

    drain(wd_copies + wg_copies + wu_copies)
    gu_sum.finish()

    def to_a(source, target):
        return [ship(source.at[p["a"]], target.at[k], p) for k, p in enumerate(a_peers)]

    def expert_grad(j, left, target, part_of):
        @pl.loop(part_of * experts // 2, (part_of + 1) * experts // 2)
        def _(e):
            for i in range(nb):
                r.pkv[0, i * tok : (i + 1) * tok, :] = expand(j, i, e)
            grad = dot(left[...].reshape(col, part), r.pkv[0], TN).astype(bf16)
            lane = pl.ds(pl.multiple_of(e * ff, ff), ff)
            for k in range(na):
                target[k, :, lane] = grad[k * sub : (k + 1) * sub, :]

    def half_to_a(source, target, part_of):
        lane = (low, high)[part_of]
        return [
            ship(source.at[p["a"], :, lane], target.at[k, :, lane], p)
            for k, p in enumerate(a_peers)
        ]

    expert_grad(1, r.scaled, r.wg, 0)
    pending = half_to_a(r.wg, r.gate_in, 0)
    arrive(late_copies)
    which16 = lax.broadcasted_iota(jnp.int32, (16, tok), 0)
    ffn_part = jnp.zeros((1, part), f32)
    attn_copies = []
    for i in range(nb):
        columns = jnp.transpose(r.late_small[i, :, mine])
        d_log = jnp.where(which16[:, :half] < experts, r.late_small[i, :, mine], 0.0).astype(bf16)
        mid = mixer.total(i, 0) + dot(d_log, router, TN)
        value = r.hidden[i]
        grad = r.cotc[i, mine, :].astype(f32) + gain_mid * mid - value * columns[:, 8:9]
        r.d_attn[i, mine, :] = grad.astype(bf16)
        attn_copies.append(ship(r.d_attn.at[i, mine, :], r.d_attn.at[i, mine, :], core))
        ffn_part = ffn_part + jnp.sum(mid * value, axis=0, keepdims=True)
        r.d_hidden[i] = grad
    act_lines[0].take(act_lines[0].order[0])
    arrive(attn_copies)

    @pl.loop(0, nb)
    def _(i):
        term = dot(r.d_attn[i], r.wo[...].reshape(part, width)).astype(bf16)
        for h in range(heads):
            r.pq[h, rows_of(i), :] = term[:, h * head : (h + 1) * head]

    heads_sum = net.reduce(r.pq, r.gq)

    expert_grad(1, r.scaled, r.wg, 1)
    pending += half_to_a(r.wg, r.gate_in, 1)
    results = [move(r.wg.at[a], r.gate_own)]
    heads_sum.inner()
    expert_grad(2, r.scaled, r.wu, 0)

    def experts_out():
        for line in act_lines:
            rest(line)

        @pl.loop(0, nb)
        def _(i):
            total = 0.0
            for e in range(experts):
                r.pkv[1, 0:tok, :] = expand(0, i, e)
                piece = r.wd[:, :, e * ff : (e + 1) * ff].reshape(part, ff)
                total = total + dot(r.pkv[1, 0:tok, :], piece, NT)
            mixer.put(i, 1, total, i)

    term = dot(r.d_attn[...].reshape(col, part), r.ho[...], TN).astype(bf16)
    r.gout[...] = term.reshape(na, sub, width)
    pending += to_a(r.gout, r.gout_in)
    extra = 0.0
    for i in range(nb):
        d_log = jnp.where(which16 < experts, r.late_small[i], 0.0).astype(bf16)
        extra = extra + dot(d_log, r.scaled[i])
    which_row = lax.broadcasted_iota(jnp.int32, (16, part), 0)
    r.extra_own[...] = jnp.where(which_row == experts + 1, ffn_part, extra)
    heads_sum.wait()
    for line in act_lines[1:]:
        line.begin()

    r.gain_acc[...] = jnp.zeros_like(r.gain_acc)

    @pl.loop(0, nb)
    def _(i):
        rows = rows_of(i)
        cot = heads_sum.total(rows).astype(bf16)
        r.pq[b, rows, :] = cot
        delta = jnp.sum(cot.astype(f32) * r.ho[rows, head_lane].astype(f32), axis=1, keepdims=True)
        r.stat[rows, 4:5] = delta

    def attend_back(block, first, last, start, stop):
        @pl.loop(start // deep, stop // deep)
        def _(i):
            rows = deep_rows(i)
            columns = deep_ids(i)
            query, cot = r.q_rot[rows, :], r.pq[b, rows, :]
            keys, values = r.kv[block, :, :head], r.kv[block, :, head:]
            scores = dot(query, keys, NT) * scale
            keep = columns[:, 3:4] == r.docs[block]
            probs = jnp.where(keep, jnp.exp(scores - r.stat[rows, 2:3]), 0.0)
            d_scores = (probs * (dot(cot, values, NT) - r.stat[rows, 4:5])).astype(bf16)
            key_term = dot(d_scores, query, TN) * scale
            value_term = dot(probs.astype(bf16), cot, TN)

            @pl.when(i == 0)
            def _():
                r.dkv_acc[:, :head] = key_term
                r.dkv_acc[:, head:] = value_term

            @pl.when(i > 0)
            def _():
                r.dkv_acc[:, :head] += key_term
                r.dkv_acc[:, head:] += value_term

            grad = dot(d_scores, keys) * scale
            if not first:
                grad = r.head_acc[rows, :] + grad
            if not last:
                r.head_acc[rows, :] = grad
            else:
                source = r.raw[rows, :head]
                grad, gain_part = unrope(
                    grad, source, r.gains[0:1, :], r.cos_tab[rows, :], r.sin_tab[rows, :]
                )
                r.gain_acc[0:1, :] += gain_part
                r.wide[0, rows, head_lane] = grad.astype(bf16)
                r.stat[rows, 3:4] = jnp.sum(grad * source, axis=1, keepdims=True)

    kv_back = []
    for k in range(1, na):
        attend_back(lax.rem(a + k, na), k == 1, False, 0, nb)
        r.dkv_send[k - 1] = r.dkv_acc[...].astype(bf16)
        kv_back.append(ship(r.dkv_send.at[k - 1], r.dkv_in.at[k - 1], a_peers[k - 1]))
    for line in act_lines[1:]:
        line.take(line.order[0])
    pending += half_to_a(r.wu, r.up_in, 0)
    q_lines = []
    for s in range(2):
        attend_back(a, na == 1, True, s * (nb // 2), (s + 1) * (nb // 2))
        q_lines.append(
            net.spread(lambda i, s=s: head_block(r.wide.at[0], i, s * (col // 2), col // 2))
        )
    expert_grad(2, r.scaled, r.wu, 1)
    pending += half_to_a(r.wu, r.up_in, 1)
    results.append(move(r.wu.at[a], r.up_own))
    for line in q_lines:
        line.take(line.order[0])
    arrive(kv_back)

    @pl.loop(0, nb)
    def _(i):
        rows = rows_of(i)
        both = r.dkv_acc[rows, :]
        for k in range(na - 1):
            both = both + r.dkv_in[k, rows, :].astype(f32)
        source = r.raw[rows, head : 2 * head]
        grad, gain_part = unrope(
            both[:, :head], source, r.gains[1:2, :], r.cos_tab[rows, :], r.sin_tab[rows, :]
        )
        r.gain_acc[1:2, :] += gain_part
        value_grad = both[:, head:]
        r.wide[1, rows, head_lane] = grad.astype(bf16)
        r.wide[2, rows, head_lane] = value_grad.astype(bf16)
        r.stat[rows, 3:4] += jnp.sum(
            grad * source + value_grad * r.raw[rows, 2 * head :], axis=1, keepdims=True
        )

    place16 = (b * 2 + y) * 2 + c
    r.s4[place16] = transpose_columns([r.stat[i * tok : (i + 1) * tok, 3:4] for i in range(nb)], tok)
    r.s4[place16, 4:6, 0:head] = r.gain_acc[0:2, :]
    s4_copies = [ship(r.s4.at[place16], r.s4.at[place16], place) for place in group]

    def kv_piece(s):
        return net.spread(
            lambda i: head_block(r.wide.at[1], i, s * tok, tok),
            lambda i: head_block(r.wide.at[2], i, s * tok, tok),
            start=s < 2,
        )

    kv_lines = [kv_piece(s) for s in range(nb)]
    def weight_grad(j):
        grad = dot(r.hn[...].reshape(col, part), r.wide[j], TN).astype(bf16)
        r.gsend[j] = grad.reshape(na, sub, width)
        return to_a(r.gsend.at[j], r.gin_w.at[j])

    for line in q_lines:
        line.take(line.order[1])
        line.take(line.order[2])
    pending += weight_grad(0)
    mixer_in = TwoLevel(net, r.acc, r.sendc, r.recvc, r.sendy, r.recvy)
    mixer.finish()
    def in_term(i):
        rest(kv_lines[i])
        rows = slice(i * tok, (i + 1) * tok)
        term = dot(r.wide[0, rows, :], weight(0), NT) + dot(r.wide[1, rows, :], weight(1), NT)
        mixer_in.put(i, 0, term + dot(r.wide[2, rows, :], weight(2), NT), i)
        mixer_in.onward(i, 0, i)

    chain(kv_lines, 0)
    experts_out()
    chain(kv_lines, 1)
    for i in range(nb):
        mixer.onward(i, 1, i)
    expert_grad(0, r.cotc, r.wd, 0)
    pending += half_to_a(r.wd, r.down_in, 0)
    arrive(s4_copies)
    in_term(0)
    chain(kv_lines, 2)
    expert_grad(0, r.cotc, r.wd, 1)
    pending += half_to_a(r.wd, r.down_in, 1)
    results.append(move(r.wd.at[a], r.down_own))
    in_term(1)
    chain(kv_lines, 3)
    for j in range(nb):
        r.out_half[j] = (r.hidden[j] + mixer.total(j, 1)).astype(bf16)
    r.block_out[mine, own_lane] = r.out_half[b]
    in_term(2)
    in_term(3)
    out_rows = pl.ds(pl.multiple_of(y * quarter, quarter), quarter)
    out_copies = [
        ship(r.out_half.at[d, out_rows, :], r.block_out.at[fourth, own_lane], {"b": d})
        for d in exchange
    ]

    def lanes_onward(copies, rows, place):
        more = []
        for source_b, copy in zip(exchange, copies):
            copy.wait_recv()
            block = r.block_out.at[rows, lane_of(source_b)]
            more.append(ship(block, block, place))
        return more

    pending += weight_grad(1)
    pending += weight_grad(2)
    sums = r.s4[0]
    for k in range(1, 4 * nb):
        sums = sums + r.s4[k]
    inner_columns = jnp.transpose(sums)
    attn_part = jnp.zeros((1, part), f32)
    in_hops = []
    base_in = net.used
    net.used += nb

    def in_hop(d, slot):
        return pltpu.make_async_remote_copy(
            src_ref=r.d_attn.at[d, pl.ds(0, half), :],
            dst_ref=r.gin.at[mine, own_lane],
            send_sem=r.send.at[base_in + d],
            recv_sem=r.recv.at[base_in + slot],
            device_id={"b": jnp.int32(d)},
            device_id_type=MESH,
        )

    drain(attn_copies)
    for i in range(nb):
        d_in = mixer_in.total(i, 0)
        r_col = r.ids[i, mine, 0:1]
        inner = jnp.where(
            c == 0, inner_columns[:half, i : i + 1], inner_columns[half:, i : i + 1]
        )
        x = r.xc[i, mine, :].astype(f32)
        scaled = d_in * r_col
        grad = r.d_hidden[i] + scaled * gain_in - x * (r_col * r_col * inner / model)
        attn_part = attn_part + jnp.sum(scaled * x, axis=0, keepdims=True)
        r.d_attn[i, :half, :] = grad.astype(bf16)

        @pl.when(b == i)
        def _():
            r.gin[mine, own_lane] = r.d_attn[i, :half, :]

        @pl.when(b != i)
        def _():
            in_hop(i, b).start()

    r.extra_own[...] = jnp.where(which_row == experts + 2, attn_part, r.extra_own[...])
    tail_copy = ship(r.extra_own, r.extra_in, core)
    tail_copy.wait_recv()
    shared = (which_row == experts + 1) | (which_row == experts + 2)
    r.tail_all[a] = r.extra_own[...] + jnp.where(shared, r.extra_in[...], 0.0)
    r.tail_all[a, experts + 3 : experts + 5, 0:head] = sums[4:6, 0:head]
    tail_copies = over_a(r.tail_all.at[a], r.tail_all)
    out_y = lanes_onward(out_copies, fourth, across)
    in_more = []
    for k in range(1, nb):
        place = lax.rem(b + k, nb)
        lane = lane_of(place)
        pltpu.make_async_remote_copy(
            src_ref=r.gin.at[mine, lane],
            dst_ref=r.gin.at[mine, lane],
            send_sem=r.send.at[base_in + place],
            recv_sem=r.recv.at[base_in + place],
            device_id=core,
            device_id_type=MESH,
        ).wait_recv()
        in_more.append(ship(r.gin.at[mine, lane], r.gin.at[mine, lane], core))
    in_more.append(ship(r.gin.at[mine, own_lane], r.gin.at[mine, own_lane], core))
    out_more = lanes_onward(out_y, mine, core)
    block = r.block_out.at[mine, own_lane]
    out_more.append(ship(block, block, core))
    arrive(pending)
    for j in range(4):
        mine_here = r.gsend[j, a] if j < 3 else r.gout[a]
        total = mine_here.astype(f32)
        for k in range(na - 1):
            came = r.gin_w[j, k] if j < 3 else r.gout_in[k]
            total = total + came.astype(f32)
        r.proj[j] = total
    results.append(move(r.proj, r.proj_out))
    arrive(out_more)
    results.append(move(r.block_out, r.out_rows))
    arrive(tail_copies)
    r.tail[...] = jnp.sum(r.tail_all[...], axis=0)
    arrive(in_more)
    results.append(move(r.gin, r.in_rows))
    mixer_in.finish()
    mixer.finish((1,))
    for line in [heads_sum, pay_line] + act_lines + cd_sums + ho_lines + q_lines + kv_lines:
        line.finish()
    for d in range(nb):

        @pl.when(b != d)
        def _():
            in_hop(d, b).wait_send()

    drain(list(sent))
    for copy in results:
        copy.wait()
    assert net.used <= r.send.shape[0] and local_used[0] <= r.local.shape[0]


def layer(sizes, dims, ins):
    nb, na, head, heads, experts, ff, top = dims
    tok, model = ins[0].shape
    part, col, half = model // nb, nb * tok, tok // 2
    sub, width, wide = part // na, heads * head, experts * ff
    others = max(na - 1, 1)
    shape = jax.ShapeDtypeStruct
    vmem, hbm = pl.BlockSpec(memory_space=pltpu.VMEM), pl.BlockSpec(memory_space=pl.ANY)
    outs = [
        shape((tok, model), bf16),
        shape((tok, model), bf16),
        shape((sub, wide), bf16),
        shape((sub, wide), bf16),
        shape((sub, wide), bf16),
        shape((others, sub, wide), bf16),
        shape((others, sub, wide), bf16),
        shape((others, sub, wide), bf16),
        shape((4, sub, width), f32),
        shape((16, part), f32),
    ]
    work = dict(
        xc=((nb, tok, part), bf16),
        cotc=((nb, tok, part), bf16),
        rows_all=((na, nb, 8, tok), f32),
        rows_own=((8, tok), f32),
        cols_own=((16, sub), f32),
        cols_all=((na, 16, sub), f32),
        cols_sum=((16, part), f32),
        wqkv=((3, na, sub, width), bf16),
        wo=((na, sub, width), bf16),
        wg=((na, sub, wide), bf16),
        wu=((na, sub, wide), bf16),
        wd=((na, sub, wide), bf16),
        stage=((sub, experts, ff), bf16),
        hn=((nb, tok, part), bf16),
        raw=((col, 3 * head), f32),
        q_rot=((col, head), bf16),
        kv=((na, col, 2 * head), bf16),
        stat=((col, 128), f32),
        ho=((col, width), bf16),
        cos_tab=((col, head), f32),
        sin_tab=((col, head), f32),
        pkv=((nb, col, 2 * head), bf16),
        gkv=((nb, col, 2 * head), bf16),
        pq=((nb, col, head), bf16),
        gq=((nb, col, head), bf16),
        pcd=((top, nb, ff // head * tok, head), bf16),
        gcd=((top, nb, ff // head * tok, head), bf16),
        acc=((nb, half, part), f32),
        sendc=((nb, half, 2 * part), bf16),
        recvc=((nb, half, 2 * part), bf16),
        sendy=((nb, half, 2 * part), bf16),
        recvy=((nb, half, 2 * part), bf16),
        hidden=((nb, half, part), f32),
        d_hidden=((nb, half, part), f32),
        scaled=((nb, tok, part), bf16),
        small=((nb, 16, tok), f32),
        small_in=((nb, 16, tok), f32),
        pay=((nb, tok, 3 * top * ff), bf16),
        wide=((3, col, width), bf16),
        pair=((4, 8, tok), f32),
        late_small=((nb, 16, tok), f32),
        extra_own=((16, part), f32),
        extra_in=((16, part), f32),
        d_attn=((nb, tok, part), bf16),
        out_half=((nb, half, part), bf16),
        block_out=((tok, model), bf16),
        head_acc=((col, head), f32),
        dkv_acc=((col, 2 * head), f32),
        dkv_send=((others, col, 2 * head), bf16),
        dkv_in=((others, col, 2 * head), bf16),
        gsend=((3, na, sub, width), bf16),
        gin_w=((3, others, sub, width), bf16),
        gout=((na, sub, width), bf16),
        gout_in=((others, sub, width), bf16),
        gin=((tok, model), bf16),
        s4=((4 * nb, 8, tok), f32),
        gain_acc=((8, head), f32),
        tail_all=((na, 16, part), f32),
        ids=((nb, tok, 8), f32),
        gains=((8, head), f32),
        docs=((na, 1, col), f32),
        proj=((4, sub, width), f32),
    )
    count = 240 + 28 * na
    scratch = [pltpu.VMEM(*work[name]) for name in WORK[:-3]] + [
        pltpu.SemaphoreType.DMA((count,)),
        pltpu.SemaphoreType.DMA((count,)),
        pltpu.SemaphoreType.DMA((24,)),
    ]
    return pl.pallas_call(
        functools.partial(layer_kernel, sizes, dims),
        out_shape=outs,
        in_specs=[hbm] * 9 + [vmem] * 8,
        out_specs=[hbm] * 9 + [vmem],
        scratch_shapes=scratch,
        compiler_params=pltpu.CompilerParams(
            collective_id=1, has_side_effects=True, vmem_limit_bytes=67043328
        ),
        name="layer",
    )(*ins)


def last_kernel(experts, ff, sub, *refs):
    out_rows, in_rows, owns, cames, proj = refs[0], refs[1], refs[2:5], refs[5:8], refs[8]
    tail, refs = refs[9], refs[10:]
    block_out, grad_in, grads, projections = refs[0], refs[1], refs[2:5], refs[5:9]
    router, gain_attn, gain_ffn, gain_q, gain_k = refs[9:]
    block_out[...] = out_rows[...]
    grad_in[...] = in_rows[...].astype(f32)
    for own, came, grad in zip(owns, cames, grads):
        for e in range(experts):
            lane = slice(e * ff, (e + 1) * ff)
            total = own[:, lane].astype(f32)
            for k in range(came.shape[0]):
                total = total + came[k, :, lane].astype(f32)
            grad[:, e, :] = total
    for j in range(4):
        projections[j][...] = proj[j]

    @pl.when(pl.program_id(0) == 0)
    def _():
        a = lax.axis_index("a")
        piece = tail[:, :sub]
        for k in range(1, tail.shape[1] // sub):
            piece = jnp.where(a == k, tail[:, k * sub : (k + 1) * sub], piece)
        router[...] = piece[:experts]
        gain_ffn[...] = piece[experts + 1 : experts + 2]
        gain_attn[...] = piece[experts + 2 : experts + 3]
        gain_q[...] = tail[experts + 3 : experts + 4, : gain_q.shape[1]]
        gain_k[...] = tail[experts + 4 : experts + 5, : gain_k.shape[1]]


def last(dims, ins):
    nb, na, head, heads, experts, ff, top = dims
    tok, model = ins[0].shape
    sub, wide = ins[2].shape
    others, width = ins[5].shape[0], ins[8].shape[2]
    steps = 2
    shape = jax.ShapeDtypeStruct
    rows = pl.BlockSpec((tok // steps, model), lambda i: (i, 0))
    own = pl.BlockSpec((sub // steps, wide), lambda i: (i, 0))
    came = pl.BlockSpec((others, sub // steps, wide), lambda i: (0, i, 0))
    grad = pl.BlockSpec((sub // steps, experts, ff), lambda i: (i, 0, 0))
    flat = pl.BlockSpec((sub // steps, width), lambda i: (i, 0))
    small = [shape((experts, sub), f32), shape((1, sub), f32), shape((1, sub), f32)]
    small += [shape((1, head), f32)] * 2
    return pl.pallas_call(
        functools.partial(last_kernel, experts, ff, sub),
        grid=(steps,),
        out_shape=[shape((tok, model), bf16), shape((tok, model), f32)]
        + [shape((sub, experts, ff), f32)] * 3
        + [shape((sub, width), f32)] * 4
        + small,
        in_specs=[rows, rows] + [own] * 3 + [came] * 3
        + [pl.BlockSpec((4, sub // steps, width), lambda i: (0, i, 0))]
        + [pl.BlockSpec(ins[9].shape, lambda i: (0, 0))],
        out_specs=[rows, rows] + [grad] * 3 + [flat] * 4
        + [pl.BlockSpec(item.shape, lambda i: (0, 0)) for item in small],
        name="last",
    )(*ins)


def on_device(
    sizes,
    tokens_in,
    doc_ids,
    expert_ids,
    attn_gain,
    q_gain,
    k_gain,
    w_query,
    w_key,
    w_value,
    w_output,
    ffn_gain,
    w_router,
    w_gate,
    w_up,
    w_down,
    cotangent,
):
    nb, na = sizes["b"], sizes["a"]
    tok, model = tokens_in.shape
    part = model // nb
    sub = part // na
    head = q_gain.shape[0]
    width = w_query.shape[1]
    heads = width // head
    experts, ff = w_gate.shape[1], w_gate.shape[2]
    top = expert_ids.shape[1]
    dims = (nb, na, head, heads, experts, ff, top)

    speed = theta ** (-2.0 * (np.arange(head) % (head // 2)) / head)
    parts = layer(
        sizes,
        dims,
        [
            tokens_in, cotangent, w_query, w_key, w_value, w_output, w_gate, w_up, w_down,
            expert_ids.T, doc_ids[None], w_router.T, attn_gain, ffn_gain, q_gain[None],
            k_gain[None], jnp.asarray(speed, f32)[None],
        ],
    )
    (
        block_out, grad_in, grad_gate, grad_up, grad_down, grad_query, grad_key, grad_value,
        grad_output, router, gain_attn, gain_ffn, gain_q, gain_k,
    ) = last(dims, parts)
    return (
        block_out,
        grad_in,
        gain_attn.reshape(sub),
        gain_q.reshape(head),
        gain_k.reshape(head),
        grad_query,
        grad_key,
        grad_value,
        grad_output,
        gain_ffn.reshape(sub),
        router.T,
        grad_gate,
        grad_up,
        grad_down,
    )


def solution(mesh):
    cp, tp = mesh.shape["cp"], mesh.shape["tp"]
    sizes = {"b": 4, "a": cp // 4, "y": 2, "c": tp // 2}
    split = Mesh(mesh.devices.reshape([sizes[axis] for axis in AXES]), AXES)
    cp, tp = ("b", "a"), ("y", "c")
    return jax.shard_map(
        functools.partial(on_device, sizes),
        mesh=split,
        in_specs=(
            P(cp, None),
            P(cp),
            P(cp, None),
            P(cp),
            P(),
            P(),
            P(cp, tp),
            P(cp, tp),
            P(cp, tp),
            P(cp, tp),
            P(cp),
            P(cp, None),
            P(cp, None, tp),
            P(cp, None, tp),
            P(cp, None, tp),
            P(cp, None),
        ),
        out_specs=(
            P(cp, None),
            P(cp, None),
            P(cp),
            P(),
            P(),
            P(cp, tp),
            P(cp, tp),
            P(cp, tp),
            P(cp, tp),
            P(cp),
            P(cp, None),
            P(cp, None, tp),
            P(cp, None, tp),
            P(cp, None, tp),
        ),
        check_vma=False,
    )
```

```python
import functools
import types

import jax
import jax.numpy as jnp
import numpy as np
from jax import lax
from jax.experimental import pallas as pl
from jax.experimental.pallas import tpu as pltpu
from jax.sharding import Mesh
from jax.sharding import PartitionSpec as P

eps = 1e-05
theta = 50000.0
negative = -1e30
AXES = ("b", "a", "y", "c")
MESH = pl.DeviceIdType.MESH
bf16 = jnp.bfloat16
f32 = jnp.float32


NT = (((1,), (1,)), ((), ()))
TN = (((0,), (0,)), ((), ()))


def dot(left, right, dims=(((1,), (0,)), ((), ()))):
    return lax.dot_general(left, right, dims, preferred_element_type=f32)


class Net:
    def __init__(self, sizes, send, recv):
        self.sizes, self.send, self.recv, self.used = sizes, send, recv, 0
        self.me = {axis: lax.axis_index(axis) for axis in AXES}

    def near(self, **offs):
        return {axis: lax.rem(self.me[axis] + off, self.sizes[axis]) for axis, off in offs.items()}

    def copy(self, source, target, place):
        slot = self.used
        self.used += 1
        return pltpu.make_async_remote_copy(
            src_ref=source,
            dst_ref=target,
            send_sem=self.send.at[slot],
            recv_sem=self.recv.at[slot],
            device_id=place,
            device_id_type=MESH,
        )

    def greet(self, places):
        barrier = pltpu.get_barrier_semaphore()
        for place in places:
            pl.semaphore_signal(barrier, inc=1, device_id=place, device_id_type=MESH)
        pl.semaphore_wait(barrier, len(places))

    def pick(self, *values):
        result = values[-1]
        for i in range(len(values) - 2, -1, -1):
            result = jnp.where(self.me["b"] == i, values[i], result)
        return result

    def reduce(self, *args):
        return Reduce(self, *args)

    def spread(self, *blocks, start=True):
        return Spread(self, blocks, start)


class Reduce:
    def __init__(self, net, parts, got, make=None):
        self.net, self.parts, self.got = net, parts, got
        self.b = b = net.me["b"]
        self.base = net.used
        net.used += 4
        self.order = [3 - b, net.pick(2, 0, 3, 1), net.pick(1, 3, 0, 2)]
        if make is None:
            for k in range(2):
                self.hop(self.order[k]).start()
            return
        if net.sizes["a"] > 2:
            for k in range(3):
                make(self.order[k])
                if k < 2:
                    self.hop(self.order[k]).start()
            return

        @pl.loop(0, 3)
        def _(k):
            d = jnp.where(k == 0, self.order[0], jnp.where(k == 1, self.order[1], self.order[2]))
            make(d)

            @pl.when(k < 2)
            def _():
                self.hop(d).start()

    def hop(self, d):
        net, b = self.net, self.b
        far = ((b == 0) & (d == 3)) | ((b == 3) & (d == 0))
        beside = jnp.where(b == 0, 1, 2)
        target, slot = jnp.where(far, beside, d), jnp.where(far, beside, b)
        return pltpu.make_async_remote_copy(
            src_ref=self.parts.at[d],
            dst_ref=self.got.at[slot],
            send_sem=net.send.at[self.base + d],
            recv_sem=net.recv.at[self.base + slot],
            device_id={"b": target},
            device_id_type=MESH,
        )

    def came(self, i):
        net = self.net
        return pltpu.make_async_remote_copy(
            src_ref=self.got.at[i],
            dst_ref=self.got.at[i],
            send_sem=net.send.at[self.base + i],
            recv_sem=net.recv.at[self.base + i],
            device_id=net.near(b=1),
            device_id_type=MESH,
        )

    def inner(self):
        b, d = self.b, self.order[2]

        @pl.when((b == 1) | (b == 2))
        def _():
            self.came(b).wait_recv()
            rows = self.parts.shape[1]
            step = 256 if rows % 256 == 0 else rows

            @pl.loop(0, rows // step)
            def _(i):
                sl = pl.ds(pl.multiple_of(i * step, step), step)
                total = self.parts[d, sl, :].astype(f32) + self.got[b, sl, :].astype(f32)
                self.parts[d, sl, :] = total.astype(bf16)

        self.hop(d).start()

    def wait(self):
        for i in range(4):

            @pl.when((self.b != i) & (jnp.abs(self.b - i) <= 2))
            def _():
                self.came(i).wait_recv()

    def total(self, *index):
        b = self.b
        value = self.parts[(b,) + index].astype(f32)
        for i in range(4):
            valid = (b != i) & (jnp.abs(b - i) <= 2)
            value = value + jnp.where(valid, self.got[(i,) + index].astype(f32), 0.0)
        return value

    def finish(self):
        for d in range(4):

            @pl.when(self.b != d)
            def _():
                self.hop(d).wait_send()


class Spread:
    def __init__(self, net, blocks, start):
        self.net, self.blocks = net, blocks
        self.b = b = net.me["b"]
        self.base = net.used
        net.used += 4 * len(blocks)
        self.targets = [net.pick(2, 3, 0, 1), net.pick(1, 0, 3, 2), net.pick(2, 2, 1, 1)]
        self.order = [net.pick(1, 3, 0, 2), net.pick(2, 0, 3, 1), net.pick(3, 2, 1, 0)]
        self.inner = (b == 1) | (b == 2)
        if start:
            self.begin()

    def begin(self):
        for k, target in enumerate(self.targets):
            if k < 2:
                for j in range(len(self.blocks)):
                    self.hop(self.b, target, target, j).start()
            else:

                @pl.when(self.inner)
                def _():
                    for j in range(len(self.blocks)):
                        self.hop(self.b, target, target, j).start()

    def hop(self, i, target, slot, j):
        net, count = self.net, len(self.blocks)
        return pltpu.make_async_remote_copy(
            src_ref=self.blocks[j](i),
            dst_ref=self.blocks[j](i),
            send_sem=net.send.at[self.base + slot * count + j],
            recv_sem=net.recv.at[self.base + i * count + j],
            device_id={"b": target},
            device_id_type=MESH,
        )

    def take(self, i):
        b = self.b
        onward = ((b == 1) & (i == 3)) | ((b == 2) & (i == 0))
        for j in range(len(self.blocks)):
            self.hop(i, self.net.near(b=1)["b"], b, j).wait_recv()

            @pl.when(onward)
            def _():
                self.hop(i, jnp.where(b == 1, 0, 3), b, j).start()

    def take_all(self):
        for i in self.order:
            self.take(i)

    def finish(self):
        b = self.b
        for k, target in enumerate(self.targets):
            for j in range(len(self.blocks)):
                if k < 2:
                    self.hop(b, target, target, j).wait_send()
                else:

                    @pl.when(self.inner)
                    def _():
                        self.hop(b, target, target, j).wait_send()
                        self.hop(b, jnp.where(b == 1, 0, 3), b, j).wait_send()


def rope(values, cos_tab, sin_tab):
    return values * cos_tab + pltpu.roll(values, values.shape[1] // 2, 1) * sin_tab


def head_norm(values):
    return lax.rsqrt(jnp.mean(values * values, axis=1, keepdims=True) + eps)


def unrope(grad, raw, gain, cos_tab, sin_tab):
    factor = head_norm(raw)
    normed = raw * factor
    turned = grad * cos_tab + pltpu.roll(grad * sin_tab, grad.shape[1] // 2, 1)
    gain_part = jnp.sum(turned * normed, axis=0, keepdims=True)
    inner = turned * gain
    slope = jnp.mean(raw * inner, axis=1, keepdims=True)
    return factor * inner - raw * (factor * factor * factor * slope), gain_part


class TwoLevel:
    def __init__(self, net, acc, sendc, recvc, sendy, recvy, kinds):
        self.net, self.acc = net, acc
        self.sendc, self.recvc, self.sendy, self.recvy = sendc, recvc, sendy, recvy
        self.base = net.used
        self.kinds = kinds
        net.used += 8 * kinds
        self.part = acc.shape[2]
        self.half = acc.shape[1]

    def lane(self, j):
        return slice(j * self.part, (j + 1) * self.part)

    def hop(self, i, j, level):
        net = self.net
        source, target = ((self.sendc, self.recvc), (self.sendy, self.recvy))[level]
        slot = self.base + 4 * self.kinds * level + self.kinds * i + j
        lane = pl.ds(j * self.part, self.part)
        return pltpu.make_async_remote_copy(
            src_ref=source.at[i, :, lane],
            dst_ref=target.at[i, :, lane],
            send_sem=net.send.at[slot],
            recv_sem=net.recv.at[slot],
            device_id=net.near(c=1) if level == 0 else net.near(y=1),
            device_id_type=MESH,
        )

    def put(self, i, j, term, k):
        first = self.net.me["c"] == 0
        low, high = term[: self.half], term[self.half :]
        self.acc[k] = jnp.where(first, low, high)
        self.sendc[i, :, self.lane(j)] = jnp.where(first, high, low).astype(bf16)
        self.hop(i, j, 0).start()

    def onward(self, i, j, k):
        self.hop(i, j, 0).wait_recv()
        total = self.acc[k] + self.recvc[i, :, self.lane(j)].astype(f32)
        self.sendy[i, :, self.lane(j)] = total.astype(bf16)
        self.hop(i, j, 1).start()

    def total(self, i, j):
        self.hop(i, j, 1).wait_recv()
        lane = self.lane(j)
        return self.sendy[i, :, lane].astype(f32) + self.recvy[i, :, lane].astype(f32)

    def finish(self, kinds=(0,)):
        for i in range(4):
            for j in kinds:
                self.hop(i, j, 0).wait_send()
                self.hop(i, j, 1).wait_send()


def transpose_columns(columns, rows):
    lane = lax.broadcasted_iota(jnp.int32, (rows, 128), 1)
    table = jnp.zeros((rows, 128), f32)
    for k, column in enumerate(columns):
        table = jnp.where(lane == k, column, table)
    return jnp.transpose(table)[:8, :]


INS = (
    "tok", "cot", "wq_in", "wk_in", "wv_in", "wo_in", "wg_in", "wu_in", "wd_in", "ids_in",
    "docs_in", "router_in", "gain_in_a", "gain_in_f", "gain_q", "gain_k", "speed_in",
)
OUTS = (
    "out_rows", "in_rows", "gate_own", "up_own", "down_own", "gate_in", "up_in", "down_in",
    "proj_out", "tail",
)
WORK = (
    "xc", "cotc", "rows_all", "rows_own", "cols_own", "cols_all", "cols_sum", "wqkv", "wo",
    "wg", "wu", "wd", "stage", "hn", "raw", "q_rot", "kv", "stat", "ho", "cos_tab", "sin_tab",
    "pkv", "gkv", "pq", "gq", "pcd", "gcd", "acc", "sendc", "recvc", "sendy", "recvy", "hidden", "d_hidden", "scaled",
    "small", "small_in", "pay", "wide", "pair", "late_small", "extra_own", "extra_in", "d_attn",
    "out_half", "block_out", "head_acc", "dkv_acc", "dkv_send", "dkv_in", "gsend", "gin_w",
    "gout", "gout_in", "gin", "s4", "gain_acc", "tail_all", "gains", "ids", "docs", "proj",
    "send", "recv", "local",
)


def layer_kernel(sizes, dims, *refs):
    r = types.SimpleNamespace(**dict(zip(INS + OUTS + WORK, refs)))
    nb, na, head, heads, experts, ff, top = dims
    net = Net(sizes, r.send, r.recv)
    me = net.me
    b, a, y, c = me["b"], me["a"], me["y"], me["c"]
    tok, part = r.xc.shape[1], r.xc.shape[2]
    half, col, model, width, sub = tok // 2, nb * tok, nb * part, heads * head, part // na
    scale = head**-0.5
    mine = pl.ds(pl.multiple_of(c * half, half), half)
    own_lane = pl.ds(pl.multiple_of(b * part, part), part)
    head_lane = pl.ds(pl.multiple_of(b * head, head), head)
    core, across = net.near(c=1), net.near(y=1)
    b_peers = [net.near(b=k) for k in range(1, nb)]
    a_peers = [net.near(a=k) for k in range(1, na)]
    group = [
        net.near(b=i, y=j, c=k)
        for i in range(nb) for j in range(2) for k in range(2) if i or j or k
    ]
    tp_peers = [net.near(y=j, c=k) for j in range(2) for k in range(2) if j or k]
    sent = []
    local_used = [0]

    def rows_of(i):
        return pl.ds(pl.multiple_of(i * tok, tok), tok)

    def lane_of(place):
        return pl.ds(pl.multiple_of(place * part, part), part)

    def move(source, target):
        copy = pltpu.make_async_copy(source, target, r.local.at[local_used[0]])
        local_used[0] += 1
        copy.start()
        return copy

    def ship(source, target, place):
        copy = net.copy(source, target, place)
        copy.start()
        sent.append(copy)
        return copy

    def arrive(copies):
        for copy in copies:
            copy.wait_recv()

    def drain(copies):
        for copy in copies:
            copy.wait_send()
            sent[:] = [other for other in sent if other is not copy]

    tok_here = move(r.tok, r.gin)
    w_here = [move(w, r.wqkv.at[j, a]) for j, w in ((1, r.wk_in), (2, r.wv_in), (0, r.wq_in))]
    stage_copy = move(r.wd_in, r.stage)
    late_here = [move(r.wo_in, r.wo.at[a]), move(r.cot.at[:, own_lane], r.cotc.at[b])]
    net.greet(group + [net.near(b=j, a=k) for j in range(nb) for k in range(1, na)])

    r.cols_own[...] = jnp.zeros_like(r.cols_own)
    r.cols_own[0:experts, :] = r.router_in[...].astype(f32)
    r.cols_own[experts : experts + 1, :] = r.gain_in_a[...].astype(f32).reshape(1, sub)
    r.cols_own[experts + 1 : experts + 2, :] = r.gain_in_f[...].astype(f32).reshape(1, sub)
    r.gains[0:1, :] = r.gain_q[...].astype(f32)
    r.gains[1:2, :] = r.gain_k[...].astype(f32)
    r.gains[2:3, :] = r.speed_in[...]
    r.rows_own[...] = jnp.zeros_like(r.rows_own)
    r.rows_own[1 : 1 + top, :] = r.ids_in[...].astype(f32)
    r.rows_own[3:4, :] = r.docs_in[...].astype(f32)

    exchange = [net.pick(2, 3, 0, 1), net.pick(3, 2, 1, 0), net.pick(1, 0, 3, 2)]

    quarter = half // 2
    fourth = pl.ds(pl.multiple_of(c * half + y * quarter, quarter), quarter)

    def to_quarters(source, target):
        return [
            ship(source.at[fourth, lane_of(d)], target.at[b, fourth, :], {"b": d})
            for d in exchange
        ]

    def over_a(source, target):
        return [ship(source, target.at[a], place) for place in a_peers]

    def onward(copies, target, rows, place):
        more = []
        for source_b, copy in zip(exchange, copies):
            copy.wait_recv()
            block = target.at[source_b, rows, :]
            more.append(ship(block, block, place))
        return more

    x_copies = to_quarters(r.tok, r.xc)
    cols_copies = over_a(r.cols_own, r.cols_all)
    r.cols_all[a] = r.cols_own[...]
    kv_weights = over_a(r.wk_in, r.wqkv.at[1]) + over_a(r.wv_in, r.wqkv.at[2])
    q_weights = over_a(r.wq_in, r.wqkv.at[0])
    tok_here.wait()
    square_columns = []
    for s in range(tok // 64):
        piece = r.gin[s * 64 : (s + 1) * 64, :].astype(f32)
        square_columns.append(jnp.sum(piece * piece, axis=1, keepdims=True))
    squares = transpose_columns([jnp.concatenate(square_columns, axis=0)], tok)[0:1, :]
    which8 = lax.broadcasted_iota(jnp.int32, (8, tok), 0)
    r.rows_own[0:1, :] = lax.rsqrt(squares / model + eps)
    rows_copies = [ship(r.rows_own, r.rows_all.at[a, b], place) for place in b_peers]
    rows_far = [
        ship(r.rows_own, r.rows_all.at[a, b], net.near(b=j, a=k))
        for j in range(nb) for k in range(1, na)
    ]
    r.rows_all[a, b] = r.rows_own[...]
    r.xc[b] = r.gin[:, own_lane]
    cot_copies = to_quarters(r.cot, r.cotc)
    wo_copies = over_a(r.wo_in, r.wo)

    def relayout(target):
        step = 32

        @pl.loop(0, sub // step)
        def _(n):
            rows = pl.ds(pl.multiple_of(n * step, step), step)
            turned = jnp.swapaxes(r.stage[rows].astype(f32), 0, 1)
            for e in range(experts):
                target[a, rows, e * ff : (e + 1) * ff] = turned[e].astype(bf16)

    stage_copy.wait()
    relayout(r.wd)
    wd_copies = over_a(r.wd.at[a], r.wd)
    stage_copy = move(r.wg_in, r.stage)

    lane_index = lax.broadcasted_iota(jnp.int32, (tok, head), 1)
    row_index = lax.broadcasted_iota(jnp.int32, (tok, head), 0)

    @pl.loop(0, nb)
    def _(i):
        place = ((i * na + a) * tok + row_index).astype(f32)
        angle = place * r.gains[2:3, :]
        r.cos_tab[rows_of(i), :] = jnp.cos(angle)
        turned = jnp.sin(angle)
        r.sin_tab[rows_of(i), :] = jnp.where(lane_index < head // 2, -turned, turned)

    x_y = onward(x_copies, r.xc, fourth, across)
    x_more = onward(x_y, r.xc, mine, core)
    arrive(rows_copies + cols_copies + x_more)
    arrive(kv_weights)
    for copy in w_here:
        copy.wait()
    for k in range(na):
        r.cols_sum[:, k * sub : (k + 1) * sub] = r.cols_all[k]
    gain_in = r.cols_sum[experts : experts + 1, :]
    for i in range(nb):
        columns = jnp.transpose(r.rows_all[a, i])
        r.ids[i] = columns
        r.hn[i] = (r.xc[i].astype(f32) * columns[:, 0:1] * gain_in).astype(bf16)

    def weight(j):
        return r.wqkv[j].reshape(part, width)

    @pl.loop(0, nb)
    def _(i):
        for j in (1, 2):
            term = dot(r.hn[i], weight(j)).astype(bf16)
            for h in range(heads):
                piece = term[:, h * head : (h + 1) * head]
                r.pkv[h, rows_of(i), (j - 1) * head : j * head] = piece

    kv_sum = net.reduce(r.pkv, r.gkv)
    cot_y = onward(cot_copies, r.cotc, fourth, across)
    arrive(q_weights)

    @pl.loop(0, nb)
    def _(i):
        term = dot(r.hn[i], weight(0)).astype(bf16)
        for h in range(heads):
            r.pq[h, rows_of(i), :] = term[:, h * head : (h + 1) * head]

    stage_copy.wait()
    relayout(r.wg)
    low, high = (pl.ds(k * experts * ff // 2, experts * ff // 2) for k in range(2))

    def half_over_a(array, lane):
        return [ship(array.at[a, :, lane], array.at[a, :, lane], place) for place in a_peers]

    wg_copies = half_over_a(r.wg, low)
    stage_copy = move(r.wu_in, r.stage)
    kv_sum.inner()
    q_sum = net.reduce(r.pq, r.gq)
    stage_copy.wait()
    relayout(r.wu)
    q_sum.inner()
    cot_more = onward(cot_y, r.cotc, mine, core)
    kv_sum.wait()

    @pl.loop(0, nb)
    def _(i):
        rows = rows_of(i)
        both = kv_sum.total(rows)
        r.raw[rows, head:] = both
        keys = both[:, :head]
        normed = keys * head_norm(keys) * r.gains[1:2, :]
        r.kv[a, rows, :head] = rope(normed, r.cos_tab[rows, :], r.sin_tab[rows, :]).astype(bf16)
        r.kv[a, rows, head:] = both[:, head:].astype(bf16)

    kv_copies = over_a(r.kv.at[a], r.kv)
    wg_copies += half_over_a(r.wg, high)
    wu_copies = over_a(r.wu.at[a], r.wu)
    arrive(wd_copies + cot_more)
    for copy in late_here:
        copy.wait()

    def chosen(left, weights, d, put):
        columns = r.ids[d]
        values = [jnp.zeros((tok, ff), f32) for k in range(top)]
        for e in range(experts):
            term = dot(left, weights[:, :, e * ff : (e + 1) * ff].reshape(part, ff))
            for k in range(top):
                values[k] = jnp.where(columns[:, 1 + k : 2 + k] == e, term, values[k])
        for k in range(top):
            put(k, values[k].astype(bf16))

    groups = ff // head

    @pl.loop(0, nb)
    def _(i):
        def put(k, value):
            for g in range(groups):
                r.pcd[k, i, g * tok : (g + 1) * tok, :] = value[:, g * head : (g + 1) * head]

        chosen(r.cotc[i], r.wd, i, put)

    cd_sums = [net.reduce(r.pcd.at[0], r.gcd.at[0])]
    arrive(rows_far)
    for i in range(nb):
        for j in range(na):
            r.docs[j, :, i * tok : (i + 1) * tok] = r.rows_all[j, i][3:4, :]
    q_sum.wait()

    @pl.loop(0, nb)
    def _(i):
        rows = rows_of(i)
        query = q_sum.total(rows)
        r.raw[rows, :head] = query
        normed = query * head_norm(query) * r.gains[0:1, :]
        r.q_rot[rows, :] = rope(normed, r.cos_tab[rows, :], r.sin_tab[rows, :]).astype(bf16)

    cd_sums[0].inner()

    deep = 2 if na <= 2 else 1

    def deep_rows(i):
        return pl.ds(pl.multiple_of(i * deep * tok, deep * tok), deep * tok)

    def deep_ids(i):
        return r.ids[pl.ds(i * deep, deep)].reshape(deep * tok, 8)

    def attend(block, first, last):
        @pl.loop(0, nb)
        def _(i):
            rows = rows_of(i)
            columns = r.ids[i]
            scores = dot(r.q_rot[rows, :], r.kv[block, :, :head], NT) * scale
            scores = jnp.where(columns[:, 3:4] == r.docs[block], scores, negative)
            most = jnp.max(scores, axis=1, keepdims=True)
            if not first:
                before = r.stat[rows, 0:1]
                most = jnp.maximum(before, most)
            terms = jnp.exp(scores - most)
            total = jnp.sum(terms, axis=1, keepdims=True)
            mixed = dot(terms.astype(bf16), r.kv[block, :, head:])
            if not first:
                fade = jnp.exp(before - most)
                total = r.stat[rows, 1:2] * fade + total
                mixed = r.head_acc[rows, :] * fade + mixed
            if last:
                r.ho[rows, head_lane] = (mixed * (1.0 / total)).astype(bf16)
                r.stat[rows, 2:3] = most + jnp.log(total)
            else:
                r.stat[rows, 0:1] = most
                r.stat[rows, 1:2] = total
                r.head_acc[rows, :] = mixed

    attend(a, True, na == 1)
    for k in range(1, na):
        kv_copies[k - 1].wait_recv()
        attend(lax.rem(a + na - k, na), False, k == na - 1)

    def head_block(array, i, start, size):
        return array.at[pl.ds(start, size), pl.ds(pl.multiple_of(i * head, head), head)]

    def chain(lines, i):
        lines[i].take(lines[i].order[0])
        if i + 2 < len(lines):
            lines[i + 2].begin()

    def rest(line):
        line.take(line.order[1])
        line.take(line.order[2])

    ho_lines = [
        net.spread(lambda i, s=s: head_block(r.ho, i, s * tok, tok), start=s < 2)
        for s in range(nb)
    ]
    arrive(wo_copies)

    mixer = TwoLevel(net, r.acc, r.sendc, r.recvc, r.sendy, r.recvy, 1)
    for i in range(nb):
        chain(ho_lines, i)
        rest(ho_lines[i])
        if i == nb - 1:
            for k in range(1, top):
                cd_sums.append(net.reduce(r.pcd.at[k], r.gcd.at[k]))
        term = dot(r.ho[i * tok : (i + 1) * tok, :], r.wo[...].reshape(part, width), NT)
        mixer.put(i, 0, term, i)
        if i:
            mixer.onward(i - 1, 0, i - 1)
    mixer.onward(nb - 1, 0, nb - 1)
    for group_sum in cd_sums[1:]:
        group_sum.inner()
    gain_mid = r.cols_sum[experts + 1 : experts + 2, :]
    router = r.cols_sum[...].astype(bf16)
    last_copies = []
    for i in range(nb):
        value = r.xc[i, mine, :].astype(f32) + mixer.total(i, 0)
        r.hidden[i] = value
        piece = (value * gain_mid).astype(bf16)
        r.scaled[i, mine, :] = piece
        logits = dot(router, piece, NT)
        squares = jnp.sum(value * value, axis=1, keepdims=True)
        squares = jnp.transpose(jnp.broadcast_to(squares, (half, 128)))[:1, :]
        which = lax.broadcasted_iota(jnp.int32, logits.shape, 0)
        r.small[i, :, mine] = jnp.where(which == experts, squares, logits)
        for array in (r.scaled.at[i, mine, :], r.small.at[i, :, mine]):
            last_copies.append(ship(array, array, core))
    arrive(wg_copies + wu_copies + last_copies)
    mixer.finish()
    kv_sum.finish()
    q_sum.finish()

    small_copies = [ship(r.small.at[p["b"]], r.small_in.at[b], p) for p in b_peers]
    r.small_in[b] = r.small[b]

    def make(d):
        for j, w in enumerate((r.wg, r.wu)):

            def put(k, value, j=j):
                r.pkv[d, (2 * k + j) * tok : (2 * k + j + 1) * tok, :] = value

            chosen(r.scaled[d], w, d, put)

    gu_sum = net.reduce(r.pkv, r.gkv, make)
    gu_sum.inner()
    make(b)
    arrive(small_copies)
    for group_sum in cd_sums:
        group_sum.wait()
    gu_sum.wait()
    total = jnp.sum(r.small_in[...], axis=0)
    r_mid = lax.rsqrt(total[experts : experts + 1] / model + eps)
    logits = total[:experts] * r_mid
    terms = jnp.exp(logits - jnp.max(logits, axis=0, keepdims=True))
    probs = terms / jnp.sum(terms, axis=0, keepdims=True)
    which = lax.broadcasted_iota(jnp.int32, probs.shape, 0).astype(f32)
    picks = [r.rows_own[1 + k : 2 + k] == which for k in range(top)]
    combine = [jnp.sum(jnp.where(pick, probs, 0.0), axis=0, keepdims=True) for pick in picks]
    table = jnp.where(which8 == 0, r_mid, 0.0)
    for k in range(top):
        table = jnp.where(which8 == 1 + k, combine[k], table)
    columns = jnp.transpose(table)
    r_col = columns[:, 0:1]
    columns_back = []
    inner = jnp.zeros((tok, 1), f32)
    for k in range(top):
        gate = gu_sum.total(slice((2 * k) * tok, (2 * k + 1) * tok)) * r_col
        up = gu_sum.total(slice((2 * k + 1) * tok, (2 * k + 2) * tok)) * r_col
        back = jnp.concatenate(
            [
                cd_sums[k].total(slice(g * tok, (g + 1) * tok))
                for g in range(groups)
            ],
            axis=1,
        )
        sig = 1.0 / (1.0 + jnp.exp(-gate))
        silu = gate * sig
        act = silu * up
        weighed = columns[:, 1 + k : 2 + k]
        d_act = weighed * back
        d_gate = d_act * up * (sig * (1.0 + gate * (1.0 - sig)))
        d_up = d_act * silu
        for j, value in enumerate((weighed * act, d_gate * r_col, d_up * r_col)):
            r.pay[b, :, (top * j + k) * ff : (top * j + k + 1) * ff] = value.astype(bf16)
        columns_back.append(jnp.sum(act * back, axis=1, keepdims=True))
        inner = inner + jnp.sum(d_gate * gate + d_up * up, axis=1, keepdims=True)

    pay_line = net.spread(lambda i: r.pay.at[i, :, pl.ds(top * ff, 2 * top * ff)])
    act_lines = [
        net.spread(lambda i, k=k: r.pay.at[i, :, pl.ds(k * ff, ff)], start=False)
        for k in range(top)
    ]
    rank = y * sizes["c"] + c
    r.pair[rank] = transpose_columns(columns_back + [inner], tok)
    arrive([ship(r.pair.at[rank], r.pair.at[rank], place) for place in tp_peers])
    sums = r.pair[0] + r.pair[1] + r.pair[2] + r.pair[3]
    d_probs = jnp.zeros_like(probs)
    for k in range(top):
        d_probs = d_probs + jnp.where(picks[k], sums[k : k + 1], 0.0)
    d_logits = probs * (d_probs - jnp.sum(probs * d_probs, axis=0, keepdims=True))
    inner_row = sums[top : top + 1] + jnp.sum(d_logits * logits, axis=0, keepdims=True)
    r.late_small[b, 0:8, :] = d_logits * r_mid
    r.late_small[b, 8:16, :] = jnp.broadcast_to(r_mid * r_mid * inner_row / model, (8, tok))
    late_copies = [ship(r.late_small.at[b], r.late_small.at[b], place) for place in b_peers]

    mixer = TwoLevel(net, r.acc, r.sendc, r.recvc, r.sendy, r.recvy, 2)
    pieces = experts * ff // width
    by_piece = width // ff

    def expand(j, i, e):
        columns = r.ids[i]
        value = jnp.zeros((tok, ff), f32)
        for k in range(top):
            taken = r.pay[i, :, (top * j + k) * ff : (top * j + k + 1) * ff].astype(f32)
            value = jnp.where(columns[:, 1 + k : 2 + k] == e, taken, value)
        return value.astype(bf16)

    def use(i):
        def widen(j):
            for e in range(experts):
                g, h = e // by_piece, e % by_piece
                r.wide[j, g * tok : (g + 1) * tok, h * ff : (h + 1) * ff] = expand(j, i, e)

        def times(j, w):
            total = 0.0
            for g in range(pieces):
                piece = w[:, :, g * width : (g + 1) * width].reshape(part, width)
                total = total + dot(r.wide[j, g * tok : (g + 1) * tok, :], piece, NT)
            return total

        widen(1)
        widen(2)
        mixer.put(i, 0, times(1, r.wg) + times(2, r.wu), 0)
        mixer.onward(i, 0, 0)

    @pl.loop(0, nb)
    def _(n):
        index = b
        for k in range(nb - 1):
            index = jnp.where(n == k + 1, pay_line.order[k], index)

        @pl.when(n > 0)
        def _():
            pay_line.take(index)

        @pl.when(n == jnp.where(pay_line.inner, 1, 3))
        def _():
            act_lines[0].begin()

        use(index)

    drain(wd_copies + wg_copies + wu_copies)
    gu_sum.finish()

    def to_a(source, target):
        return [ship(source.at[p["a"]], target.at[k], p) for k, p in enumerate(a_peers)]

    def expert_grad(j, left, target, part_of):
        @pl.loop(part_of * experts // 2, (part_of + 1) * experts // 2)
        def _(e):
            for i in range(nb):
                r.pkv[0, i * tok : (i + 1) * tok, :] = expand(j, i, e)
            grad = dot(left[...].reshape(col, part), r.pkv[0], TN).astype(bf16)
            lane = pl.ds(pl.multiple_of(e * ff, ff), ff)
            for k in range(na):
                target[k, :, lane] = grad[k * sub : (k + 1) * sub, :]

    def half_to_a(source, target, part_of):
        lane = (low, high)[part_of]
        return [
            ship(source.at[p["a"], :, lane], target.at[k, :, lane], p)
            for k, p in enumerate(a_peers)
        ]

    expert_grad(1, r.scaled, r.wg, 0)
    pending = half_to_a(r.wg, r.gate_in, 0)
    arrive(late_copies)
    which16 = lax.broadcasted_iota(jnp.int32, (16, tok), 0)
    ffn_part = jnp.zeros((1, part), f32)
    attn_copies = []
    for i in range(nb):
        columns = jnp.transpose(r.late_small[i, :, mine])
        d_log = jnp.where(which16[:, :half] < experts, r.late_small[i, :, mine], 0.0).astype(bf16)
        mid = mixer.total(i, 0) + dot(d_log, router, TN)
        value = r.hidden[i]
        grad = r.cotc[i, mine, :].astype(f32) + gain_mid * mid - value * columns[:, 8:9]
        r.d_attn[i, mine, :] = grad.astype(bf16)
        attn_copies.append(ship(r.d_attn.at[i, mine, :], r.d_attn.at[i, mine, :], core))
        ffn_part = ffn_part + jnp.sum(mid * value, axis=0, keepdims=True)
        r.d_hidden[i] = grad
    act_lines[0].take(act_lines[0].order[0])
    arrive(attn_copies)

    @pl.loop(0, nb)
    def _(i):
        term = dot(r.d_attn[i], r.wo[...].reshape(part, width)).astype(bf16)
        for h in range(heads):
            r.pq[h, rows_of(i), :] = term[:, h * head : (h + 1) * head]

    heads_sum = net.reduce(r.pq, r.gq)

    expert_grad(1, r.scaled, r.wg, 1)
    pending += half_to_a(r.wg, r.gate_in, 1)
    results = [move(r.wg.at[a], r.gate_own)]
    heads_sum.inner()
    expert_grad(2, r.scaled, r.wu, 0)

    def experts_out():
        for line in act_lines:
            rest(line)

        @pl.loop(0, nb)
        def _(i):
            total = 0.0
            for e in range(experts):
                r.pkv[1, 0:tok, :] = expand(0, i, e)
                piece = r.wd[:, :, e * ff : (e + 1) * ff].reshape(part, ff)
                total = total + dot(r.pkv[1, 0:tok, :], piece, NT)
            mixer.put(i, 1, total, i)

    term = dot(r.d_attn[...].reshape(col, part), r.ho[...], TN).astype(bf16)
    r.gout[...] = term.reshape(na, sub, width)
    pending += to_a(r.gout, r.gout_in)
    extra = 0.0
    for i in range(nb):
        d_log = jnp.where(which16 < experts, r.late_small[i], 0.0).astype(bf16)
        extra = extra + dot(d_log, r.scaled[i])
    which_row = lax.broadcasted_iota(jnp.int32, (16, part), 0)
    r.extra_own[...] = jnp.where(which_row == experts + 1, ffn_part, extra)
    heads_sum.wait()
    for line in act_lines[1:]:
        line.begin()

    r.gain_acc[...] = jnp.zeros_like(r.gain_acc)

    @pl.loop(0, nb)
    def _(i):
        rows = rows_of(i)
        cot = heads_sum.total(rows).astype(bf16)
        r.pq[b, rows, :] = cot
        delta = jnp.sum(cot.astype(f32) * r.ho[rows, head_lane].astype(f32), axis=1, keepdims=True)
        r.stat[rows, 4:5] = delta

    def attend_back(block, first, last, start, stop):
        @pl.loop(start // deep, stop // deep)
        def _(i):
            rows = deep_rows(i)
            columns = deep_ids(i)
            query, cot = r.q_rot[rows, :], r.pq[b, rows, :]
            keys, values = r.kv[block, :, :head], r.kv[block, :, head:]
            scores = dot(query, keys, NT) * scale
            keep = columns[:, 3:4] == r.docs[block]
            probs = jnp.where(keep, jnp.exp(scores - r.stat[rows, 2:3]), 0.0)
            d_scores = (probs * (dot(cot, values, NT) - r.stat[rows, 4:5])).astype(bf16)
            key_term = dot(d_scores, query, TN) * scale
            value_term = dot(probs.astype(bf16), cot, TN)

            @pl.when(i == 0)
            def _():
                r.dkv_acc[:, :head] = key_term
                r.dkv_acc[:, head:] = value_term

            @pl.when(i > 0)
            def _():
                r.dkv_acc[:, :head] += key_term
                r.dkv_acc[:, head:] += value_term

            grad = dot(d_scores, keys) * scale
            if not first:
                grad = r.head_acc[rows, :] + grad
            if not last:
                r.head_acc[rows, :] = grad
            else:
                source = r.raw[rows, :head]
                grad, gain_part = unrope(
                    grad, source, r.gains[0:1, :], r.cos_tab[rows, :], r.sin_tab[rows, :]
                )
                r.gain_acc[0:1, :] += gain_part
                r.wide[0, rows, head_lane] = grad.astype(bf16)
                r.stat[rows, 3:4] = jnp.sum(grad * source, axis=1, keepdims=True)

    kv_back = []
    for k in range(1, na):
        attend_back(lax.rem(a + k, na), k == 1, False, 0, nb)
        r.dkv_send[k - 1] = r.dkv_acc[...].astype(bf16)
        kv_back.append(ship(r.dkv_send.at[k - 1], r.dkv_in.at[k - 1], a_peers[k - 1]))
    for line in act_lines[1:]:
        line.take(line.order[0])
    pending += half_to_a(r.wu, r.up_in, 0)
    q_lines = []
    for s in range(2):
        attend_back(a, na == 1, True, s * (nb // 2), (s + 1) * (nb // 2))
        q_lines.append(
            net.spread(lambda i, s=s: head_block(r.wide.at[0], i, s * (col // 2), col // 2))
        )
    expert_grad(2, r.scaled, r.wu, 1)
    pending += half_to_a(r.wu, r.up_in, 1)
    results.append(move(r.wu.at[a], r.up_own))
    for line in q_lines:
        line.take(line.order[0])
    arrive(kv_back)

    @pl.loop(0, nb)
    def _(i):
        rows = rows_of(i)
        both = r.dkv_acc[rows, :]
        for k in range(na - 1):
            both = both + r.dkv_in[k, rows, :].astype(f32)
        source = r.raw[rows, head : 2 * head]
        grad, gain_part = unrope(
            both[:, :head], source, r.gains[1:2, :], r.cos_tab[rows, :], r.sin_tab[rows, :]
        )
        r.gain_acc[1:2, :] += gain_part
        value_grad = both[:, head:]
        r.wide[1, rows, head_lane] = grad.astype(bf16)
        r.wide[2, rows, head_lane] = value_grad.astype(bf16)
        r.stat[rows, 3:4] += jnp.sum(
            grad * source + value_grad * r.raw[rows, 2 * head :], axis=1, keepdims=True
        )

    place16 = (b * 2 + y) * 2 + c
    r.s4[place16] = transpose_columns([r.stat[i * tok : (i + 1) * tok, 3:4] for i in range(nb)], tok)
    r.s4[place16, 4:6, 0:head] = r.gain_acc[0:2, :]
    s4_copies = [ship(r.s4.at[place16], r.s4.at[place16], place) for place in group]

    def kv_piece(s):
        return net.spread(
            lambda i: head_block(r.wide.at[1], i, s * tok, tok),
            lambda i: head_block(r.wide.at[2], i, s * tok, tok),
            start=s < 2,
        )

    kv_lines = [kv_piece(s) for s in range(nb)]
    def weight_grad(j):
        grad = dot(r.hn[...].reshape(col, part), r.wide[j], TN).astype(bf16)
        r.gsend[j] = grad.reshape(na, sub, width)
        return to_a(r.gsend.at[j], r.gin_w.at[j])

    for line in q_lines:
        line.take(line.order[1])
        line.take(line.order[2])
    pending += weight_grad(0)
    mixer_in = TwoLevel(net, r.acc, r.sendc, r.recvc, r.sendy, r.recvy, 1)
    mixer.finish()
    def in_term(i):
        rest(kv_lines[i])
        rows = slice(i * tok, (i + 1) * tok)
        term = dot(r.wide[0, rows, :], weight(0), NT) + dot(r.wide[1, rows, :], weight(1), NT)
        mixer_in.put(i, 0, term + dot(r.wide[2, rows, :], weight(2), NT), i)
        mixer_in.onward(i, 0, i)

    chain(kv_lines, 0)
    experts_out()
    chain(kv_lines, 1)
    for i in range(nb):
        mixer.onward(i, 1, i)
    expert_grad(0, r.cotc, r.wd, 0)
    pending += half_to_a(r.wd, r.down_in, 0)
    arrive(s4_copies)
    in_term(0)
    chain(kv_lines, 2)
    expert_grad(0, r.cotc, r.wd, 1)
    pending += half_to_a(r.wd, r.down_in, 1)
    results.append(move(r.wd.at[a], r.down_own))
    in_term(1)
    chain(kv_lines, 3)
    for j in range(nb):
        r.out_half[j] = (r.hidden[j] + mixer.total(j, 1)).astype(bf16)
    r.block_out[mine, own_lane] = r.out_half[b]
    in_term(2)
    in_term(3)
    out_rows = pl.ds(pl.multiple_of(y * quarter, quarter), quarter)
    out_copies = [
        ship(r.out_half.at[d, out_rows, :], r.block_out.at[fourth, own_lane], {"b": d})
        for d in exchange
    ]

    def lanes_onward(copies, rows, place):
        more = []
        for source_b, copy in zip(exchange, copies):
            copy.wait_recv()
            block = r.block_out.at[rows, lane_of(source_b)]
            more.append(ship(block, block, place))
        return more

    pending += weight_grad(1)
    pending += weight_grad(2)
    sums = r.s4[0]
    for k in range(1, 4 * nb):
        sums = sums + r.s4[k]
    inner_columns = jnp.transpose(sums)
    attn_part = jnp.zeros((1, part), f32)
    in_hops = []
    base_in = net.used
    net.used += nb

    def in_hop(d, slot):
        return pltpu.make_async_remote_copy(
            src_ref=r.d_attn.at[d, pl.ds(0, half), :],
            dst_ref=r.gin.at[mine, own_lane],
            send_sem=r.send.at[base_in + d],
            recv_sem=r.recv.at[base_in + slot],
            device_id={"b": jnp.int32(d)},
            device_id_type=MESH,
        )

    drain(attn_copies)
    for i in range(nb):
        d_in = mixer_in.total(i, 0)
        r_col = r.ids[i, mine, 0:1]
        inner = jnp.where(
            c == 0, inner_columns[:half, i : i + 1], inner_columns[half:, i : i + 1]
        )
        x = r.xc[i, mine, :].astype(f32)
        scaled = d_in * r_col
        grad = r.d_hidden[i] + scaled * gain_in - x * (r_col * r_col * inner / model)
        attn_part = attn_part + jnp.sum(scaled * x, axis=0, keepdims=True)
        r.d_attn[i, :half, :] = grad.astype(bf16)

        @pl.when(b == i)
        def _():
            r.gin[mine, own_lane] = r.d_attn[i, :half, :]

        @pl.when(b != i)
        def _():
            in_hop(i, b).start()

    r.extra_own[...] = jnp.where(which_row == experts + 2, attn_part, r.extra_own[...])
    tail_copy = ship(r.extra_own, r.extra_in, core)
    tail_copy.wait_recv()
    shared = (which_row == experts + 1) | (which_row == experts + 2)
    r.tail_all[a] = r.extra_own[...] + jnp.where(shared, r.extra_in[...], 0.0)
    r.tail_all[a, experts + 3 : experts + 5, 0:head] = sums[4:6, 0:head]
    tail_copies = over_a(r.tail_all.at[a], r.tail_all)
    out_y = lanes_onward(out_copies, fourth, across)
    in_more = []
    for k in range(1, nb):
        place = lax.rem(b + k, nb)
        lane = lane_of(place)
        pltpu.make_async_remote_copy(
            src_ref=r.gin.at[mine, lane],
            dst_ref=r.gin.at[mine, lane],
            send_sem=r.send.at[base_in + place],
            recv_sem=r.recv.at[base_in + place],
            device_id=core,
            device_id_type=MESH,
        ).wait_recv()
        in_more.append(ship(r.gin.at[mine, lane], r.gin.at[mine, lane], core))
    in_more.append(ship(r.gin.at[mine, own_lane], r.gin.at[mine, own_lane], core))
    out_more = lanes_onward(out_y, mine, core)
    block = r.block_out.at[mine, own_lane]
    out_more.append(ship(block, block, core))
    arrive(pending)
    for j in range(4):
        mine_here = r.gsend[j, a] if j < 3 else r.gout[a]
        total = mine_here.astype(f32)
        for k in range(na - 1):
            came = r.gin_w[j, k] if j < 3 else r.gout_in[k]
            total = total + came.astype(f32)
        r.proj[j] = total
    results.append(move(r.proj, r.proj_out))
    arrive(out_more)
    results.append(move(r.block_out, r.out_rows))
    arrive(tail_copies)
    r.tail[...] = jnp.sum(r.tail_all[...], axis=0)
    arrive(in_more)
    results.append(move(r.gin, r.in_rows))
    mixer_in.finish()
    mixer.finish((1,))
    for line in [heads_sum, pay_line] + act_lines + cd_sums + ho_lines + q_lines + kv_lines:
        line.finish()
    for d in range(nb):

        @pl.when(b != d)
        def _():
            in_hop(d, b).wait_send()

    drain(list(sent))
    for copy in results:
        copy.wait()
    assert net.used <= r.send.shape[0] and local_used[0] <= r.local.shape[0]


def layer(sizes, dims, ins):
    nb, na, head, heads, experts, ff, top = dims
    tok, model = ins[0].shape
    part, col, half = model // nb, nb * tok, tok // 2
    sub, width, wide = part // na, heads * head, experts * ff
    others = max(na - 1, 1)
    shape = jax.ShapeDtypeStruct
    vmem, hbm = pl.BlockSpec(memory_space=pltpu.VMEM), pl.BlockSpec(memory_space=pl.ANY)
    outs = [
        shape((tok, model), bf16),
        shape((tok, model), bf16),
        shape((sub, wide), bf16),
        shape((sub, wide), bf16),
        shape((sub, wide), bf16),
        shape((others, sub, wide), bf16),
        shape((others, sub, wide), bf16),
        shape((others, sub, wide), bf16),
        shape((4, sub, width), f32),
        shape((16, part), f32),
    ]
    work = dict(
        xc=((nb, tok, part), bf16),
        cotc=((nb, tok, part), bf16),
        rows_all=((na, nb, 8, tok), f32),
        rows_own=((8, tok), f32),
        cols_own=((16, sub), f32),
        cols_all=((na, 16, sub), f32),
        cols_sum=((16, part), f32),
        wqkv=((3, na, sub, width), bf16),
        wo=((na, sub, width), bf16),
        wg=((na, sub, wide), bf16),
        wu=((na, sub, wide), bf16),
        wd=((na, sub, wide), bf16),
        stage=((sub, experts, ff), bf16),
        hn=((nb, tok, part), bf16),
        raw=((col, 3 * head), f32),
        q_rot=((col, head), bf16),
        kv=((na, col, 2 * head), bf16),
        stat=((col, 128), f32),
        ho=((col, width), bf16),
        cos_tab=((col, head), f32),
        sin_tab=((col, head), f32),
        pkv=((nb, col, 2 * head), bf16),
        gkv=((nb, col, 2 * head), bf16),
        pq=((nb, col, head), bf16),
        gq=((nb, col, head), bf16),
        pcd=((top, nb, ff // head * tok, head), bf16),
        gcd=((top, nb, ff // head * tok, head), bf16),
        acc=((nb, half, part), f32),
        sendc=((nb, half, 2 * part), bf16),
        recvc=((nb, half, 2 * part), bf16),
        sendy=((nb, half, 2 * part), bf16),
        recvy=((nb, half, 2 * part), bf16),
        hidden=((nb, half, part), f32),
        d_hidden=((nb, half, part), f32),
        scaled=((nb, tok, part), bf16),
        small=((nb, 16, tok), f32),
        small_in=((nb, 16, tok), f32),
        pay=((nb, tok, 3 * top * ff), bf16),
        wide=((3, col, width), bf16),
        pair=((4, 8, tok), f32),
        late_small=((nb, 16, tok), f32),
        extra_own=((16, part), f32),
        extra_in=((16, part), f32),
        d_attn=((nb, tok, part), bf16),
        out_half=((nb, half, part), bf16),
        block_out=((tok, model), bf16),
        head_acc=((col, head), f32),
        dkv_acc=((col, 2 * head), f32),
        dkv_send=((others, col, 2 * head), bf16),
        dkv_in=((others, col, 2 * head), bf16),
        gsend=((3, na, sub, width), bf16),
        gin_w=((3, others, sub, width), bf16),
        gout=((na, sub, width), bf16),
        gout_in=((others, sub, width), bf16),
        gin=((tok, model), bf16),
        s4=((4 * nb, 8, tok), f32),
        gain_acc=((8, head), f32),
        tail_all=((na, 16, part), f32),
        ids=((nb, tok, 8), f32),
        gains=((8, head), f32),
        docs=((na, 1, col), f32),
        proj=((4, sub, width), f32),
    )
    count = 174 + 26 * na
    scratch = [pltpu.VMEM(*work[name]) for name in WORK[:-3]] + [
        pltpu.SemaphoreType.DMA((count,)),
        pltpu.SemaphoreType.DMA((count,)),
        pltpu.SemaphoreType.DMA((15,)),
    ]
    return pl.pallas_call(
        functools.partial(layer_kernel, sizes, dims),
        out_shape=outs,
        in_specs=[hbm] * 9 + [vmem] * 8,
        out_specs=[hbm] * 9 + [vmem],
        scratch_shapes=scratch,
        compiler_params=pltpu.CompilerParams(
            collective_id=1, has_side_effects=True, vmem_limit_bytes=67043328
        ),
        name="layer",
    )(*ins)


def last_kernel(experts, ff, sub, *refs):
    out_rows, in_rows, owns, cames, proj = refs[0], refs[1], refs[2:5], refs[5:8], refs[8]
    tail, refs = refs[9], refs[10:]
    block_out, grad_in, grads, projections = refs[0], refs[1], refs[2:5], refs[5:9]
    router, gain_attn, gain_ffn, gain_q, gain_k = refs[9:]
    step = 32

    @pl.loop(0, block_out.shape[0] // step)
    def _(n):
        rows = pl.ds(pl.multiple_of(n * step, step), step)
        block_out[rows, :] = out_rows[rows, :]
        grad_in[rows, :] = in_rows[rows, :].astype(f32)

    @pl.loop(0, owns[0].shape[0] // step)
    def _(n):
        rows = pl.ds(pl.multiple_of(n * step, step), step)
        for own, came, grad in zip(owns, cames, grads):
            for e in range(experts):
                lane = slice(e * ff, (e + 1) * ff)
                total = own[rows, lane].astype(f32)
                for k in range(came.shape[0]):
                    total = total + came[k, rows, lane].astype(f32)
                grad[rows, e, :] = total
        for j in range(4):
            projections[j][rows, :] = proj[j, rows, :]

    @pl.when(pl.program_id(0) == 0)
    def _():
        a = lax.axis_index("a")
        piece = tail[:, :sub]
        for k in range(1, tail.shape[1] // sub):
            piece = jnp.where(a == k, tail[:, k * sub : (k + 1) * sub], piece)
        router[...] = piece[:experts]
        gain_ffn[...] = piece[experts + 1 : experts + 2]
        gain_attn[...] = piece[experts + 2 : experts + 3]
        gain_q[...] = tail[experts + 3 : experts + 4, : gain_q.shape[1]]
        gain_k[...] = tail[experts + 4 : experts + 5, : gain_k.shape[1]]


def last(dims, ins):
    nb, na, head, heads, experts, ff, top = dims
    tok, model = ins[0].shape
    sub, wide = ins[2].shape
    others, width = ins[5].shape[0], ins[8].shape[2]
    steps = 2
    shape = jax.ShapeDtypeStruct
    rows = pl.BlockSpec((tok // steps, model), lambda i: (i, 0))
    own = pl.BlockSpec((sub // steps, wide), lambda i: (i, 0))
    came = pl.BlockSpec((others, sub // steps, wide), lambda i: (0, i, 0))
    grad = pl.BlockSpec((sub // steps, experts, ff), lambda i: (i, 0, 0))
    flat = pl.BlockSpec((sub // steps, width), lambda i: (i, 0))
    small = [shape((experts, sub), f32), shape((1, sub), f32), shape((1, sub), f32)]
    small += [shape((1, head), f32)] * 2
    return pl.pallas_call(
        functools.partial(last_kernel, experts, ff, sub),
        grid=(steps,),
        out_shape=[shape((tok, model), bf16), shape((tok, model), f32)]
        + [shape((sub, experts, ff), f32)] * 3
        + [shape((sub, width), f32)] * 4
        + small,
        in_specs=[rows, rows] + [own] * 3 + [came] * 3
        + [pl.BlockSpec((4, sub // steps, width), lambda i: (0, i, 0))]
        + [pl.BlockSpec(ins[9].shape, lambda i: (0, 0))],
        out_specs=[rows, rows] + [grad] * 3 + [flat] * 4
        + [pl.BlockSpec(item.shape, lambda i: (0, 0)) for item in small],
        name="last",
    )(*ins)


def on_device(
    sizes,
    tokens_in,
    doc_ids,
    expert_ids,
    attn_gain,
    q_gain,
    k_gain,
    w_query,
    w_key,
    w_value,
    w_output,
    ffn_gain,
    w_router,
    w_gate,
    w_up,
    w_down,
    cotangent,
):
    nb, na = sizes["b"], sizes["a"]
    tok, model = tokens_in.shape
    part = model // nb
    sub = part // na
    head = q_gain.shape[0]
    width = w_query.shape[1]
    heads = width // head
    experts, ff = w_gate.shape[1], w_gate.shape[2]
    top = expert_ids.shape[1]
    dims = (nb, na, head, heads, experts, ff, top)

    speed = theta ** (-2.0 * (np.arange(head) % (head // 2)) / head)
    parts = layer(
        sizes,
        dims,
        [
            tokens_in, cotangent, w_query, w_key, w_value, w_output, w_gate, w_up, w_down,
            expert_ids.T, doc_ids[None], w_router.T, attn_gain, ffn_gain, q_gain[None],
            k_gain[None], jnp.asarray(speed, f32)[None],
        ],
    )
    (
        block_out, grad_in, grad_gate, grad_up, grad_down, grad_query, grad_key, grad_value,
        grad_output, router, gain_attn, gain_ffn, gain_q, gain_k,
    ) = last(dims, parts)
    return (
        block_out,
        grad_in,
        gain_attn.reshape(sub),
        gain_q.reshape(head),
        gain_k.reshape(head),
        grad_query,
        grad_key,
        grad_value,
        grad_output,
        gain_ffn.reshape(sub),
        router.T,
        grad_gate,
        grad_up,
        grad_down,
    )


def solution(mesh):
    cp, tp = mesh.shape["cp"], mesh.shape["tp"]
    sizes = {"b": 4, "a": cp // 4, "y": 2, "c": tp // 2}
    split = Mesh(mesh.devices.reshape([sizes[axis] for axis in AXES]), AXES)
    cp, tp = ("b", "a"), ("y", "c")
    return jax.shard_map(
        functools.partial(on_device, sizes),
        mesh=split,
        in_specs=(
            P(cp, None),
            P(cp),
            P(cp, None),
            P(cp),
            P(),
            P(),
            P(cp, tp),
            P(cp, tp),
            P(cp, tp),
            P(cp, tp),
            P(cp),
            P(cp, None),
            P(cp, None, tp),
            P(cp, None, tp),
            P(cp, None, tp),
            P(cp, None),
        ),
        out_specs=(
            P(cp, None),
            P(cp, None),
            P(cp),
            P(),
            P(),
            P(cp, tp),
            P(cp, tp),
            P(cp, tp),
            P(cp, tp),
            P(cp),
            P(cp, None),
            P(cp, None, tp),
            P(cp, None, tp),
            P(cp, None, tp),
        ),
        check_vma=False,
    )
```

```python
import functools
import types

import jax
import jax.numpy as jnp
import numpy as np
from jax import lax
from jax.experimental import pallas as pl
from jax.experimental.pallas import tpu as pltpu
from jax.sharding import Mesh
from jax.sharding import PartitionSpec as P

eps = 1e-05
theta = 50000.0
negative = -1e30
AXES = ("b", "a", "y", "c")
MESH = pl.DeviceIdType.MESH
bf16 = jnp.bfloat16
f32 = jnp.float32


NT = (((1,), (1,)), ((), ()))
TN = (((0,), (0,)), ((), ()))


def dot(left, right, dims=(((1,), (0,)), ((), ()))):
    return lax.dot_general(left, right, dims, preferred_element_type=f32)


class Net:
    def __init__(self, sizes, send, recv):
        self.sizes, self.send, self.recv, self.used = sizes, send, recv, 0
        self.me = {axis: lax.axis_index(axis) for axis in AXES}

    def near(self, **offs):
        return {axis: lax.rem(self.me[axis] + off, self.sizes[axis]) for axis, off in offs.items()}

    def copy(self, source, target, place):
        slot = self.used
        self.used += 1
        return pltpu.make_async_remote_copy(
            src_ref=source,
            dst_ref=target,
            send_sem=self.send.at[slot],
            recv_sem=self.recv.at[slot],
            device_id=place,
            device_id_type=MESH,
        )

    def greet(self, places):
        barrier = pltpu.get_barrier_semaphore()
        for place in places:
            pl.semaphore_signal(barrier, inc=1, device_id=place, device_id_type=MESH)
        pl.semaphore_wait(barrier, len(places))

    def pick(self, *values):
        result = values[-1]
        for i in range(len(values) - 2, -1, -1):
            result = jnp.where(self.me["b"] == i, values[i], result)
        return result

    def reduce(self, *args, **options):
        return Reduce(self, *args, **options)

    def spread(self, *blocks, start=True):
        return Spread(self, blocks, start)


class Reduce:
    def __init__(self, net, parts, got, make=None, pieces=1):
        self.net, self.parts, self.got, self.pieces = net, parts, got, pieces
        self.b = b = net.me["b"]
        self.base = net.used
        self.rows = parts.shape[1] // pieces
        net.used += 4 * pieces
        self.order = [3 - b, net.pick(2, 0, 3, 1), net.pick(1, 3, 0, 2)]
        if make is None:
            for k in range(2):
                self.start(self.order[k])
            return
        if net.sizes["a"] > 2:
            for k in range(3):
                make(self.order[k])
                if k < 2:
                    self.start(self.order[k])
            return

        @pl.loop(0, 3)
        def _(k):
            d = jnp.where(k == 0, self.order[0], jnp.where(k == 1, self.order[1], self.order[2]))
            make(d)

            @pl.when(k < 2)
            def _():
                self.start(d)

    def start(self, d):
        for p in range(self.pieces):
            self.hop(d, p).start()

    def piece(self, p):
        return pl.ds(p * self.rows, self.rows)

    def hop(self, d, p):
        net, b = self.net, self.b
        far = ((b == 0) & (d == 3)) | ((b == 3) & (d == 0))
        beside = jnp.where(b == 0, 1, 2)
        target, slot = jnp.where(far, beside, d), jnp.where(far, beside, b)
        return pltpu.make_async_remote_copy(
            src_ref=self.parts.at[d, self.piece(p), :],
            dst_ref=self.got.at[slot, self.piece(p), :],
            send_sem=net.send.at[self.base + 4 * p + d],
            recv_sem=net.recv.at[self.base + 4 * p + slot],
            device_id={"b": target},
            device_id_type=MESH,
        )

    def came(self, i, p):
        net = self.net
        block = self.got.at[i, self.piece(p), :]
        return pltpu.make_async_remote_copy(
            src_ref=block,
            dst_ref=block,
            send_sem=net.send.at[self.base + 4 * p + i],
            recv_sem=net.recv.at[self.base + 4 * p + i],
            device_id=net.near(b=1),
            device_id_type=MESH,
        )

    def inner(self):
        b, d = self.b, self.order[2]
        for p in range(self.pieces):

            @pl.when((b == 1) | (b == 2))
            def _():
                self.came(b, p).wait_recv()
                step = 256 if self.rows % 256 == 0 else self.rows

                @pl.loop(0, self.rows // step)
                def _(i):
                    sl = pl.ds(pl.multiple_of(p * self.rows + i * step, step), step)
                    total = self.parts[d, sl, :].astype(f32) + self.got[b, sl, :].astype(f32)
                    self.parts[d, sl, :] = total.astype(bf16)

            self.hop(d, p).start()

    def wait(self):
        for i in range(4):

            @pl.when((self.b != i) & (jnp.abs(self.b - i) <= 2))
            def _():
                for p in range(self.pieces):
                    self.came(i, p).wait_recv()

    def total(self, *index):
        b = self.b
        value = self.parts[(b,) + index].astype(f32)
        for i in range(4):
            valid = (b != i) & (jnp.abs(b - i) <= 2)
            value = value + jnp.where(valid, self.got[(i,) + index].astype(f32), 0.0)
        return value

    def finish(self):
        for d in range(4):

            @pl.when(self.b != d)
            def _():
                for p in range(self.pieces):
                    self.hop(d, p).wait_send()


class Spread:
    def __init__(self, net, blocks, start):
        self.net, self.blocks = net, blocks
        self.b = b = net.me["b"]
        self.base = net.used
        net.used += 4 * len(blocks)
        self.targets = [net.pick(2, 3, 0, 1), net.pick(1, 0, 3, 2), net.pick(2, 2, 1, 1)]
        self.order = [net.pick(1, 3, 0, 2), net.pick(2, 0, 3, 1), net.pick(3, 2, 1, 0)]
        self.inner = (b == 1) | (b == 2)
        if start:
            self.begin()

    def begin(self):
        for k, target in enumerate(self.targets):
            if k < 2:
                for j in range(len(self.blocks)):
                    self.hop(self.b, target, target, j).start()
            else:

                @pl.when(self.inner)
                def _():
                    for j in range(len(self.blocks)):
                        self.hop(self.b, target, target, j).start()

    def hop(self, i, target, slot, j):
        net, count = self.net, len(self.blocks)
        return pltpu.make_async_remote_copy(
            src_ref=self.blocks[j](i),
            dst_ref=self.blocks[j](i),
            send_sem=net.send.at[self.base + slot * count + j],
            recv_sem=net.recv.at[self.base + i * count + j],
            device_id={"b": target},
            device_id_type=MESH,
        )

    def take(self, i):
        b = self.b
        onward = ((b == 1) & (i == 3)) | ((b == 2) & (i == 0))
        for j in range(len(self.blocks)):
            self.hop(i, self.net.near(b=1)["b"], b, j).wait_recv()

            @pl.when(onward)
            def _():
                self.hop(i, jnp.where(b == 1, 0, 3), b, j).start()

    def take_all(self):
        for i in self.order:
            self.take(i)

    def finish(self):
        b = self.b
        for k, target in enumerate(self.targets):
            for j in range(len(self.blocks)):
                if k < 2:
                    self.hop(b, target, target, j).wait_send()
                else:

                    @pl.when(self.inner)
                    def _():
                        self.hop(b, target, target, j).wait_send()
                        self.hop(b, jnp.where(b == 1, 0, 3), b, j).wait_send()


def rope(values, cos_tab, sin_tab):
    return values * cos_tab + pltpu.roll(values, values.shape[1] // 2, 1) * sin_tab


def head_norm(values):
    return lax.rsqrt(jnp.mean(values * values, axis=1, keepdims=True) + eps)


def unrope(grad, raw, gain, cos_tab, sin_tab):
    factor = head_norm(raw)
    normed = raw * factor
    turned = grad * cos_tab + pltpu.roll(grad * sin_tab, grad.shape[1] // 2, 1)
    gain_part = jnp.sum(turned * normed, axis=0, keepdims=True)
    inner = turned * gain
    slope = jnp.mean(raw * inner, axis=1, keepdims=True)
    return factor * inner - raw * (factor * factor * factor * slope), gain_part


class TwoLevel:
    def __init__(self, net, acc, sendc, recvc, sendy, recvy, kinds):
        self.net, self.acc = net, acc
        self.sendc, self.recvc, self.sendy, self.recvy = sendc, recvc, sendy, recvy
        self.base = net.used
        self.kinds = kinds
        net.used += 8 * kinds
        self.part = acc.shape[2]
        self.half = acc.shape[1]

    def lane(self, j):
        return slice(j * self.part, (j + 1) * self.part)

    def hop(self, i, j, level):
        net = self.net
        source, target = ((self.sendc, self.recvc), (self.sendy, self.recvy))[level]
        slot = self.base + 4 * self.kinds * level + self.kinds * i + j
        lane = pl.ds(j * self.part, self.part)
        return pltpu.make_async_remote_copy(
            src_ref=source.at[i, :, lane],
            dst_ref=target.at[i, :, lane],
            send_sem=net.send.at[slot],
            recv_sem=net.recv.at[slot],
            device_id=net.near(c=1) if level == 0 else net.near(y=1),
            device_id_type=MESH,
        )

    def put(self, i, j, term, k):
        first = self.net.me["c"] == 0
        low, high = term[: self.half], term[self.half :]
        self.acc[k] = jnp.where(first, low, high)
        self.sendc[i, :, self.lane(j)] = jnp.where(first, high, low).astype(bf16)
        self.hop(i, j, 0).start()

    def onward(self, i, j, k):
        self.hop(i, j, 0).wait_recv()
        total = self.acc[k] + self.recvc[i, :, self.lane(j)].astype(f32)
        self.sendy[i, :, self.lane(j)] = total.astype(bf16)
        self.hop(i, j, 1).start()

    def total(self, i, j):
        self.hop(i, j, 1).wait_recv()
        lane = self.lane(j)
        return self.sendy[i, :, lane].astype(f32) + self.recvy[i, :, lane].astype(f32)

    def finish(self, kinds=(0,)):
        for i in range(4):
            for j in kinds:
                self.hop(i, j, 0).wait_send()
                self.hop(i, j, 1).wait_send()


def transpose_columns(columns, rows):
    lane = lax.broadcasted_iota(jnp.int32, (rows, 128), 1)
    table = jnp.zeros((rows, 128), f32)
    for k, column in enumerate(columns):
        table = jnp.where(lane == k, column, table)
    return jnp.transpose(table)[:8, :]


INS = (
    "tok", "cot", "wq_in", "wk_in", "wv_in", "wo_in", "wg_in", "wu_in", "wd_in", "ids_in",
    "docs_in", "router_in", "gain_in_a", "gain_in_f", "gain_q", "gain_k", "speed_in",
)
OUTS = (
    "out_rows", "in_rows", "gate_own", "up_own", "down_own", "gate_in", "up_in", "down_in",
    "proj_out", "tail",
)
WORK = (
    "xc", "cotc", "rows_all", "rows_own", "cols_own", "cols_all", "cols_sum", "wqkv", "wo",
    "wg", "wu", "wd", "stage", "hn", "raw", "q_rot", "kv", "stat", "ho", "cos_tab", "sin_tab",
    "pkv", "gkv", "pq", "gq", "pcd", "gcd", "acc", "sendc", "recvc", "sendy", "recvy", "hidden", "d_hidden", "scaled",
    "small", "small_in", "pay", "wide", "pair", "late_small", "extra_own", "extra_in", "d_attn",
    "out_half", "block_out", "head_acc", "dkv_acc", "dkv_send", "dkv_in", "gsend", "gin_w",
    "gout", "gout_in", "gin", "s4", "gain_acc", "tail_all", "gains", "ids", "docs", "proj",
    "send", "recv", "local",
)


def layer_kernel(sizes, dims, *refs):
    r = types.SimpleNamespace(**dict(zip(INS + OUTS + WORK, refs)))
    nb, na, head, heads, experts, ff, top = dims
    net = Net(sizes, r.send, r.recv)
    me = net.me
    b, a, y, c = me["b"], me["a"], me["y"], me["c"]
    tok, part = r.xc.shape[1], r.xc.shape[2]
    half, col, model, width, sub = tok // 2, nb * tok, nb * part, heads * head, part // na
    scale = head**-0.5
    mine = pl.ds(pl.multiple_of(c * half, half), half)
    own_lane = pl.ds(pl.multiple_of(b * part, part), part)
    head_lane = pl.ds(pl.multiple_of(b * head, head), head)
    core, across = net.near(c=1), net.near(y=1)
    b_peers = [net.near(b=k) for k in range(1, nb)]
    a_peers = [net.near(a=k) for k in range(1, na)]
    group = [
        net.near(b=i, y=j, c=k)
        for i in range(nb) for j in range(2) for k in range(2) if i or j or k
    ]
    tp_peers = [net.near(y=j, c=k) for j in range(2) for k in range(2) if j or k]
    sent = []
    local_used = [0]

    def rows_of(i):
        return pl.ds(pl.multiple_of(i * tok, tok), tok)

    def lane_of(place):
        return pl.ds(pl.multiple_of(place * part, part), part)

    def move(source, target):
        copy = pltpu.make_async_copy(source, target, r.local.at[local_used[0]])
        local_used[0] += 1
        copy.start()
        return copy

    def ship(source, target, place):
        copy = net.copy(source, target, place)
        copy.start()
        sent.append(copy)
        return copy

    def arrive(copies):
        for copy in copies:
            copy.wait_recv()

    def drain(copies):
        for copy in copies:
            copy.wait_send()
            sent[:] = [other for other in sent if other is not copy]

    tok_here = move(r.tok, r.gin)
    w_here = [move(w, r.wqkv.at[j, a]) for j, w in ((1, r.wk_in), (2, r.wv_in), (0, r.wq_in))]
    stage_copy = move(r.wd_in, r.stage)
    late_here = [move(r.wo_in, r.wo.at[a]), move(r.cot.at[:, own_lane], r.cotc.at[b])]
    net.greet(group + [net.near(b=j, a=k) for j in range(nb) for k in range(1, na)])

    r.cols_own[...] = jnp.zeros_like(r.cols_own)
    r.cols_own[0:experts, :] = r.router_in[...].astype(f32)
    r.cols_own[experts : experts + 1, :] = r.gain_in_a[...].astype(f32).reshape(1, sub)
    r.cols_own[experts + 1 : experts + 2, :] = r.gain_in_f[...].astype(f32).reshape(1, sub)
    r.gains[0:1, :] = r.gain_q[...].astype(f32)
    r.gains[1:2, :] = r.gain_k[...].astype(f32)
    r.gains[2:3, :] = r.speed_in[...]
    r.rows_own[...] = jnp.zeros_like(r.rows_own)
    r.rows_own[1 : 1 + top, :] = r.ids_in[...].astype(f32)
    r.rows_own[3:4, :] = r.docs_in[...].astype(f32)

    exchange = [net.pick(2, 3, 0, 1), net.pick(3, 2, 1, 0), net.pick(1, 0, 3, 2)]

    quarter = half // 2
    fourth = pl.ds(pl.multiple_of(c * half + y * quarter, quarter), quarter)

    def to_quarters(source, target):
        return [
            ship(source.at[fourth, lane_of(d)], target.at[b, fourth, :], {"b": d})
            for d in exchange
        ]

    def over_a(source, target):
        return [ship(source, target.at[a], place) for place in a_peers]

    def onward(copies, target, rows, place):
        more = []
        for source_b, copy in zip(exchange, copies):
            copy.wait_recv()
            block = target.at[source_b, rows, :]
            more.append(ship(block, block, place))
        return more

    x_copies = to_quarters(r.tok, r.xc)
    cols_copies = over_a(r.cols_own, r.cols_all)
    r.cols_all[a] = r.cols_own[...]
    kv_weights = over_a(r.wk_in, r.wqkv.at[1]) + over_a(r.wv_in, r.wqkv.at[2])
    q_weights = over_a(r.wq_in, r.wqkv.at[0])
    tok_here.wait()
    square_columns = []
    for s in range(tok // 64):
        piece = r.gin[s * 64 : (s + 1) * 64, :].astype(f32)
        square_columns.append(jnp.sum(piece * piece, axis=1, keepdims=True))
    squares = transpose_columns([jnp.concatenate(square_columns, axis=0)], tok)[0:1, :]
    which8 = lax.broadcasted_iota(jnp.int32, (8, tok), 0)
    r.rows_own[0:1, :] = lax.rsqrt(squares / model + eps)
    rows_copies = [ship(r.rows_own, r.rows_all.at[a, b], place) for place in b_peers]
    rows_far = [
        ship(r.rows_own, r.rows_all.at[a, b], net.near(b=j, a=k))
        for j in range(nb) for k in range(1, na)
    ]
    r.rows_all[a, b] = r.rows_own[...]
    r.xc[b] = r.gin[:, own_lane]
    cot_copies = to_quarters(r.cot, r.cotc)
    wo_copies = over_a(r.wo_in, r.wo)

    def relayout(target):
        step = 32

        @pl.loop(0, sub // step)
        def _(n):
            rows = pl.ds(pl.multiple_of(n * step, step), step)
            turned = jnp.swapaxes(r.stage[rows].astype(f32), 0, 1)
            for e in range(experts):
                target[a, rows, e * ff : (e + 1) * ff] = turned[e].astype(bf16)

    stage_copy.wait()
    relayout(r.wd)
    wd_copies = over_a(r.wd.at[a], r.wd)
    stage_copy = move(r.wg_in, r.stage)

    lane_index = lax.broadcasted_iota(jnp.int32, (tok, head), 1)
    row_index = lax.broadcasted_iota(jnp.int32, (tok, head), 0)

    @pl.loop(0, nb)
    def _(i):
        place = ((i * na + a) * tok + row_index).astype(f32)
        angle = place * r.gains[2:3, :]
        r.cos_tab[rows_of(i), :] = jnp.cos(angle)
        turned = jnp.sin(angle)
        r.sin_tab[rows_of(i), :] = jnp.where(lane_index < head // 2, -turned, turned)

    x_y = onward(x_copies, r.xc, fourth, across)
    x_more = onward(x_y, r.xc, mine, core)
    arrive(rows_copies + cols_copies + x_more)
    arrive(kv_weights)
    for copy in w_here:
        copy.wait()
    for k in range(na):
        r.cols_sum[:, k * sub : (k + 1) * sub] = r.cols_all[k]
    gain_in = r.cols_sum[experts : experts + 1, :]
    for i in range(nb):
        columns = jnp.transpose(r.rows_all[a, i])
        r.ids[i] = columns
        r.hn[i] = (r.xc[i].astype(f32) * columns[:, 0:1] * gain_in).astype(bf16)

    def weight(j):
        return r.wqkv[j].reshape(part, width)

    @pl.loop(0, nb)
    def _(i):
        for j in (1, 2):
            term = dot(r.hn[i], weight(j)).astype(bf16)
            for h in range(heads):
                piece = term[:, h * head : (h + 1) * head]
                r.pkv[h, rows_of(i), (j - 1) * head : j * head] = piece

    kv_sum = net.reduce(r.pkv, r.gkv, pieces=2)
    cot_y = onward(cot_copies, r.cotc, fourth, across)
    arrive(q_weights)

    @pl.loop(0, nb)
    def _(i):
        term = dot(r.hn[i], weight(0)).astype(bf16)
        for h in range(heads):
            r.pq[h, rows_of(i), :] = term[:, h * head : (h + 1) * head]

    stage_copy.wait()
    relayout(r.wg)
    low, high = (pl.ds(k * experts * ff // 2, experts * ff // 2) for k in range(2))

    def half_over_a(array, lane):
        return [ship(array.at[a, :, lane], array.at[a, :, lane], place) for place in a_peers]

    wg_copies = half_over_a(r.wg, low)
    stage_copy = move(r.wu_in, r.stage)
    kv_sum.inner()
    q_sum = net.reduce(r.pq, r.gq)
    stage_copy.wait()
    relayout(r.wu)
    q_sum.inner()
    cot_more = onward(cot_y, r.cotc, mine, core)
    kv_sum.wait()

    @pl.loop(0, nb)
    def _(i):
        rows = rows_of(i)
        both = kv_sum.total(rows)
        r.raw[rows, head:] = both
        keys = both[:, :head]
        normed = keys * head_norm(keys) * r.gains[1:2, :]
        r.kv[a, rows, :head] = rope(normed, r.cos_tab[rows, :], r.sin_tab[rows, :]).astype(bf16)
        r.kv[a, rows, head:] = both[:, head:].astype(bf16)

    kv_copies = over_a(r.kv.at[a], r.kv)
    wg_copies += half_over_a(r.wg, high)
    wu_copies = over_a(r.wu.at[a], r.wu)
    arrive(wd_copies + cot_more)
    for copy in late_here:
        copy.wait()

    def chosen(left, weights, d, put):
        columns = r.ids[d]
        values = [jnp.zeros((tok, ff), f32) for k in range(top)]
        for e in range(experts):
            term = dot(left, weights[:, :, e * ff : (e + 1) * ff].reshape(part, ff))
            for k in range(top):
                values[k] = jnp.where(columns[:, 1 + k : 2 + k] == e, term, values[k])
        for k in range(top):
            put(k, values[k].astype(bf16))

    groups = ff // head

    @pl.loop(0, nb)
    def _(i):
        def put(k, value):
            for g in range(groups):
                r.pcd[k, i, g * tok : (g + 1) * tok, :] = value[:, g * head : (g + 1) * head]

        chosen(r.cotc[i], r.wd, i, put)

    cd_sums = [net.reduce(r.pcd.at[0], r.gcd.at[0])]
    arrive(rows_far)
    for i in range(nb):
        for j in range(na):
            r.docs[j, :, i * tok : (i + 1) * tok] = r.rows_all[j, i][3:4, :]
    q_sum.wait()

    @pl.loop(0, nb)
    def _(i):
        rows = rows_of(i)
        query = q_sum.total(rows)
        r.raw[rows, :head] = query
        normed = query * head_norm(query) * r.gains[0:1, :]
        r.q_rot[rows, :] = rope(normed, r.cos_tab[rows, :], r.sin_tab[rows, :]).astype(bf16)

    cd_sums[0].inner()

    deep = 2 if na <= 2 else 1

    def deep_rows(i):
        return pl.ds(pl.multiple_of(i * deep * tok, deep * tok), deep * tok)

    def deep_ids(i):
        return r.ids[pl.ds(i * deep, deep)].reshape(deep * tok, 8)

    def attend(block, first, last):
        @pl.loop(0, nb)
        def _(i):
            rows = rows_of(i)
            columns = r.ids[i]
            scores = dot(r.q_rot[rows, :], r.kv[block, :, :head], NT) * scale
            scores = jnp.where(columns[:, 3:4] == r.docs[block], scores, negative)
            most = jnp.max(scores, axis=1, keepdims=True)
            if not first:
                before = r.stat[rows, 0:1]
                most = jnp.maximum(before, most)
            terms = jnp.exp(scores - most)
            total = jnp.sum(terms, axis=1, keepdims=True)
            mixed = dot(terms.astype(bf16), r.kv[block, :, head:])
            if not first:
                fade = jnp.exp(before - most)
                total = r.stat[rows, 1:2] * fade + total
                mixed = r.head_acc[rows, :] * fade + mixed
            if last:
                r.ho[rows, head_lane] = (mixed * (1.0 / total)).astype(bf16)
                r.stat[rows, 2:3] = most + jnp.log(total)
            else:
                r.stat[rows, 0:1] = most
                r.stat[rows, 1:2] = total
                r.head_acc[rows, :] = mixed

    attend(a, True, na == 1)
    for k in range(1, na):
        kv_copies[k - 1].wait_recv()
        attend(lax.rem(a + na - k, na), False, k == na - 1)

    def head_block(array, i, start, size):
        return array.at[pl.ds(start, size), pl.ds(pl.multiple_of(i * head, head), head)]

    def chain(lines, i):
        lines[i].take(lines[i].order[0])
        if i + 2 < len(lines):
            lines[i + 2].begin()

    def rest(line):
        line.take(line.order[1])
        line.take(line.order[2])

    ho_lines = [
        net.spread(lambda i, s=s: head_block(r.ho, i, s * tok, tok), start=s < 2)
        for s in range(nb)
    ]
    arrive(wo_copies)

    mixer = TwoLevel(net, r.acc, r.sendc, r.recvc, r.sendy, r.recvy, 1)
    for i in range(nb):
        chain(ho_lines, i)
        rest(ho_lines[i])
        if i == nb - 1:
            for k in range(1, top):
                cd_sums.append(net.reduce(r.pcd.at[k], r.gcd.at[k]))
        term = dot(r.ho[i * tok : (i + 1) * tok, :], r.wo[...].reshape(part, width), NT)
        mixer.put(i, 0, term, i)
        if i:
            mixer.onward(i - 1, 0, i - 1)
    mixer.onward(nb - 1, 0, nb - 1)
    for group_sum in cd_sums[1:]:
        group_sum.inner()
    gain_mid = r.cols_sum[experts + 1 : experts + 2, :]
    router = r.cols_sum[...].astype(bf16)
    last_copies = []
    for i in range(nb):
        value = r.xc[i, mine, :].astype(f32) + mixer.total(i, 0)
        r.hidden[i] = value
        piece = (value * gain_mid).astype(bf16)
        r.scaled[i, mine, :] = piece
        logits = dot(router, piece, NT)
        squares = jnp.sum(value * value, axis=1, keepdims=True)
        squares = jnp.transpose(jnp.broadcast_to(squares, (half, 128)))[:1, :]
        which = lax.broadcasted_iota(jnp.int32, logits.shape, 0)
        r.small[i, :, mine] = jnp.where(which == experts, squares, logits)
        for array in (r.scaled.at[i, mine, :], r.small.at[i, :, mine]):
            last_copies.append(ship(array, array, core))
    arrive(wg_copies + wu_copies + last_copies)
    mixer.finish()
    kv_sum.finish()
    q_sum.finish()

    small_copies = [ship(r.small.at[p["b"]], r.small_in.at[b], p) for p in b_peers]
    r.small_in[b] = r.small[b]

    def make(d):
        for j, w in enumerate((r.wg, r.wu)):

            def put(k, value, j=j):
                r.pkv[d, (2 * k + j) * tok : (2 * k + j + 1) * tok, :] = value

            chosen(r.scaled[d], w, d, put)

    gu_sum = net.reduce(r.pkv, r.gkv, make, pieces=2)
    gu_sum.inner()
    make(b)
    arrive(small_copies)
    for group_sum in cd_sums:
        group_sum.wait()
    gu_sum.wait()
    total = jnp.sum(r.small_in[...], axis=0)
    r_mid = lax.rsqrt(total[experts : experts + 1] / model + eps)
    logits = total[:experts] * r_mid
    terms = jnp.exp(logits - jnp.max(logits, axis=0, keepdims=True))
    probs = terms / jnp.sum(terms, axis=0, keepdims=True)
    which = lax.broadcasted_iota(jnp.int32, probs.shape, 0).astype(f32)
    picks = [r.rows_own[1 + k : 2 + k] == which for k in range(top)]
    combine = [jnp.sum(jnp.where(pick, probs, 0.0), axis=0, keepdims=True) for pick in picks]
    table = jnp.where(which8 == 0, r_mid, 0.0)
    for k in range(top):
        table = jnp.where(which8 == 1 + k, combine[k], table)
    columns = jnp.transpose(table)
    r_col = columns[:, 0:1]
    columns_back = []
    inner = jnp.zeros((tok, 1), f32)
    for k in range(top):
        gate = gu_sum.total(slice((2 * k) * tok, (2 * k + 1) * tok)) * r_col
        up = gu_sum.total(slice((2 * k + 1) * tok, (2 * k + 2) * tok)) * r_col
        back = jnp.concatenate(
            [
                cd_sums[k].total(slice(g * tok, (g + 1) * tok))
                for g in range(groups)
            ],
            axis=1,
        )
        sig = 1.0 / (1.0 + jnp.exp(-gate))
        silu = gate * sig
        act = silu * up
        weighed = columns[:, 1 + k : 2 + k]
        d_act = weighed * back
        d_gate = d_act * up * (sig * (1.0 + gate * (1.0 - sig)))
        d_up = d_act * silu
        for j, value in enumerate((weighed * act, d_gate * r_col, d_up * r_col)):
            r.pay[b, :, (top * j + k) * ff : (top * j + k + 1) * ff] = value.astype(bf16)
        columns_back.append(jnp.sum(act * back, axis=1, keepdims=True))
        inner = inner + jnp.sum(d_gate * gate + d_up * up, axis=1, keepdims=True)

    pay_line = net.spread(lambda i: r.pay.at[i, :, pl.ds(top * ff, 2 * top * ff)])
    act_lines = [
        net.spread(lambda i, k=k: r.pay.at[i, :, pl.ds(k * ff, ff)], start=False)
        for k in range(top)
    ]
    rank = y * sizes["c"] + c
    r.pair[rank] = transpose_columns(columns_back + [inner], tok)
    arrive([ship(r.pair.at[rank], r.pair.at[rank], place) for place in tp_peers])
    sums = r.pair[0] + r.pair[1] + r.pair[2] + r.pair[3]
    d_probs = jnp.zeros_like(probs)
    for k in range(top):
        d_probs = d_probs + jnp.where(picks[k], sums[k : k + 1], 0.0)
    d_logits = probs * (d_probs - jnp.sum(probs * d_probs, axis=0, keepdims=True))
    inner_row = sums[top : top + 1] + jnp.sum(d_logits * logits, axis=0, keepdims=True)
    r.late_small[b, 0:8, :] = d_logits * r_mid
    r.late_small[b, 8:16, :] = jnp.broadcast_to(r_mid * r_mid * inner_row / model, (8, tok))
    late_copies = [ship(r.late_small.at[b], r.late_small.at[b], place) for place in b_peers]

    mixer = TwoLevel(net, r.acc, r.sendc, r.recvc, r.sendy, r.recvy, 2)
    pieces = experts * ff // width
    by_piece = width // ff

    def expand(j, i, e):
        columns = r.ids[i]
        value = jnp.zeros((tok, ff), f32)
        for k in range(top):
            taken = r.pay[i, :, (top * j + k) * ff : (top * j + k + 1) * ff].astype(f32)
            value = jnp.where(columns[:, 1 + k : 2 + k] == e, taken, value)
        return value.astype(bf16)

    def use(i):
        def widen(j):
            for e in range(experts):
                g, h = e // by_piece, e % by_piece
                r.wide[j, g * tok : (g + 1) * tok, h * ff : (h + 1) * ff] = expand(j, i, e)

        def times(j, w):
            total = 0.0
            for g in range(pieces):
                piece = w[:, :, g * width : (g + 1) * width].reshape(part, width)
                total = total + dot(r.wide[j, g * tok : (g + 1) * tok, :], piece, NT)
            return total

        widen(1)
        widen(2)
        mixer.put(i, 0, times(1, r.wg) + times(2, r.wu), 0)
        mixer.onward(i, 0, 0)

    @pl.loop(0, nb)
    def _(n):
        index = b
        for k in range(nb - 1):
            index = jnp.where(n == k + 1, pay_line.order[k], index)

        @pl.when(n > 0)
        def _():
            pay_line.take(index)

        @pl.when(n == jnp.where(pay_line.inner, 1, 3))
        def _():
            act_lines[0].begin()

        use(index)

    drain(wd_copies + wg_copies + wu_copies)
    gu_sum.finish()

    def to_a(source, target):
        return [ship(source.at[p["a"]], target.at[k], p) for k, p in enumerate(a_peers)]

    def expert_grad(j, left, target, part_of):
        @pl.loop(part_of * experts // 2, (part_of + 1) * experts // 2)
        def _(e):
            for i in range(nb):
                r.pkv[0, i * tok : (i + 1) * tok, :] = expand(j, i, e)
            grad = dot(left[...].reshape(col, part), r.pkv[0], TN).astype(bf16)
            lane = pl.ds(pl.multiple_of(e * ff, ff), ff)
            for k in range(na):
                target[k, :, lane] = grad[k * sub : (k + 1) * sub, :]

    def half_to_a(source, target, part_of):
        lane = (low, high)[part_of]
        return [
            ship(source.at[p["a"], :, lane], target.at[k, :, lane], p)
            for k, p in enumerate(a_peers)
        ]

    expert_grad(1, r.scaled, r.wg, 0)
    pending = half_to_a(r.wg, r.gate_in, 0)
    arrive(late_copies)
    which16 = lax.broadcasted_iota(jnp.int32, (16, tok), 0)
    ffn_part = jnp.zeros((1, part), f32)
    attn_copies = []
    for i in range(nb):
        columns = jnp.transpose(r.late_small[i, :, mine])
        d_log = jnp.where(which16[:, :half] < experts, r.late_small[i, :, mine], 0.0).astype(bf16)
        mid = mixer.total(i, 0) + dot(d_log, router, TN)
        value = r.hidden[i]
        grad = r.cotc[i, mine, :].astype(f32) + gain_mid * mid - value * columns[:, 8:9]
        r.d_attn[i, mine, :] = grad.astype(bf16)
        attn_copies.append(ship(r.d_attn.at[i, mine, :], r.d_attn.at[i, mine, :], core))
        ffn_part = ffn_part + jnp.sum(mid * value, axis=0, keepdims=True)
        r.d_hidden[i] = grad
    act_lines[0].take(act_lines[0].order[0])
    arrive(attn_copies)

    @pl.loop(0, nb)
    def _(i):
        term = dot(r.d_attn[i], r.wo[...].reshape(part, width)).astype(bf16)
        for h in range(heads):
            r.pq[h, rows_of(i), :] = term[:, h * head : (h + 1) * head]

    heads_sum = net.reduce(r.pq, r.gq, pieces=2)

    expert_grad(1, r.scaled, r.wg, 1)
    pending += half_to_a(r.wg, r.gate_in, 1)
    results = [move(r.wg.at[a], r.gate_own)]
    heads_sum.inner()
    expert_grad(2, r.scaled, r.wu, 0)

    def experts_out():
        for line in act_lines:
            rest(line)

        @pl.loop(0, nb)
        def _(i):
            total = 0.0
            for e in range(experts):
                r.pkv[1, 0:tok, :] = expand(0, i, e)
                piece = r.wd[:, :, e * ff : (e + 1) * ff].reshape(part, ff)
                total = total + dot(r.pkv[1, 0:tok, :], piece, NT)
            mixer.put(i, 1, total, i)

    term = dot(r.d_attn[...].reshape(col, part), r.ho[...], TN).astype(bf16)
    r.gout[...] = term.reshape(na, sub, width)
    pending += to_a(r.gout, r.gout_in)
    extra = 0.0
    for i in range(nb):
        d_log = jnp.where(which16 < experts, r.late_small[i], 0.0).astype(bf16)
        extra = extra + dot(d_log, r.scaled[i])
    which_row = lax.broadcasted_iota(jnp.int32, (16, part), 0)
    r.extra_own[...] = jnp.where(which_row == experts + 1, ffn_part, extra)
    heads_sum.wait()
    for line in act_lines[1:]:
        line.begin()

    r.gain_acc[...] = jnp.zeros_like(r.gain_acc)

    @pl.loop(0, nb)
    def _(i):
        rows = rows_of(i)
        cot = heads_sum.total(rows).astype(bf16)
        r.pq[b, rows, :] = cot
        delta = jnp.sum(cot.astype(f32) * r.ho[rows, head_lane].astype(f32), axis=1, keepdims=True)
        r.stat[rows, 4:5] = delta

    def attend_back(block, first, last, start, stop):
        @pl.loop(start // deep, stop // deep)
        def _(i):
            rows = deep_rows(i)
            columns = deep_ids(i)
            query, cot = r.q_rot[rows, :], r.pq[b, rows, :]
            keys, values = r.kv[block, :, :head], r.kv[block, :, head:]
            scores = dot(query, keys, NT) * scale
            keep = columns[:, 3:4] == r.docs[block]
            probs = jnp.where(keep, jnp.exp(scores - r.stat[rows, 2:3]), 0.0)
            d_scores = (probs * (dot(cot, values, NT) - r.stat[rows, 4:5])).astype(bf16)
            key_term = dot(d_scores, query, TN) * scale
            value_term = dot(probs.astype(bf16), cot, TN)

            @pl.when(i == 0)
            def _():
                r.dkv_acc[:, :head] = key_term
                r.dkv_acc[:, head:] = value_term

            @pl.when(i > 0)
            def _():
                r.dkv_acc[:, :head] += key_term
                r.dkv_acc[:, head:] += value_term

            grad = dot(d_scores, keys) * scale
            if not first:
                grad = r.head_acc[rows, :] + grad
            if not last:
                r.head_acc[rows, :] = grad
            else:
                source = r.raw[rows, :head]
                grad, gain_part = unrope(
                    grad, source, r.gains[0:1, :], r.cos_tab[rows, :], r.sin_tab[rows, :]
                )
                r.gain_acc[0:1, :] += gain_part
                r.wide[0, rows, head_lane] = grad.astype(bf16)
                r.stat[rows, 3:4] = jnp.sum(grad * source, axis=1, keepdims=True)

    kv_back = []
    for k in range(1, na):
        attend_back(lax.rem(a + k, na), k == 1, False, 0, nb)
        r.dkv_send[k - 1] = r.dkv_acc[...].astype(bf16)
        kv_back.append(ship(r.dkv_send.at[k - 1], r.dkv_in.at[k - 1], a_peers[k - 1]))
    for line in act_lines[1:]:
        line.take(line.order[0])
    pending += half_to_a(r.wu, r.up_in, 0)
    q_lines = []
    for s in range(2):
        attend_back(a, na == 1, True, s * (nb // 2), (s + 1) * (nb // 2))
        q_lines.append(
            net.spread(lambda i, s=s: head_block(r.wide.at[0], i, s * (col // 2), col // 2))
        )
    expert_grad(2, r.scaled, r.wu, 1)
    pending += half_to_a(r.wu, r.up_in, 1)
    results.append(move(r.wu.at[a], r.up_own))
    for line in q_lines:
        line.take(line.order[0])
    arrive(kv_back)

    @pl.loop(0, nb)
    def _(i):
        rows = rows_of(i)
        both = r.dkv_acc[rows, :]
        for k in range(na - 1):
            both = both + r.dkv_in[k, rows, :].astype(f32)
        source = r.raw[rows, head : 2 * head]
        grad, gain_part = unrope(
            both[:, :head], source, r.gains[1:2, :], r.cos_tab[rows, :], r.sin_tab[rows, :]
        )
        r.gain_acc[1:2, :] += gain_part
        value_grad = both[:, head:]
        r.wide[1, rows, head_lane] = grad.astype(bf16)
        r.wide[2, rows, head_lane] = value_grad.astype(bf16)
        r.stat[rows, 3:4] += jnp.sum(
            grad * source + value_grad * r.raw[rows, 2 * head :], axis=1, keepdims=True
        )

    place16 = (b * 2 + y) * 2 + c
    r.s4[place16] = transpose_columns([r.stat[i * tok : (i + 1) * tok, 3:4] for i in range(nb)], tok)
    r.s4[place16, 4:6, 0:head] = r.gain_acc[0:2, :]
    s4_copies = [ship(r.s4.at[place16], r.s4.at[place16], place) for place in group]

    def kv_piece(s):
        def block(i):
            lane = pl.ds(pl.multiple_of(i * head, head), head)
            return r.wide.at[pl.ds(1, 2), pl.ds(s * tok, tok), lane]

        return net.spread(block, start=s < 2)

    kv_lines = [kv_piece(s) for s in range(nb)]
    def weight_grad(j):
        grad = dot(r.hn[...].reshape(col, part), r.wide[j], TN).astype(bf16)
        r.gsend[j] = grad.reshape(na, sub, width)
        return to_a(r.gsend.at[j], r.gin_w.at[j])

    for line in q_lines:
        line.take(line.order[1])
        line.take(line.order[2])
    pending += weight_grad(0)
    mixer_in = TwoLevel(net, r.acc, r.sendc, r.recvc, r.sendy, r.recvy, 1)
    mixer.finish()
    def in_term(i):
        rest(kv_lines[i])
        rows = slice(i * tok, (i + 1) * tok)
        term = dot(r.wide[0, rows, :], weight(0), NT) + dot(r.wide[1, rows, :], weight(1), NT)
        mixer_in.put(i, 0, term + dot(r.wide[2, rows, :], weight(2), NT), i)
        mixer_in.onward(i, 0, i)

    chain(kv_lines, 0)
    experts_out()
    chain(kv_lines, 1)
    for i in range(nb):
        mixer.onward(i, 1, i)
    expert_grad(0, r.cotc, r.wd, 0)
    pending += half_to_a(r.wd, r.down_in, 0)
    arrive(s4_copies)
    in_term(0)
    chain(kv_lines, 2)
    expert_grad(0, r.cotc, r.wd, 1)
    pending += half_to_a(r.wd, r.down_in, 1)
    results.append(move(r.wd.at[a], r.down_own))
    in_term(1)
    chain(kv_lines, 3)
    for j in range(nb):
        r.out_half[j] = (r.hidden[j] + mixer.total(j, 1)).astype(bf16)
    r.block_out[mine, own_lane] = r.out_half[b]
    in_term(2)
    in_term(3)
    out_rows = pl.ds(pl.multiple_of(y * quarter, quarter), quarter)
    out_copies = [
        ship(r.out_half.at[d, out_rows, :], r.block_out.at[fourth, own_lane], {"b": d})
        for d in exchange
    ]

    def lanes_onward(copies, rows, place):
        more = []
        for source_b, copy in zip(exchange, copies):
            copy.wait_recv()
            block = r.block_out.at[rows, lane_of(source_b)]
            more.append(ship(block, block, place))
        return more

    pending += weight_grad(1)
    pending += weight_grad(2)
    sums = r.s4[0]
    for k in range(1, 4 * nb):
        sums = sums + r.s4[k]
    inner_columns = jnp.transpose(sums)
    attn_part = jnp.zeros((1, part), f32)
    in_hops = []
    base_in = net.used
    net.used += nb

    def in_hop(d, slot):
        return pltpu.make_async_remote_copy(
            src_ref=r.d_attn.at[d, pl.ds(0, half), :],
            dst_ref=r.gin.at[mine, own_lane],
            send_sem=r.send.at[base_in + d],
            recv_sem=r.recv.at[base_in + slot],
            device_id={"b": jnp.int32(d)},
            device_id_type=MESH,
        )

    drain(attn_copies)
    for i in range(nb):
        d_in = mixer_in.total(i, 0)
        r_col = r.ids[i, mine, 0:1]
        inner = jnp.where(
            c == 0, inner_columns[:half, i : i + 1], inner_columns[half:, i : i + 1]
        )
        x = r.xc[i, mine, :].astype(f32)
        scaled = d_in * r_col
        grad = r.d_hidden[i] + scaled * gain_in - x * (r_col * r_col * inner / model)
        attn_part = attn_part + jnp.sum(scaled * x, axis=0, keepdims=True)
        r.d_attn[i, :half, :] = grad.astype(bf16)

        @pl.when(b == i)
        def _():
            r.gin[mine, own_lane] = r.d_attn[i, :half, :]

        @pl.when(b != i)
        def _():
            in_hop(i, b).start()

    r.extra_own[...] = jnp.where(which_row == experts + 2, attn_part, r.extra_own[...])
    tail_copy = ship(r.extra_own, r.extra_in, core)
    tail_copy.wait_recv()
    shared = (which_row == experts + 1) | (which_row == experts + 2)
    r.tail_all[a] = r.extra_own[...] + jnp.where(shared, r.extra_in[...], 0.0)
    r.tail_all[a, experts + 3 : experts + 5, 0:head] = sums[4:6, 0:head]
    tail_copies = over_a(r.tail_all.at[a], r.tail_all)
    out_y = lanes_onward(out_copies, fourth, across)
    in_more = []
    for k in range(1, nb):
        place = lax.rem(b + k, nb)
        lane = lane_of(place)
        pltpu.make_async_remote_copy(
            src_ref=r.gin.at[mine, lane],
            dst_ref=r.gin.at[mine, lane],
            send_sem=r.send.at[base_in + place],
            recv_sem=r.recv.at[base_in + place],
            device_id=core,
            device_id_type=MESH,
        ).wait_recv()
        in_more.append(ship(r.gin.at[mine, lane], r.gin.at[mine, lane], core))
    in_more.append(ship(r.gin.at[mine, own_lane], r.gin.at[mine, own_lane], core))
    out_more = lanes_onward(out_y, mine, core)
    block = r.block_out.at[mine, own_lane]
    out_more.append(ship(block, block, core))
    arrive(pending)
    for j in range(4):
        mine_here = r.gsend[j, a] if j < 3 else r.gout[a]
        total = mine_here.astype(f32)
        for k in range(na - 1):
            came = r.gin_w[j, k] if j < 3 else r.gout_in[k]
            total = total + came.astype(f32)
        r.proj[j] = total
    results.append(move(r.proj, r.proj_out))
    arrive(out_more)
    results.append(move(r.block_out, r.out_rows))
    arrive(tail_copies)
    r.tail[...] = jnp.sum(r.tail_all[...], axis=0)
    arrive(in_more)
    results.append(move(r.gin, r.in_rows))
    mixer_in.finish()
    mixer.finish((1,))
    for line in [heads_sum, pay_line] + act_lines + cd_sums + ho_lines + q_lines + kv_lines:
        line.finish()
    for d in range(nb):

        @pl.when(b != d)
        def _():
            in_hop(d, b).wait_send()

    drain(list(sent))
    for copy in results:
        copy.wait()
    assert net.used <= r.send.shape[0] and local_used[0] <= r.local.shape[0]


def layer(sizes, dims, ins):
    nb, na, head, heads, experts, ff, top = dims
    tok, model = ins[0].shape
    part, col, half = model // nb, nb * tok, tok // 2
    sub, width, wide = part // na, heads * head, experts * ff
    others = max(na - 1, 1)
    shape = jax.ShapeDtypeStruct
    vmem, hbm = pl.BlockSpec(memory_space=pltpu.VMEM), pl.BlockSpec(memory_space=pl.ANY)
    outs = [
        shape((tok, model), bf16),
        shape((tok, model), bf16),
        shape((sub, wide), bf16),
        shape((sub, wide), bf16),
        shape((sub, wide), bf16),
        shape((others, sub, wide), bf16),
        shape((others, sub, wide), bf16),
        shape((others, sub, wide), bf16),
        shape((4, sub, width), f32),
        shape((16, part), f32),
    ]
    work = dict(
        xc=((nb, tok, part), bf16),
        cotc=((nb, tok, part), bf16),
        rows_all=((na, nb, 8, tok), f32),
        rows_own=((8, tok), f32),
        cols_own=((16, sub), f32),
        cols_all=((na, 16, sub), f32),
        cols_sum=((16, part), f32),
        wqkv=((3, na, sub, width), bf16),
        wo=((na, sub, width), bf16),
        wg=((na, sub, wide), bf16),
        wu=((na, sub, wide), bf16),
        wd=((na, sub, wide), bf16),
        stage=((sub, experts, ff), bf16),
        hn=((nb, tok, part), bf16),
        raw=((col, 3 * head), f32),
        q_rot=((col, head), bf16),
        kv=((na, col, 2 * head), bf16),
        stat=((col, 128), f32),
        ho=((col, width), bf16),
        cos_tab=((col, head), f32),
        sin_tab=((col, head), f32),
        pkv=((nb, col, 2 * head), bf16),
        gkv=((nb, col, 2 * head), bf16),
        pq=((nb, col, head), bf16),
        gq=((nb, col, head), bf16),
        pcd=((top, nb, ff // head * tok, head), bf16),
        gcd=((top, nb, ff // head * tok, head), bf16),
        acc=((nb, half, part), f32),
        sendc=((nb, half, 2 * part), bf16),
        recvc=((nb, half, 2 * part), bf16),
        sendy=((nb, half, 2 * part), bf16),
        recvy=((nb, half, 2 * part), bf16),
        hidden=((nb, half, part), f32),
        d_hidden=((nb, half, part), f32),
        scaled=((nb, tok, part), bf16),
        small=((nb, 16, tok), f32),
        small_in=((nb, 16, tok), f32),
        pay=((nb, tok, 3 * top * ff), bf16),
        wide=((3, col, width), bf16),
        pair=((4, 8, tok), f32),
        late_small=((nb, 16, tok), f32),
        extra_own=((16, part), f32),
        extra_in=((16, part), f32),
        d_attn=((nb, tok, part), bf16),
        out_half=((nb, half, part), bf16),
        block_out=((tok, model), bf16),
        head_acc=((col, head), f32),
        dkv_acc=((col, 2 * head), f32),
        dkv_send=((others, col, 2 * head), bf16),
        dkv_in=((others, col, 2 * head), bf16),
        gsend=((3, na, sub, width), bf16),
        gin_w=((3, others, sub, width), bf16),
        gout=((na, sub, width), bf16),
        gout_in=((others, sub, width), bf16),
        gin=((tok, model), bf16),
        s4=((4 * nb, 8, tok), f32),
        gain_acc=((8, head), f32),
        tail_all=((na, 16, part), f32),
        ids=((nb, tok, 8), f32),
        gains=((8, head), f32),
        docs=((na, 1, col), f32),
        proj=((4, sub, width), f32),
    )
    count = 170 + 26 * na
    scratch = [pltpu.VMEM(*work[name]) for name in WORK[:-3]] + [
        pltpu.SemaphoreType.DMA((count,)),
        pltpu.SemaphoreType.DMA((count,)),
        pltpu.SemaphoreType.DMA((15,)),
    ]
    return pl.pallas_call(
        functools.partial(layer_kernel, sizes, dims),
        out_shape=outs,
        in_specs=[hbm] * 9 + [vmem] * 8,
        out_specs=[hbm] * 9 + [vmem],
        scratch_shapes=scratch,
        compiler_params=pltpu.CompilerParams(
            collective_id=1, has_side_effects=True, vmem_limit_bytes=67043328
        ),
        name="layer",
    )(*ins)


def last_kernel(experts, ff, sub, *refs):
    out_rows, in_rows, owns, cames, proj = refs[0], refs[1], refs[2:5], refs[5:8], refs[8]
    tail, refs = refs[9], refs[10:]
    block_out, grad_in, grads, projections = refs[0], refs[1], refs[2:5], refs[5:9]
    router, gain_attn, gain_ffn, gain_q, gain_k = refs[9:]
    step = 32

    @pl.loop(0, block_out.shape[0] // step)
    def _(n):
        rows = pl.ds(pl.multiple_of(n * step, step), step)
        block_out[rows, :] = out_rows[rows, :]
        grad_in[rows, :] = in_rows[rows, :].astype(f32)

    @pl.loop(0, owns[0].shape[0] // step)
    def _(n):
        rows = pl.ds(pl.multiple_of(n * step, step), step)
        for own, came, grad in zip(owns, cames, grads):
            for e in range(experts):
                lane = slice(e * ff, (e + 1) * ff)
                total = own[rows, lane].astype(f32)
                for k in range(came.shape[0]):
                    total = total + came[k, rows, lane].astype(f32)
                grad[rows, e, :] = total
        for j in range(4):
            projections[j][rows, :] = proj[j, rows, :]

    @pl.when(pl.program_id(0) == 0)
    def _():
        a = lax.axis_index("a")
        piece = tail[:, :sub]
        for k in range(1, tail.shape[1] // sub):
            piece = jnp.where(a == k, tail[:, k * sub : (k + 1) * sub], piece)
        router[...] = piece[:experts]
        gain_ffn[...] = piece[experts + 1 : experts + 2]
        gain_attn[...] = piece[experts + 2 : experts + 3]
        gain_q[...] = tail[experts + 3 : experts + 4, : gain_q.shape[1]]
        gain_k[...] = tail[experts + 4 : experts + 5, : gain_k.shape[1]]


def last(dims, ins):
    nb, na, head, heads, experts, ff, top = dims
    tok, model = ins[0].shape
    sub, wide = ins[2].shape
    others, width = ins[5].shape[0], ins[8].shape[2]
    steps = 2
    shape = jax.ShapeDtypeStruct
    rows = pl.BlockSpec((tok // steps, model), lambda i: (i, 0))
    own = pl.BlockSpec((sub // steps, wide), lambda i: (i, 0))
    came = pl.BlockSpec((others, sub // steps, wide), lambda i: (0, i, 0))
    grad = pl.BlockSpec((sub // steps, experts, ff), lambda i: (i, 0, 0))
    flat = pl.BlockSpec((sub // steps, width), lambda i: (i, 0))
    small = [shape((experts, sub), f32), shape((1, sub), f32), shape((1, sub), f32)]
    small += [shape((1, head), f32)] * 2
    return pl.pallas_call(
        functools.partial(last_kernel, experts, ff, sub),
        grid=(steps,),
        out_shape=[shape((tok, model), bf16), shape((tok, model), f32)]
        + [shape((sub, experts, ff), f32)] * 3
        + [shape((sub, width), f32)] * 4
        + small,
        in_specs=[rows, rows] + [own] * 3 + [came] * 3
        + [pl.BlockSpec((4, sub // steps, width), lambda i: (0, i, 0))]
        + [pl.BlockSpec(ins[9].shape, lambda i: (0, 0))],
        out_specs=[rows, rows] + [grad] * 3 + [flat] * 4
        + [pl.BlockSpec(item.shape, lambda i: (0, 0)) for item in small],
        name="last",
    )(*ins)


def on_device(
    sizes,
    tokens_in,
    doc_ids,
    expert_ids,
    attn_gain,
    q_gain,
    k_gain,
    w_query,
    w_key,
    w_value,
    w_output,
    ffn_gain,
    w_router,
    w_gate,
    w_up,
    w_down,
    cotangent,
):
    nb, na = sizes["b"], sizes["a"]
    tok, model = tokens_in.shape
    part = model // nb
    sub = part // na
    head = q_gain.shape[0]
    width = w_query.shape[1]
    heads = width // head
    experts, ff = w_gate.shape[1], w_gate.shape[2]
    top = expert_ids.shape[1]
    dims = (nb, na, head, heads, experts, ff, top)

    speed = theta ** (-2.0 * (np.arange(head) % (head // 2)) / head)
    parts = layer(
        sizes,
        dims,
        [
            tokens_in, cotangent, w_query, w_key, w_value, w_output, w_gate, w_up, w_down,
            expert_ids.T, doc_ids[None], w_router.T, attn_gain, ffn_gain, q_gain[None],
            k_gain[None], jnp.asarray(speed, f32)[None],
        ],
    )
    (
        block_out, grad_in, grad_gate, grad_up, grad_down, grad_query, grad_key, grad_value,
        grad_output, router, gain_attn, gain_ffn, gain_q, gain_k,
    ) = last(dims, parts)
    return (
        block_out,
        grad_in,
        gain_attn.reshape(sub),
        gain_q.reshape(head),
        gain_k.reshape(head),
        grad_query,
        grad_key,
        grad_value,
        grad_output,
        gain_ffn.reshape(sub),
        router.T,
        grad_gate,
        grad_up,
        grad_down,
    )


def solution(mesh):
    cp, tp = mesh.shape["cp"], mesh.shape["tp"]
    sizes = {"b": 4, "a": cp // 4, "y": 2, "c": tp // 2}
    split = Mesh(mesh.devices.reshape([sizes[axis] for axis in AXES]), AXES)
    cp, tp = ("b", "a"), ("y", "c")
    return jax.shard_map(
        functools.partial(on_device, sizes),
        mesh=split,
        in_specs=(
            P(cp, None),
            P(cp),
            P(cp, None),
            P(cp),
            P(),
            P(),
            P(cp, tp),
            P(cp, tp),
            P(cp, tp),
            P(cp, tp),
            P(cp),
            P(cp, None),
            P(cp, None, tp),
            P(cp, None, tp),
            P(cp, None, tp),
            P(cp, None),
        ),
        out_specs=(
            P(cp, None),
            P(cp, None),
            P(cp),
            P(),
            P(),
            P(cp, tp),
            P(cp, tp),
            P(cp, tp),
            P(cp, tp),
            P(cp),
            P(cp, None),
            P(cp, None, tp),
            P(cp, None, tp),
            P(cp, None, tp),
        ),
        check_vma=False,
    )
```

```python
import functools
import types

import jax
import jax.numpy as jnp
import numpy as np
from jax import lax
from jax.experimental import pallas as pl
from jax.experimental.pallas import tpu as pltpu
from jax.sharding import Mesh
from jax.sharding import PartitionSpec as P

eps = 1e-05
theta = 50000.0
negative = -1e30
AXES = ("b", "a", "y", "c")
MESH = pl.DeviceIdType.MESH
bf16 = jnp.bfloat16
f32 = jnp.float32


NT = (((1,), (1,)), ((), ()))
TN = (((0,), (0,)), ((), ()))


def dot(left, right, dims=(((1,), (0,)), ((), ()))):
    return lax.dot_general(left, right, dims, preferred_element_type=f32)


class Net:
    def __init__(self, sizes, send, recv):
        self.sizes, self.send, self.recv, self.used = sizes, send, recv, 0
        self.me = {axis: lax.axis_index(axis) for axis in AXES}

    def near(self, **offs):
        return {axis: lax.rem(self.me[axis] + off, self.sizes[axis]) for axis, off in offs.items()}

    def copy(self, source, target, place):
        slot = self.used
        self.used += 1
        return pltpu.make_async_remote_copy(
            src_ref=source,
            dst_ref=target,
            send_sem=self.send.at[slot],
            recv_sem=self.recv.at[slot],
            device_id=place,
            device_id_type=MESH,
        )

    def greet(self, places):
        barrier = pltpu.get_barrier_semaphore()
        for place in places:
            pl.semaphore_signal(barrier, inc=1, device_id=place, device_id_type=MESH)
        pl.semaphore_wait(barrier, len(places))

    def pick(self, *values):
        result = values[-1]
        for i in range(len(values) - 2, -1, -1):
            result = jnp.where(self.me["b"] == i, values[i], result)
        return result

    def reduce(self, *args):
        return Reduce(self, *args)

    def spread(self, *blocks, start=True):
        return Spread(self, blocks, start)


class Reduce:
    def __init__(self, net, parts, got, make=None):
        self.net, self.parts, self.got = net, parts, got
        self.b = b = net.me["b"]
        self.base = net.used
        net.used += 4
        self.order = [3 - b, net.pick(2, 0, 3, 1), net.pick(1, 3, 0, 2)]
        if make is None:
            for k in range(2):
                self.hop(self.order[k]).start()
            return
        if net.sizes["a"] > 2:
            for k in range(3):
                make(self.order[k])
                if k < 2:
                    self.hop(self.order[k]).start()
            return

        @pl.loop(0, 3)
        def _(k):
            d = jnp.where(k == 0, self.order[0], jnp.where(k == 1, self.order[1], self.order[2]))
            make(d)

            @pl.when(k < 2)
            def _():
                self.hop(d).start()

    def hop(self, d):
        net, b = self.net, self.b
        far = ((b == 0) & (d == 3)) | ((b == 3) & (d == 0))
        beside = jnp.where(b == 0, 1, 2)
        target, slot = jnp.where(far, beside, d), jnp.where(far, beside, b)
        return pltpu.make_async_remote_copy(
            src_ref=self.parts.at[d],
            dst_ref=self.got.at[slot],
            send_sem=net.send.at[self.base + d],
            recv_sem=net.recv.at[self.base + slot],
            device_id={"b": target},
            device_id_type=MESH,
        )

    def came(self, i):
        net = self.net
        return pltpu.make_async_remote_copy(
            src_ref=self.got.at[i],
            dst_ref=self.got.at[i],
            send_sem=net.send.at[self.base + i],
            recv_sem=net.recv.at[self.base + i],
            device_id=net.near(b=1),
            device_id_type=MESH,
        )

    def inner(self):
        b, d = self.b, self.order[2]

        @pl.when((b == 1) | (b == 2))
        def _():
            self.came(b).wait_recv()
            rows = self.parts.shape[1]
            step = 256 if rows % 256 == 0 else rows

            @pl.loop(0, rows // step)
            def _(i):
                sl = pl.ds(pl.multiple_of(i * step, step), step)
                total = self.parts[d, sl, :].astype(f32) + self.got[b, sl, :].astype(f32)
                self.parts[d, sl, :] = total.astype(bf16)

        self.hop(d).start()

    def wait(self):
        for i in range(4):

            @pl.when((self.b != i) & (jnp.abs(self.b - i) <= 2))
            def _():
                self.came(i).wait_recv()

    def total(self, *index):
        b = self.b
        value = self.parts[(b,) + index].astype(f32)
        for i in range(4):
            valid = (b != i) & (jnp.abs(b - i) <= 2)
            value = value + jnp.where(valid, self.got[(i,) + index].astype(f32), 0.0)
        return value

    def finish(self):
        for d in range(4):

            @pl.when(self.b != d)
            def _():
                self.hop(d).wait_send()


class Spread:
    def __init__(self, net, blocks, start):
        self.net, self.blocks = net, blocks
        self.b = b = net.me["b"]
        self.base = net.used
        net.used += 4 * len(blocks)
        self.targets = [net.pick(2, 3, 0, 1), net.pick(1, 0, 3, 2), net.pick(2, 2, 1, 1)]
        self.order = [net.pick(1, 3, 0, 2), net.pick(2, 0, 3, 1), net.pick(3, 2, 1, 0)]
        self.inner = (b == 1) | (b == 2)
        if start:
            self.begin()

    def begin(self):
        for k, target in enumerate(self.targets):
            if k < 2:
                for j in range(len(self.blocks)):
                    self.hop(self.b, target, target, j).start()
            else:

                @pl.when(self.inner)
                def _():
                    for j in range(len(self.blocks)):
                        self.hop(self.b, target, target, j).start()

    def hop(self, i, target, slot, j):
        net, count = self.net, len(self.blocks)
        return pltpu.make_async_remote_copy(
            src_ref=self.blocks[j](i),
            dst_ref=self.blocks[j](i),
            send_sem=net.send.at[self.base + slot * count + j],
            recv_sem=net.recv.at[self.base + i * count + j],
            device_id={"b": target},
            device_id_type=MESH,
        )

    def take(self, i):
        b = self.b
        onward = ((b == 1) & (i == 3)) | ((b == 2) & (i == 0))
        for j in range(len(self.blocks)):
            self.hop(i, self.net.near(b=1)["b"], b, j).wait_recv()

            @pl.when(onward)
            def _():
                self.hop(i, jnp.where(b == 1, 0, 3), b, j).start()

    def take_all(self):
        for i in self.order:
            self.take(i)

    def finish(self):
        b = self.b
        for k, target in enumerate(self.targets):
            for j in range(len(self.blocks)):
                if k < 2:
                    self.hop(b, target, target, j).wait_send()
                else:

                    @pl.when(self.inner)
                    def _():
                        self.hop(b, target, target, j).wait_send()
                        self.hop(b, jnp.where(b == 1, 0, 3), b, j).wait_send()


def rope(values, cos_tab, sin_tab):
    return values * cos_tab + pltpu.roll(values, values.shape[1] // 2, 1) * sin_tab


def head_norm(values):
    return lax.rsqrt(jnp.mean(values * values, axis=1, keepdims=True) + eps)


def unrope(grad, raw, gain, cos_tab, sin_tab):
    factor = head_norm(raw)
    normed = raw * factor
    turned = grad * cos_tab + pltpu.roll(grad * sin_tab, grad.shape[1] // 2, 1)
    gain_part = jnp.sum(turned * normed, axis=0, keepdims=True)
    inner = turned * gain
    slope = jnp.mean(raw * inner, axis=1, keepdims=True)
    return factor * inner - raw * (factor * factor * factor * slope), gain_part


class TwoLevel:
    def __init__(self, net, acc, sendc, recvc, sendy, recvy, kinds):
        self.net, self.acc = net, acc
        self.sendc, self.recvc, self.sendy, self.recvy = sendc, recvc, sendy, recvy
        self.base = net.used
        self.kinds = kinds
        net.used += 8 * kinds
        self.part = acc.shape[2]
        self.half = acc.shape[1]

    def lane(self, j):
        return slice(j * self.part, (j + 1) * self.part)

    def hop(self, i, j, level):
        net = self.net
        source, target = ((self.sendc, self.recvc), (self.sendy, self.recvy))[level]
        slot = self.base + 4 * self.kinds * level + self.kinds * i + j
        lane = pl.ds(j * self.part, self.part)
        return pltpu.make_async_remote_copy(
            src_ref=source.at[i, :, lane],
            dst_ref=target.at[i, :, lane],
            send_sem=net.send.at[slot],
            recv_sem=net.recv.at[slot],
            device_id=net.near(c=1) if level == 0 else net.near(y=1),
            device_id_type=MESH,
        )

    def put(self, i, j, term, k):
        first = self.net.me["c"] == 0
        low, high = term[: self.half], term[self.half :]
        self.acc[k] = jnp.where(first, low, high)
        self.sendc[i, :, self.lane(j)] = jnp.where(first, high, low).astype(bf16)
        self.hop(i, j, 0).start()

    def onward(self, i, j, k):
        self.hop(i, j, 0).wait_recv()
        total = self.acc[k] + self.recvc[i, :, self.lane(j)].astype(f32)
        self.sendy[i, :, self.lane(j)] = total.astype(bf16)
        self.hop(i, j, 1).start()

    def total(self, i, j):
        self.hop(i, j, 1).wait_recv()
        lane = self.lane(j)
        return self.sendy[i, :, lane].astype(f32) + self.recvy[i, :, lane].astype(f32)

    def finish(self, kinds=(0,)):
        for i in range(4):
            for j in kinds:
                self.hop(i, j, 0).wait_send()
                self.hop(i, j, 1).wait_send()


def transpose_columns(columns, rows):
    lane = lax.broadcasted_iota(jnp.int32, (rows, 128), 1)
    table = jnp.zeros((rows, 128), f32)
    for k, column in enumerate(columns):
        table = jnp.where(lane == k, column, table)
    return jnp.transpose(table)[:8, :]


INS = (
    "tok", "cot", "wq_in", "wk_in", "wv_in", "wo_in", "wg_in", "wu_in", "wd_in", "ids_in",
    "docs_in", "router_in", "gain_in_a", "gain_in_f", "gain_q", "gain_k", "speed_in",
)
OUTS = (
    "out_rows", "in_rows", "gate_own", "up_own", "down_own", "gate_in", "up_in", "down_in",
    "proj_out", "tail",
)
WORK = (
    "xc", "cotc", "rows_all", "rows_own", "cols_own", "cols_all", "cols_sum", "wqkv", "wo",
    "wg", "wu", "wd", "stage", "hn", "raw", "q_rot", "kv", "stat", "ho", "cos_tab", "sin_tab",
    "pkv", "gkv", "pq", "gq", "pcd", "gcd", "acc", "sendc", "recvc", "sendy", "recvy", "hidden", "d_hidden", "scaled",
    "small", "small_in", "pay", "wide", "pair", "late_small", "extra_own", "extra_in", "d_attn",
    "out_half", "block_out", "head_acc", "dkv_acc", "dkv_send", "dkv_in", "gsend", "gin_w",
    "gout", "gout_in", "gin", "s4", "gain_acc", "tail_all", "gains", "ids", "docs", "proj",
    "send", "recv", "local",
)


def layer_kernel(sizes, dims, *refs):
    r = types.SimpleNamespace(**dict(zip(INS + OUTS + WORK, refs)))
    nb, na, head, heads, experts, ff, top = dims
    net = Net(sizes, r.send, r.recv)
    me = net.me
    b, a, y, c = me["b"], me["a"], me["y"], me["c"]
    tok, part = r.xc.shape[1], r.xc.shape[2]
    half, col, model, width, sub = tok // 2, nb * tok, nb * part, heads * head, part // na
    scale = head**-0.5
    mine = pl.ds(pl.multiple_of(c * half, half), half)
    own_lane = pl.ds(pl.multiple_of(b * part, part), part)
    head_lane = pl.ds(pl.multiple_of(b * head, head), head)
    core, across = net.near(c=1), net.near(y=1)
    b_peers = [net.near(b=k) for k in range(1, nb)]
    a_peers = [net.near(a=k) for k in range(1, na)]
    group = [
        net.near(b=i, y=j, c=k)
        for i in range(nb) for j in range(2) for k in range(2) if i or j or k
    ]
    tp_peers = [net.near(y=j, c=k) for j in range(2) for k in range(2) if j or k]
    sent = []
    local_used = [0]

    def rows_of(i):
        return pl.ds(pl.multiple_of(i * tok, tok), tok)

    def lane_of(place):
        return pl.ds(pl.multiple_of(place * part, part), part)

    def move(source, target):
        copy = pltpu.make_async_copy(source, target, r.local.at[local_used[0]])
        local_used[0] += 1
        copy.start()
        return copy

    def ship(source, target, place):
        copy = net.copy(source, target, place)
        copy.start()
        sent.append(copy)
        return copy

    def arrive(copies):
        for copy in copies:
            copy.wait_recv()

    def drain(copies):
        for copy in copies:
            copy.wait_send()
            sent[:] = [other for other in sent if other is not copy]

    tok_here = move(r.tok, r.gin)
    w_here = [move(w, r.wqkv.at[j, a]) for j, w in ((1, r.wk_in), (2, r.wv_in), (0, r.wq_in))]
    stage_copy = move(r.wd_in, r.stage)
    late_here = [move(r.wo_in, r.wo.at[a]), move(r.cot.at[:, own_lane], r.cotc.at[b])]
    net.greet(group + [net.near(b=j, a=k) for j in range(nb) for k in range(1, na)])

    r.cols_own[...] = jnp.zeros_like(r.cols_own)
    r.cols_own[0:experts, :] = r.router_in[...].astype(f32)
    r.cols_own[experts : experts + 1, :] = r.gain_in_a[...].astype(f32).reshape(1, sub)
    r.cols_own[experts + 1 : experts + 2, :] = r.gain_in_f[...].astype(f32).reshape(1, sub)
    r.gains[0:1, :] = r.gain_q[...].astype(f32)
    r.gains[1:2, :] = r.gain_k[...].astype(f32)
    r.gains[2:3, :] = r.speed_in[...]
    r.rows_own[...] = jnp.zeros_like(r.rows_own)
    r.rows_own[1 : 1 + top, :] = r.ids_in[...].astype(f32)
    r.rows_own[3:4, :] = r.docs_in[...].astype(f32)

    exchange = [net.pick(2, 3, 0, 1), net.pick(3, 2, 1, 0), net.pick(1, 0, 3, 2)]

    quarter = half // 2
    fourth = pl.ds(pl.multiple_of(c * half + y * quarter, quarter), quarter)

    def to_quarters(source, target):
        return [
            ship(source.at[fourth, lane_of(d)], target.at[b, fourth, :], {"b": d})
            for d in exchange
        ]

    def over_a(source, target):
        return [ship(source, target.at[a], place) for place in a_peers]

    def onward(copies, target, rows, place):
        more = []
        for source_b, copy in zip(exchange, copies):
            copy.wait_recv()
            block = target.at[source_b, rows, :]
            more.append(ship(block, block, place))
        return more

    x_copies = to_quarters(r.tok, r.xc)
    cols_copies = over_a(r.cols_own, r.cols_all)
    r.cols_all[a] = r.cols_own[...]
    kv_weights = over_a(r.wk_in, r.wqkv.at[1]) + over_a(r.wv_in, r.wqkv.at[2])
    q_weights = over_a(r.wq_in, r.wqkv.at[0])
    tok_here.wait()
    square_columns = []
    for s in range(tok // 64):
        piece = r.gin[s * 64 : (s + 1) * 64, :].astype(f32)
        square_columns.append(jnp.sum(piece * piece, axis=1, keepdims=True))
    squares = transpose_columns([jnp.concatenate(square_columns, axis=0)], tok)[0:1, :]
    which8 = lax.broadcasted_iota(jnp.int32, (8, tok), 0)
    r.rows_own[0:1, :] = lax.rsqrt(squares / model + eps)
    rows_copies = [ship(r.rows_own, r.rows_all.at[a, b], place) for place in b_peers]
    rows_far = [
        ship(r.rows_own, r.rows_all.at[a, b], net.near(b=j, a=k))
        for j in range(nb) for k in range(1, na)
    ]
    r.rows_all[a, b] = r.rows_own[...]
    r.xc[b] = r.gin[:, own_lane]
    cot_copies = to_quarters(r.cot, r.cotc)
    wo_copies = over_a(r.wo_in, r.wo)

    def relayout(target):
        step = 32

        @pl.loop(0, sub // step)
        def _(n):
            rows = pl.ds(pl.multiple_of(n * step, step), step)
            turned = jnp.swapaxes(r.stage[rows].astype(f32), 0, 1)
            for e in range(experts):
                target[a, rows, e * ff : (e + 1) * ff] = turned[e].astype(bf16)

    stage_copy.wait()
    relayout(r.wd)
    wd_copies = over_a(r.wd.at[a], r.wd)
    stage_copy = move(r.wg_in, r.stage)

    lane_index = lax.broadcasted_iota(jnp.int32, (tok, head), 1)
    row_index = lax.broadcasted_iota(jnp.int32, (tok, head), 0)

    @pl.loop(0, nb)
    def _(i):
        place = ((i * na + a) * tok + row_index).astype(f32)
        angle = place * r.gains[2:3, :]
        r.cos_tab[rows_of(i), :] = jnp.cos(angle)
        turned = jnp.sin(angle)
        r.sin_tab[rows_of(i), :] = jnp.where(lane_index < head // 2, -turned, turned)

    x_y = onward(x_copies, r.xc, fourth, across)
    x_more = onward(x_y, r.xc, mine, core)
    arrive(rows_copies + cols_copies + x_more)
    arrive(kv_weights)
    for copy in w_here:
        copy.wait()
    for k in range(na):
        r.cols_sum[:, k * sub : (k + 1) * sub] = r.cols_all[k]
    gain_in = r.cols_sum[experts : experts + 1, :]
    for i in range(nb):
        columns = jnp.transpose(r.rows_all[a, i])
        r.ids[i] = columns
        r.hn[i] = (r.xc[i].astype(f32) * columns[:, 0:1] * gain_in).astype(bf16)

    def weight(j):
        return r.wqkv[j].reshape(part, width)

    @pl.loop(0, nb)
    def _(i):
        for j in (1, 2):
            term = dot(r.hn[i], weight(j)).astype(bf16)
            for h in range(heads):
                piece = term[:, h * head : (h + 1) * head]
                r.pkv[h, rows_of(i), (j - 1) * head : j * head] = piece

    kv_sum = net.reduce(r.pkv, r.gkv)
    cot_y = onward(cot_copies, r.cotc, fourth, across)
    arrive(q_weights)

    @pl.loop(0, nb)
    def _(i):
        term = dot(r.hn[i], weight(0)).astype(bf16)
        for h in range(heads):
            r.pq[h, rows_of(i), :] = term[:, h * head : (h + 1) * head]

    stage_copy.wait()
    relayout(r.wg)
    low, high = (pl.ds(k * experts * ff // 2, experts * ff // 2) for k in range(2))

    def half_over_a(array, lane):
        return [ship(array.at[a, :, lane], array.at[a, :, lane], place) for place in a_peers]

    wg_copies = half_over_a(r.wg, low)
    stage_copy = move(r.wu_in, r.stage)
    kv_sum.inner()
    q_sum = net.reduce(r.pq, r.gq)
    stage_copy.wait()
    relayout(r.wu)
    q_sum.inner()
    cot_more = onward(cot_y, r.cotc, mine, core)
    kv_sum.wait()

    @pl.loop(0, nb)
    def _(i):
        rows = rows_of(i)
        both = kv_sum.total(rows)
        r.raw[rows, head:] = both
        keys = both[:, :head]
        normed = keys * head_norm(keys) * r.gains[1:2, :]
        r.kv[a, rows, :head] = rope(normed, r.cos_tab[rows, :], r.sin_tab[rows, :]).astype(bf16)
        r.kv[a, rows, head:] = both[:, head:].astype(bf16)

    kv_copies = over_a(r.kv.at[a], r.kv)
    wg_copies += half_over_a(r.wg, high)
    wu_copies = over_a(r.wu.at[a], r.wu)
    arrive(wd_copies + cot_more)
    for copy in late_here:
        copy.wait()

    def chosen(left, weights, d, put):
        columns = r.ids[d]
        values = [jnp.zeros((tok, ff), f32) for k in range(top)]
        for e in range(experts):
            term = dot(left, weights[:, :, e * ff : (e + 1) * ff].reshape(part, ff))
            for k in range(top):
                values[k] = jnp.where(columns[:, 1 + k : 2 + k] == e, term, values[k])
        for k in range(top):
            put(k, values[k].astype(bf16))

    groups = ff // head

    @pl.loop(0, nb)
    def _(i):
        def put(k, value):
            for g in range(groups):
                r.pcd[k, i, g * tok : (g + 1) * tok, :] = value[:, g * head : (g + 1) * head]

        chosen(r.cotc[i], r.wd, i, put)

    cd_sums = [net.reduce(r.pcd.at[0], r.gcd.at[0])]
    arrive(rows_far)
    for i in range(nb):
        for j in range(na):
            r.docs[j, :, i * tok : (i + 1) * tok] = r.rows_all[j, i][3:4, :]
    q_sum.wait()

    @pl.loop(0, nb)
    def _(i):
        rows = rows_of(i)
        query = q_sum.total(rows)
        r.raw[rows, :head] = query
        normed = query * head_norm(query) * r.gains[0:1, :]
        r.q_rot[rows, :] = rope(normed, r.cos_tab[rows, :], r.sin_tab[rows, :]).astype(bf16)

    cd_sums[0].inner()

    deep = 2 if na <= 2 else 1

    def deep_rows(i):
        return pl.ds(pl.multiple_of(i * deep * tok, deep * tok), deep * tok)

    def deep_ids(i):
        return r.ids[pl.ds(i * deep, deep)].reshape(deep * tok, 8)

    def attend(block, first, last):
        @pl.loop(0, nb)
        def _(i):
            rows = rows_of(i)
            columns = r.ids[i]
            scores = dot(r.q_rot[rows, :], r.kv[block, :, :head], NT) * scale
            scores = jnp.where(columns[:, 3:4] == r.docs[block], scores, negative)
            most = jnp.max(scores, axis=1, keepdims=True)
            if not first:
                before = r.stat[rows, 0:1]
                most = jnp.maximum(before, most)
            terms = jnp.exp(scores - most)
            total = jnp.sum(terms, axis=1, keepdims=True)
            mixed = dot(terms.astype(bf16), r.kv[block, :, head:])
            if not first:
                fade = jnp.exp(before - most)
                total = r.stat[rows, 1:2] * fade + total
                mixed = r.head_acc[rows, :] * fade + mixed
            if last:
                r.ho[rows, head_lane] = (mixed * (1.0 / total)).astype(bf16)
                r.stat[rows, 2:3] = most + jnp.log(total)
            else:
                r.stat[rows, 0:1] = most
                r.stat[rows, 1:2] = total
                r.head_acc[rows, :] = mixed

    attend(a, True, na == 1)
    for k in range(1, na):
        kv_copies[k - 1].wait_recv()
        attend(lax.rem(a + na - k, na), False, k == na - 1)

    def head_block(array, i, start, size):
        return array.at[pl.ds(start, size), pl.ds(pl.multiple_of(i * head, head), head)]

    def chain(lines, i):
        lines[i].take(lines[i].order[0])
        if i + 2 < len(lines):
            lines[i + 2].begin()

    def rest(line):
        line.take(line.order[1])
        line.take(line.order[2])

    ho_lines = [
        net.spread(lambda i, s=s: head_block(r.ho, i, s * tok, tok), start=s < 2)
        for s in range(nb)
    ]
    arrive(wo_copies)

    mixer = TwoLevel(net, r.acc, r.sendc, r.recvc, r.sendy, r.recvy, 1)
    for i in range(nb):
        chain(ho_lines, i)
        rest(ho_lines[i])
        if i == nb - 1:
            for k in range(1, top):
                cd_sums.append(net.reduce(r.pcd.at[k], r.gcd.at[k]))
        term = dot(r.ho[i * tok : (i + 1) * tok, :], r.wo[...].reshape(part, width), NT)
        mixer.put(i, 0, term, i)
        if i:
            mixer.onward(i - 1, 0, i - 1)
    mixer.onward(nb - 1, 0, nb - 1)
    for group_sum in cd_sums[1:]:
        group_sum.inner()
    gain_mid = r.cols_sum[experts + 1 : experts + 2, :]
    router = r.cols_sum[...].astype(bf16)
    last_copies = []
    for i in range(nb):
        value = r.xc[i, mine, :].astype(f32) + mixer.total(i, 0)
        r.hidden[i] = value
        piece = (value * gain_mid).astype(bf16)
        r.scaled[i, mine, :] = piece
        logits = dot(router, piece, NT)
        squares = jnp.sum(value * value, axis=1, keepdims=True)
        squares = jnp.transpose(jnp.broadcast_to(squares, (half, 128)))[:1, :]
        which = lax.broadcasted_iota(jnp.int32, logits.shape, 0)
        r.small[i, :, mine] = jnp.where(which == experts, squares, logits)
        for array in (r.scaled.at[i, mine, :], r.small.at[i, :, mine]):
            last_copies.append(ship(array, array, core))
    arrive(wg_copies + wu_copies + last_copies)
    mixer.finish()
    kv_sum.finish()
    q_sum.finish()

    small_copies = [ship(r.small.at[p["b"]], r.small_in.at[b], p) for p in b_peers]
    r.small_in[b] = r.small[b]

    def make(d):
        for j, w in enumerate((r.wg, r.wu)):

            def put(k, value, j=j):
                r.pkv[d, (2 * k + j) * tok : (2 * k + j + 1) * tok, :] = value

            chosen(r.scaled[d], w, d, put)

    gu_sum = net.reduce(r.pkv, r.gkv, make)
    gu_sum.inner()
    make(b)
    arrive(small_copies)
    for group_sum in cd_sums:
        group_sum.wait()
    gu_sum.wait()
    total = jnp.sum(r.small_in[...], axis=0)
    r_mid = lax.rsqrt(total[experts : experts + 1] / model + eps)
    logits = total[:experts] * r_mid
    terms = jnp.exp(logits - jnp.max(logits, axis=0, keepdims=True))
    probs = terms / jnp.sum(terms, axis=0, keepdims=True)
    which = lax.broadcasted_iota(jnp.int32, probs.shape, 0).astype(f32)
    picks = [r.rows_own[1 + k : 2 + k] == which for k in range(top)]
    combine = [jnp.sum(jnp.where(pick, probs, 0.0), axis=0, keepdims=True) for pick in picks]
    table = jnp.where(which8 == 0, r_mid, 0.0)
    for k in range(top):
        table = jnp.where(which8 == 1 + k, combine[k], table)
    columns = jnp.transpose(table)
    r_col = columns[:, 0:1]
    columns_back = []
    inner = jnp.zeros((tok, 1), f32)
    for k in range(top):
        gate = gu_sum.total(slice((2 * k) * tok, (2 * k + 1) * tok)) * r_col
        up = gu_sum.total(slice((2 * k + 1) * tok, (2 * k + 2) * tok)) * r_col
        back = jnp.concatenate(
            [
                cd_sums[k].total(slice(g * tok, (g + 1) * tok))
                for g in range(groups)
            ],
            axis=1,
        )
        sig = 1.0 / (1.0 + jnp.exp(-gate))
        silu = gate * sig
        act = silu * up
        weighed = columns[:, 1 + k : 2 + k]
        d_act = weighed * back
        d_gate = d_act * up * (sig * (1.0 + gate * (1.0 - sig)))
        d_up = d_act * silu
        for j, value in enumerate((weighed * act, d_gate * r_col, d_up * r_col)):
            r.pay[b, :, (top * j + k) * ff : (top * j + k + 1) * ff] = value.astype(bf16)
        columns_back.append(jnp.sum(act * back, axis=1, keepdims=True))
        inner = inner + jnp.sum(d_gate * gate + d_up * up, axis=1, keepdims=True)

    pay_line = net.spread(lambda i: r.pay.at[i, :, pl.ds(top * ff, 2 * top * ff)])
    act_lines = [
        net.spread(lambda i, k=k: r.pay.at[i, :, pl.ds(k * ff, ff)], start=False)
        for k in range(top)
    ]
    rank = y * sizes["c"] + c
    r.pair[rank] = transpose_columns(columns_back + [inner], tok)
    arrive([ship(r.pair.at[rank], r.pair.at[rank], place) for place in tp_peers])
    sums = r.pair[0] + r.pair[1] + r.pair[2] + r.pair[3]
    d_probs = jnp.zeros_like(probs)
    for k in range(top):
        d_probs = d_probs + jnp.where(picks[k], sums[k : k + 1], 0.0)
    d_logits = probs * (d_probs - jnp.sum(probs * d_probs, axis=0, keepdims=True))
    inner_row = sums[top : top + 1] + jnp.sum(d_logits * logits, axis=0, keepdims=True)
    r.late_small[b, 0:8, :] = d_logits * r_mid
    r.late_small[b, 8:16, :] = jnp.broadcast_to(r_mid * r_mid * inner_row / model, (8, tok))
    late_copies = [ship(r.late_small.at[b], r.late_small.at[b], place) for place in b_peers]

    mixer = TwoLevel(net, r.acc, r.sendc, r.recvc, r.sendy, r.recvy, 2)
    pieces = experts * ff // width
    by_piece = width // ff

    def expand(j, i, e):
        columns = r.ids[i]
        value = jnp.zeros((tok, ff), f32)
        for k in range(top):
            taken = r.pay[i, :, (top * j + k) * ff : (top * j + k + 1) * ff].astype(f32)
            value = jnp.where(columns[:, 1 + k : 2 + k] == e, taken, value)
        return value.astype(bf16)

    def use(i):
        def widen(j):
            for e in range(experts):
                g, h = e // by_piece, e % by_piece
                r.wide[j, g * tok : (g + 1) * tok, h * ff : (h + 1) * ff] = expand(j, i, e)

        def times(j, w):
            total = 0.0
            for g in range(pieces):
                piece = w[:, :, g * width : (g + 1) * width].reshape(part, width)
                total = total + dot(r.wide[j, g * tok : (g + 1) * tok, :], piece, NT)
            return total

        widen(1)
        widen(2)
        mixer.put(i, 0, times(1, r.wg) + times(2, r.wu), 0)
        mixer.onward(i, 0, 0)

    @pl.loop(0, nb)
    def _(n):
        index = b
        for k in range(nb - 1):
            index = jnp.where(n == k + 1, pay_line.order[k], index)

        @pl.when(n > 0)
        def _():
            pay_line.take(index)

        @pl.when(n == jnp.where(pay_line.inner, 1, 3))
        def _():
            act_lines[0].begin()

        use(index)

    drain(wd_copies + wg_copies + wu_copies)
    gu_sum.finish()

    def to_a(source, target):
        return [ship(source.at[p["a"]], target.at[k], p) for k, p in enumerate(a_peers)]

    def expert_grad(j, left, target, part_of):
        @pl.loop(part_of * experts // 2, (part_of + 1) * experts // 2)
        def _(e):
            for i in range(nb):
                r.pkv[0, i * tok : (i + 1) * tok, :] = expand(j, i, e)
            grad = dot(left[...].reshape(col, part), r.pkv[0], TN).astype(bf16)
            lane = pl.ds(pl.multiple_of(e * ff, ff), ff)
            for k in range(na):
                target[k, :, lane] = grad[k * sub : (k + 1) * sub, :]

    def half_to_a(source, target, part_of):
        lane = (low, high)[part_of]
        return [
            ship(source.at[p["a"], :, lane], target.at[k, :, lane], p)
            for k, p in enumerate(a_peers)
        ]

    expert_grad(1, r.scaled, r.wg, 0)
    pending = half_to_a(r.wg, r.gate_in, 0)
    arrive(late_copies)
    which16 = lax.broadcasted_iota(jnp.int32, (16, tok), 0)
    ffn_part = jnp.zeros((1, part), f32)
    attn_copies = []
    for i in range(nb):
        columns = jnp.transpose(r.late_small[i, :, mine])
        d_log = jnp.where(which16[:, :half] < experts, r.late_small[i, :, mine], 0.0).astype(bf16)
        mid = mixer.total(i, 0) + dot(d_log, router, TN)
        value = r.hidden[i]
        grad = r.cotc[i, mine, :].astype(f32) + gain_mid * mid - value * columns[:, 8:9]
        r.d_attn[i, mine, :] = grad.astype(bf16)
        attn_copies.append(ship(r.d_attn.at[i, mine, :], r.d_attn.at[i, mine, :], core))
        ffn_part = ffn_part + jnp.sum(mid * value, axis=0, keepdims=True)
        r.d_hidden[i] = grad
    act_lines[0].take(act_lines[0].order[0])
    arrive(attn_copies)

    @pl.loop(0, nb)
    def _(i):
        term = dot(r.d_attn[i], r.wo[...].reshape(part, width)).astype(bf16)
        for h in range(heads):
            r.pq[h, rows_of(i), :] = term[:, h * head : (h + 1) * head]

    heads_sum = net.reduce(r.pq, r.gq)

    expert_grad(1, r.scaled, r.wg, 1)
    pending += half_to_a(r.wg, r.gate_in, 1)
    results = [move(r.wg.at[a], r.gate_own)]
    heads_sum.inner()
    expert_grad(2, r.scaled, r.wu, 0)

    def experts_out():
        for line in act_lines:
            rest(line)

        @pl.loop(0, nb)
        def _(i):
            total = 0.0
            for e in range(experts):
                r.pkv[1, 0:tok, :] = expand(0, i, e)
                piece = r.wd[:, :, e * ff : (e + 1) * ff].reshape(part, ff)
                total = total + dot(r.pkv[1, 0:tok, :], piece, NT)
            mixer.put(i, 1, total, i)

    term = dot(r.d_attn[...].reshape(col, part), r.ho[...], TN).astype(bf16)
    r.gout[...] = term.reshape(na, sub, width)
    pending += to_a(r.gout, r.gout_in)
    extra = 0.0
    for i in range(nb):
        d_log = jnp.where(which16 < experts, r.late_small[i], 0.0).astype(bf16)
        extra = extra + dot(d_log, r.scaled[i])
    which_row = lax.broadcasted_iota(jnp.int32, (16, part), 0)
    r.extra_own[...] = jnp.where(which_row == experts + 1, ffn_part, extra)
    heads_sum.wait()
    for line in act_lines[1:]:
        line.begin()

    r.gain_acc[...] = jnp.zeros_like(r.gain_acc)

    @pl.loop(0, nb)
    def _(i):
        rows = rows_of(i)
        cot = heads_sum.total(rows).astype(bf16)
        r.pq[b, rows, :] = cot
        delta = jnp.sum(cot.astype(f32) * r.ho[rows, head_lane].astype(f32), axis=1, keepdims=True)
        r.stat[rows, 4:5] = delta

    def attend_back(block, first, last, start, stop):
        @pl.loop(start // deep, stop // deep)
        def _(i):
            rows = deep_rows(i)
            columns = deep_ids(i)
            query, cot = r.q_rot[rows, :], r.pq[b, rows, :]
            keys, values = r.kv[block, :, :head], r.kv[block, :, head:]
            scores = dot(query, keys, NT) * scale
            keep = columns[:, 3:4] == r.docs[block]
            probs = jnp.where(keep, jnp.exp(scores - r.stat[rows, 2:3]), 0.0)
            d_scores = (probs * (dot(cot, values, NT) - r.stat[rows, 4:5])).astype(bf16)
            key_term = dot(d_scores, query, TN) * scale
            value_term = dot(probs.astype(bf16), cot, TN)

            @pl.when(i == 0)
            def _():
                r.dkv_acc[:, :head] = key_term
                r.dkv_acc[:, head:] = value_term

            @pl.when(i > 0)
            def _():
                r.dkv_acc[:, :head] += key_term
                r.dkv_acc[:, head:] += value_term

            grad = dot(d_scores, keys) * scale
            if not first:
                grad = r.head_acc[rows, :] + grad
            if not last:
                r.head_acc[rows, :] = grad
            else:
                source = r.raw[rows, :head]
                grad, gain_part = unrope(
                    grad, source, r.gains[0:1, :], r.cos_tab[rows, :], r.sin_tab[rows, :]
                )
                r.gain_acc[0:1, :] += gain_part
                r.wide[0, rows, head_lane] = grad.astype(bf16)
                r.stat[rows, 3:4] = jnp.sum(grad * source, axis=1, keepdims=True)

    kv_back = []
    for k in range(1, na):
        attend_back(lax.rem(a + k, na), k == 1, False, 0, nb)
        r.dkv_send[k - 1] = r.dkv_acc[...].astype(bf16)
        kv_back.append(ship(r.dkv_send.at[k - 1], r.dkv_in.at[k - 1], a_peers[k - 1]))
    for line in act_lines[1:]:
        line.take(line.order[0])
    pending += half_to_a(r.wu, r.up_in, 0)
    q_lines = []
    for s in range(2):
        attend_back(a, na == 1, True, s * (nb // 2), (s + 1) * (nb // 2))
        q_lines.append(
            net.spread(lambda i, s=s: head_block(r.wide.at[0], i, s * (col // 2), col // 2))
        )
    expert_grad(2, r.scaled, r.wu, 1)
    pending += half_to_a(r.wu, r.up_in, 1)
    results.append(move(r.wu.at[a], r.up_own))
    for line in q_lines:
        line.take(line.order[0])
    arrive(kv_back)

    @pl.loop(0, nb)
    def _(i):
        rows = rows_of(i)
        both = r.dkv_acc[rows, :]
        for k in range(na - 1):
            both = both + r.dkv_in[k, rows, :].astype(f32)
        source = r.raw[rows, head : 2 * head]
        grad, gain_part = unrope(
            both[:, :head], source, r.gains[1:2, :], r.cos_tab[rows, :], r.sin_tab[rows, :]
        )
        r.gain_acc[1:2, :] += gain_part
        value_grad = both[:, head:]
        r.wide[1, rows, head_lane] = grad.astype(bf16)
        r.wide[2, rows, head_lane] = value_grad.astype(bf16)
        r.stat[rows, 3:4] += jnp.sum(
            grad * source + value_grad * r.raw[rows, 2 * head :], axis=1, keepdims=True
        )

    place16 = (b * 2 + y) * 2 + c
    r.s4[place16] = transpose_columns([r.stat[i * tok : (i + 1) * tok, 3:4] for i in range(nb)], tok)
    r.s4[place16, 4:6, 0:head] = r.gain_acc[0:2, :]
    s4_copies = [ship(r.s4.at[place16], r.s4.at[place16], place) for place in group]

    def kv_piece(s):
        def block(i):
            lane = pl.ds(pl.multiple_of(i * head, head), head)
            return r.wide.at[pl.ds(1, 2), pl.ds(s * tok, tok), lane]

        return net.spread(block, start=s < 2)

    kv_lines = [kv_piece(s) for s in range(nb)]
    def weight_grad(j):
        grad = dot(r.hn[...].reshape(col, part), r.wide[j], TN).astype(bf16)
        r.gsend[j] = grad.reshape(na, sub, width)
        return to_a(r.gsend.at[j], r.gin_w.at[j])

    for line in q_lines:
        line.take(line.order[1])
        line.take(line.order[2])
    pending += weight_grad(0)
    mixer_in = TwoLevel(net, r.acc, r.sendc, r.recvc, r.sendy, r.recvy, 1)
    mixer.finish()
    def in_term(i):
        rest(kv_lines[i])
        rows = slice(i * tok, (i + 1) * tok)
        term = dot(r.wide[0, rows, :], weight(0), NT) + dot(r.wide[1, rows, :], weight(1), NT)
        mixer_in.put(i, 0, term + dot(r.wide[2, rows, :], weight(2), NT), i)
        mixer_in.onward(i, 0, i)

    chain(kv_lines, 0)
    experts_out()
    chain(kv_lines, 1)
    for i in range(nb):
        mixer.onward(i, 1, i)
    expert_grad(0, r.cotc, r.wd, 0)
    pending += half_to_a(r.wd, r.down_in, 0)
    arrive(s4_copies)
    in_term(0)
    chain(kv_lines, 2)
    expert_grad(0, r.cotc, r.wd, 1)
    pending += half_to_a(r.wd, r.down_in, 1)
    results.append(move(r.wd.at[a], r.down_own))
    in_term(1)
    chain(kv_lines, 3)
    for j in range(nb):
        r.out_half[j] = (r.hidden[j] + mixer.total(j, 1)).astype(bf16)
    r.block_out[mine, own_lane] = r.out_half[b]
    in_term(2)
    in_term(3)
    out_rows = pl.ds(pl.multiple_of(y * quarter, quarter), quarter)
    out_copies = [
        ship(r.out_half.at[d, out_rows, :], r.block_out.at[fourth, own_lane], {"b": d})
        for d in exchange
    ]

    def lanes_onward(copies, rows, place):
        more = []
        for source_b, copy in zip(exchange, copies):
            copy.wait_recv()
            block = r.block_out.at[rows, lane_of(source_b)]
            more.append(ship(block, block, place))
        return more

    pending += weight_grad(1)
    pending += weight_grad(2)
    sums = r.s4[0]
    for k in range(1, 4 * nb):
        sums = sums + r.s4[k]
    inner_columns = jnp.transpose(sums)
    attn_part = jnp.zeros((1, part), f32)
    in_hops = []
    base_in = net.used
    net.used += nb

    def in_hop(d, slot):
        return pltpu.make_async_remote_copy(
            src_ref=r.d_attn.at[d, pl.ds(0, half), :],
            dst_ref=r.gin.at[mine, own_lane],
            send_sem=r.send.at[base_in + d],
            recv_sem=r.recv.at[base_in + slot],
            device_id={"b": jnp.int32(d)},
            device_id_type=MESH,
        )

    drain(attn_copies)
    for i in range(nb):
        d_in = mixer_in.total(i, 0)
        r_col = r.ids[i, mine, 0:1]
        inner = jnp.where(
            c == 0, inner_columns[:half, i : i + 1], inner_columns[half:, i : i + 1]
        )
        x = r.xc[i, mine, :].astype(f32)
        scaled = d_in * r_col
        grad = r.d_hidden[i] + scaled * gain_in - x * (r_col * r_col * inner / model)
        attn_part = attn_part + jnp.sum(scaled * x, axis=0, keepdims=True)
        r.d_attn[i, :half, :] = grad.astype(bf16)

        @pl.when(b == i)
        def _():
            r.gin[mine, own_lane] = r.d_attn[i, :half, :]

        @pl.when(b != i)
        def _():
            in_hop(i, b).start()

    r.extra_own[...] = jnp.where(which_row == experts + 2, attn_part, r.extra_own[...])
    tail_copy = ship(r.extra_own, r.extra_in, core)
    tail_copy.wait_recv()
    shared = (which_row == experts + 1) | (which_row == experts + 2)
    r.tail_all[a] = r.extra_own[...] + jnp.where(shared, r.extra_in[...], 0.0)
    r.tail_all[a, experts + 3 : experts + 5, 0:head] = sums[4:6, 0:head]
    tail_copies = over_a(r.tail_all.at[a], r.tail_all)
    out_y = lanes_onward(out_copies, fourth, across)
    in_more = []
    for k in range(1, nb):
        place = lax.rem(b + k, nb)
        lane = lane_of(place)
        pltpu.make_async_remote_copy(
            src_ref=r.gin.at[mine, lane],
            dst_ref=r.gin.at[mine, lane],
            send_sem=r.send.at[base_in + place],
            recv_sem=r.recv.at[base_in + place],
            device_id=core,
            device_id_type=MESH,
        ).wait_recv()
        in_more.append(ship(r.gin.at[mine, lane], r.gin.at[mine, lane], core))
    in_more.append(ship(r.gin.at[mine, own_lane], r.gin.at[mine, own_lane], core))
    out_more = lanes_onward(out_y, mine, core)
    block = r.block_out.at[mine, own_lane]
    out_more.append(ship(block, block, core))
    arrive(pending)
    for j in range(4):
        mine_here = r.gsend[j, a] if j < 3 else r.gout[a]
        total = mine_here.astype(f32)
        for k in range(na - 1):
            came = r.gin_w[j, k] if j < 3 else r.gout_in[k]
            total = total + came.astype(f32)
        r.proj[j] = total
    results.append(move(r.proj, r.proj_out))
    arrive(out_more)
    results.append(move(r.block_out, r.out_rows))
    arrive(tail_copies)
    r.tail[...] = jnp.sum(r.tail_all[...], axis=0)
    arrive(in_more)
    results.append(move(r.gin, r.in_rows))
    mixer_in.finish()
    mixer.finish((1,))
    for line in [heads_sum, pay_line] + act_lines + cd_sums + ho_lines + q_lines + kv_lines:
        line.finish()
    for d in range(nb):

        @pl.when(b != d)
        def _():
            in_hop(d, b).wait_send()

    drain(list(sent))
    for copy in results:
        copy.wait()
    assert net.used <= r.send.shape[0] and local_used[0] <= r.local.shape[0]


def layer(sizes, dims, ins):
    nb, na, head, heads, experts, ff, top = dims
    tok, model = ins[0].shape
    part, col, half = model // nb, nb * tok, tok // 2
    sub, width, wide = part // na, heads * head, experts * ff
    others = max(na - 1, 1)
    shape = jax.ShapeDtypeStruct
    vmem, hbm = pl.BlockSpec(memory_space=pltpu.VMEM), pl.BlockSpec(memory_space=pl.ANY)
    outs = [
        shape((tok, model), bf16),
        shape((tok, model), bf16),
        shape((sub, wide), bf16),
        shape((sub, wide), bf16),
        shape((sub, wide), bf16),
        shape((others, sub, wide), bf16),
        shape((others, sub, wide), bf16),
        shape((others, sub, wide), bf16),
        shape((4, sub, width), f32),
        shape((16, part), f32),
    ]
    work = dict(
        xc=((nb, tok, part), bf16),
        cotc=((nb, tok, part), bf16),
        rows_all=((na, nb, 8, tok), f32),
        rows_own=((8, tok), f32),
        cols_own=((16, sub), f32),
        cols_all=((na, 16, sub), f32),
        cols_sum=((16, part), f32),
        wqkv=((3, na, sub, width), bf16),
        wo=((na, sub, width), bf16),
        wg=((na, sub, wide), bf16),
        wu=((na, sub, wide), bf16),
        wd=((na, sub, wide), bf16),
        stage=((sub, experts, ff), bf16),
        hn=((nb, tok, part), bf16),
        raw=((col, 3 * head), f32),
        q_rot=((col, head), bf16),
        kv=((na, col, 2 * head), bf16),
        stat=((col, 128), f32),
        ho=((col, width), bf16),
        cos_tab=((col, head), f32),
        sin_tab=((col, head), f32),
        pkv=((nb, col, 2 * head), bf16),
        gkv=((nb, col, 2 * head), bf16),
        pq=((nb, col, head), bf16),
        gq=((nb, col, head), bf16),
        pcd=((top, nb, ff // head * tok, head), bf16),
        gcd=((top, nb, ff // head * tok, head), bf16),
        acc=((nb, half, part), f32),
        sendc=((nb, half, 2 * part), bf16),
        recvc=((nb, half, 2 * part), bf16),
        sendy=((nb, half, 2 * part), bf16),
        recvy=((nb, half, 2 * part), bf16),
        hidden=((nb, half, part), f32),
        d_hidden=((nb, half, part), f32),
        scaled=((nb, tok, part), bf16),
        small=((nb, 16, tok), f32),
        small_in=((nb, 16, tok), f32),
        pay=((nb, tok, 3 * top * ff), bf16),
        wide=((3, col, width), bf16),
        pair=((4, 8, tok), f32),
        late_small=((nb, 16, tok), f32),
        extra_own=((16, part), f32),
        extra_in=((16, part), f32),
        d_attn=((nb, tok, part), bf16),
        out_half=((nb, half, part), bf16),
        block_out=((tok, model), bf16),
        head_acc=((col, head), f32),
        dkv_acc=((col, 2 * head), f32),
        dkv_send=((others, col, 2 * head), bf16),
        dkv_in=((others, col, 2 * head), bf16),
        gsend=((3, na, sub, width), bf16),
        gin_w=((3, others, sub, width), bf16),
        gout=((na, sub, width), bf16),
        gout_in=((others, sub, width), bf16),
        gin=((tok, model), bf16),
        s4=((4 * nb, 8, tok), f32),
        gain_acc=((8, head), f32),
        tail_all=((na, 16, part), f32),
        ids=((nb, tok, 8), f32),
        gains=((8, head), f32),
        docs=((na, 1, col), f32),
        proj=((4, sub, width), f32),
    )
    count = 158 + 26 * na
    scratch = [pltpu.VMEM(*work[name]) for name in WORK[:-3]] + [
        pltpu.SemaphoreType.DMA((count,)),
        pltpu.SemaphoreType.DMA((count,)),
        pltpu.SemaphoreType.DMA((15,)),
    ]
    return pl.pallas_call(
        functools.partial(layer_kernel, sizes, dims),
        out_shape=outs,
        in_specs=[hbm] * 9 + [vmem] * 8,
        out_specs=[hbm] * 9 + [vmem],
        scratch_shapes=scratch,
        compiler_params=pltpu.CompilerParams(
            collective_id=1, has_side_effects=True, vmem_limit_bytes=67043328
        ),
        name="layer",
    )(*ins)


def last_kernel(experts, ff, sub, *refs):
    out_rows, in_rows, owns, cames, proj = refs[0], refs[1], refs[2:5], refs[5:8], refs[8]
    tail, refs = refs[9], refs[10:]
    block_out, grad_in, grads, projections = refs[0], refs[1], refs[2:5], refs[5:9]
    router, gain_attn, gain_ffn, gain_q, gain_k = refs[9:]
    step = 32

    @pl.loop(0, block_out.shape[0] // step)
    def _(n):
        rows = pl.ds(pl.multiple_of(n * step, step), step)
        block_out[rows, :] = out_rows[rows, :]
        grad_in[rows, :] = in_rows[rows, :].astype(f32)

    @pl.loop(0, owns[0].shape[0] // step)
    def _(n):
        rows = pl.ds(pl.multiple_of(n * step, step), step)
        for own, came, grad in zip(owns, cames, grads):
            for e in range(experts):
                lane = slice(e * ff, (e + 1) * ff)
                total = own[rows, lane].astype(f32)
                for k in range(came.shape[0]):
                    total = total + came[k, rows, lane].astype(f32)
                grad[rows, e, :] = total
        for j in range(4):
            projections[j][rows, :] = proj[j, rows, :]

    @pl.when(pl.program_id(0) == 0)
    def _():
        a = lax.axis_index("a")
        piece = tail[:, :sub]
        for k in range(1, tail.shape[1] // sub):
            piece = jnp.where(a == k, tail[:, k * sub : (k + 1) * sub], piece)
        router[...] = piece[:experts]
        gain_ffn[...] = piece[experts + 1 : experts + 2]
        gain_attn[...] = piece[experts + 2 : experts + 3]
        gain_q[...] = tail[experts + 3 : experts + 4, : gain_q.shape[1]]
        gain_k[...] = tail[experts + 4 : experts + 5, : gain_k.shape[1]]


def last(dims, ins):
    nb, na, head, heads, experts, ff, top = dims
    tok, model = ins[0].shape
    sub, wide = ins[2].shape
    others, width = ins[5].shape[0], ins[8].shape[2]
    steps = 2
    shape = jax.ShapeDtypeStruct
    rows = pl.BlockSpec((tok // steps, model), lambda i: (i, 0))
    own = pl.BlockSpec((sub // steps, wide), lambda i: (i, 0))
    came = pl.BlockSpec((others, sub // steps, wide), lambda i: (0, i, 0))
    grad = pl.BlockSpec((sub // steps, experts, ff), lambda i: (i, 0, 0))
    flat = pl.BlockSpec((sub // steps, width), lambda i: (i, 0))
    small = [shape((experts, sub), f32), shape((1, sub), f32), shape((1, sub), f32)]
    small += [shape((1, head), f32)] * 2
    return pl.pallas_call(
        functools.partial(last_kernel, experts, ff, sub),
        grid=(steps,),
        out_shape=[shape((tok, model), bf16), shape((tok, model), f32)]
        + [shape((sub, experts, ff), f32)] * 3
        + [shape((sub, width), f32)] * 4
        + small,
        in_specs=[rows, rows] + [own] * 3 + [came] * 3
        + [pl.BlockSpec((4, sub // steps, width), lambda i: (0, i, 0))]
        + [pl.BlockSpec(ins[9].shape, lambda i: (0, 0))],
        out_specs=[rows, rows] + [grad] * 3 + [flat] * 4
        + [pl.BlockSpec(item.shape, lambda i: (0, 0)) for item in small],
        name="last",
    )(*ins)


def on_device(
    sizes,
    tokens_in,
    doc_ids,
    expert_ids,
    attn_gain,
    q_gain,
    k_gain,
    w_query,
    w_key,
    w_value,
    w_output,
    ffn_gain,
    w_router,
    w_gate,
    w_up,
    w_down,
    cotangent,
):
    nb, na = sizes["b"], sizes["a"]
    tok, model = tokens_in.shape
    part = model // nb
    sub = part // na
    head = q_gain.shape[0]
    width = w_query.shape[1]
    heads = width // head
    experts, ff = w_gate.shape[1], w_gate.shape[2]
    top = expert_ids.shape[1]
    dims = (nb, na, head, heads, experts, ff, top)

    speed = theta ** (-2.0 * (np.arange(head) % (head // 2)) / head)
    parts = layer(
        sizes,
        dims,
        [
            tokens_in, cotangent, w_query, w_key, w_value, w_output, w_gate, w_up, w_down,
            expert_ids.T, doc_ids[None], w_router.T, attn_gain, ffn_gain, q_gain[None],
            k_gain[None], jnp.asarray(speed, f32)[None],
        ],
    )
    (
        block_out, grad_in, grad_gate, grad_up, grad_down, grad_query, grad_key, grad_value,
        grad_output, router, gain_attn, gain_ffn, gain_q, gain_k,
    ) = last(dims, parts)
    return (
        block_out,
        grad_in,
        gain_attn.reshape(sub),
        gain_q.reshape(head),
        gain_k.reshape(head),
        grad_query,
        grad_key,
        grad_value,
        grad_output,
        gain_ffn.reshape(sub),
        router.T,
        grad_gate,
        grad_up,
        grad_down,
    )


def solution(mesh):
    cp, tp = mesh.shape["cp"], mesh.shape["tp"]
    sizes = {"b": 4, "a": cp // 4, "y": 2, "c": tp // 2}
    split = Mesh(mesh.devices.reshape([sizes[axis] for axis in AXES]), AXES)
    cp, tp = ("b", "a"), ("y", "c")
    return jax.shard_map(
        functools.partial(on_device, sizes),
        mesh=split,
        in_specs=(
            P(cp, None),
            P(cp),
            P(cp, None),
            P(cp),
            P(),
            P(),
            P(cp, tp),
            P(cp, tp),
            P(cp, tp),
            P(cp, tp),
            P(cp),
            P(cp, None),
            P(cp, None, tp),
            P(cp, None, tp),
            P(cp, None, tp),
            P(cp, None),
        ),
        out_specs=(
            P(cp, None),
            P(cp, None),
            P(cp),
            P(),
            P(),
            P(cp, tp),
            P(cp, tp),
            P(cp, tp),
            P(cp, tp),
            P(cp),
            P(cp, None),
            P(cp, None, tp),
            P(cp, None, tp),
            P(cp, None, tp),
        ),
        check_vma=False,
    )
```
